128 devices in a mesh: gx: 4 (over z_hi, core), gy: 4 (over y), gz: 8 (over x, z_lo).
Axes of the slice: x: 4, y: 4, z: 4 (z_hi: 2, z_lo: 2; z = z_hi * 2 + z_lo), core: 2. Of those that a mesh axis runs over, the one named last changes fastest.
Arguments:
- right_side: float32 [128, 128, 1024], P('gx', 'gy', 'gz'), may hold values from -8 to 8
- guess: float32 [128, 128, 1024], P('gx', 'gy', 'gz'), may hold values from -4 to 4
Outputs:
- solution_field: float32 [128, 128, 1024], P('gx', 'gy', 'gz')
- residual: float32 [128, 128, 1024], P('gx', 'gy', 'gz')
The draws below stay inside these ranges and needn't reach their ends.
All inputs are finite; a program needn't handle non-finite values.
Results may differ from the reference program's by a relative error of at most 0.0001.
Values sent between devices are 32-bit elements; how exact they have to be, the bound alone decides.
A program may use at most 128 MiB of HBM per device.

```python
import jax
import jax.numpy as jnp

LEVELS = 6
SWEEPS = 4
STEPS = 2
NX = 128
NY = 128
NZ = 1024


def level_of(stream_key, dims, cuts, low, largest):
    level = 1.0
    for position, shards_of in cuts:
        heights = jax.random.uniform(jax.random.fold_in(jax.random.fold_in(stream_key, 6), position), (shards_of,), jnp.float32, low / len(cuts), largest / len(cuts))
        level = level * jnp.repeat(jnp.exp(heights), dims[position] // shards_of).reshape((-1,) + (1,) * (len(dims) - 1 - position))
    return level


def centred(own_key, shape, width, limit, pieces=(), kind=jnp.bfloat16):
    drawn = width * jax.random.normal(own_key, shape, jnp.float32)
    if pieces:
        drawn = drawn * level_of(own_key, shape, pieces, -0.22, 0.18)
    return jnp.clip(drawn, -limit, limit).astype(kind)


def setup_inputs(seed: int = 0) -> dict:
    keys = jax.random.split(jax.random.key(seed), 3)
    return {
        "right_side": centred(keys[0], (NX, NY, NZ), 1.0, 8.0, ((0, 4), (1, 4), (2, 8)), jnp.float32),
        "guess": centred(keys[1], (NX, NY, NZ), 0.5, 4.0, ((0, 4), (1, 4), (2, 8)), jnp.float32),
    }


damping = 2.0 / 3.0


def stencil(field):
    padded = jnp.pad(field, 1)
    beside = padded[2:, 1:-1, 1:-1] + padded[:-2, 1:-1, 1:-1]
    beside = beside + padded[1:-1, 2:, 1:-1] + padded[1:-1, :-2, 1:-1]
    beside = beside + padded[1:-1, 1:-1, 2:] + padded[1:-1, 1:-1, :-2]
    return 6.0 * field - beside


def restrict(field):
    first, second, third = field.shape
    blocks = field.reshape(first // 2, 2, second // 2, 2, third // 2, 2)
    return jnp.mean(blocks, axis=(1, 3, 5))


def prolong(field):
    first, second, third = field.shape
    spread = jnp.broadcast_to(field[:, None, :, None, :, None], (first, 2, second, 2, third, 2))
    return spread.reshape(first * 2, second * 2, third * 2)


def smooth(rhs, level_index):
    scaling = 0.25 ** level_index
    diagonal_value = 6.0 * scaling
    approx = damping * rhs / diagonal_value
    for sweep_index in range(SWEEPS - 1):
        approx = approx + damping * (rhs - scaling * stencil(approx)) / diagonal_value
    return approx


def precondition(residual):
    chain = [residual]
    for level_index in range(1, LEVELS):
        chain.append(restrict(chain[-1]))
    correction = smooth(chain[LEVELS - 1], LEVELS - 1)
    for level_index in range(LEVELS - 2, -1, -1):
        correction = prolong(correction) + smooth(chain[level_index], level_index)
    return correction


def reference(right_side, guess):
    solution_field = guess
    residual = right_side - stencil(guess)
    for step_index in range(STEPS):
        direction = precondition(residual)
        image = stencil(direction)
        alpha = jnp.sum(residual * direction) / jnp.sum(direction * image)
        solution_field = solution_field + alpha * direction
        residual = residual - alpha * image
    return solution_field, residual
```

```python
import functools

import jax
import jax.numpy as jnp
from jax import lax
from jax.experimental import pallas as pl
from jax.experimental.pallas import tpu as pltpu
from jax.sharding import PartitionSpec as P

F32 = jnp.float32
BF16 = jnp.bfloat16
MESH = pl.DeviceIdType.MESH
NGX, NGY, NGZ = 4, 4, 8

S_R1 = 0
S_SET = 6
SET = 50
O_X, O_Y, O_Z, O_Z3, O_C3, O_ARX, O_ARY, O_ARZ = 0, 6, 8, 10, 12, 28, 32, 36
NSEM = S_SET + 2 * SET


def roll(v, shift, axis):
    n = v.shape[axis]
    shift = shift % n
    return v if shift == 0 else pltpu.roll(v, shift, axis)


def iota(shape, axis):
    return lax.broadcasted_iota(jnp.int32, shape, axis)


def dotx(x, m):
    hi = x.astype(BF16)
    rest = x - hi.astype(F32)
    mid = rest.astype(BF16)
    low = (rest - mid.astype(F32)).astype(BF16)
    dot = functools.partial(jnp.dot, preferred_element_type=F32)
    return dot(hi, m) + dot(mid, m) + dot(low, m)


def kernel(
    rhs, u, sol, res,
    UR, ZR, G0, G1, G2, SA0, SB0, SA1, SB1, SA2, SB2, R, W, V, Z0, Y0,
    Q1, Q2, YS, YR, ZS, ZV, R1S, R1R, C3, H3, H3R,
    G3, SA3, SB3, C3P, G4, SA4, SB4, G5, SA5, SB5,
    ZP0, ZP1, ZP2, ZP3, ZP4, M0, ARX, ARY, ARZ, ss, rs,
):
    gx, gy, gz = lax.axis_index("gx"), lax.axis_index("gy"), lax.axis_index("gz")
    x_up, x_dn = gx < NGX - 1, gx > 0
    y_up, y_dn = gy < NGY - 1, gy > 0
    z_up, z_dn = gz < NGZ - 1, gz > 0
    one = lambda c: jnp.where(c, F32(1.0), F32(0.0))
    fxu, fxd, fyu, fyd, fzu, fzd = map(one, (x_up, x_dn, y_up, y_dn, z_up, z_dn))
    gxu, gxd = lax.rem(gx + 1, NGX), lax.rem(gx + NGX - 1, NGX)
    gyu, gyd = lax.rem(gy + 1, NGY), lax.rem(gy + NGY - 1, NGY)
    gzu, gzd = lax.rem(gz + 1, NGZ), lax.rem(gz + NGZ - 1, NGZ)

    pending = []

    def rcopy(src, dst, i, dev):
        return pltpu.make_async_remote_copy(
            src_ref=src, dst_ref=dst, send_sem=ss.at[i], recv_sem=rs.at[i],
            device_id=dev, device_id_type=MESH,
        )

    def send(copy, cond=None):
        if cond is None:
            copy.start()
        else:
            pl.when(cond)(lambda: copy.start())
        pending.append((copy, cond))

    def sent(copy, cond):
        pending[:] = [q for q in pending if q[0] is not copy]
        pl.when(cond)(copy.wait_send)

    def recv(copy, cond=None):
        if cond is None:
            copy.wait_recv()
        else:
            pl.when(cond)(lambda: copy.wait_recv())

    UR[...] = jnp.zeros_like(UR)
    for k in range(2):
        G0[k, 0, 32:40] = jnp.zeros((8, 40, 128), F32)
        G1[k, 16:24] = jnp.zeros((8, 24, 128), F32)
        G2[k, 8:16] = jnp.zeros((8, 16, 128), F32)
    YR[...] = jnp.zeros_like(YR)
    ZV[...] = jnp.zeros_like(ZV)
    R1R[...] = jnp.zeros_like(R1R)
    H3R[...] = jnp.zeros_like(H3R)

    bar = pltpu.get_barrier_semaphore()
    peers = 0
    for dx in range(NGX):
        for dy in range(NGY):
            if dx or dy:
                peers += 1
                pl.semaphore_signal(
                    bar, inc=1, device_id_type=MESH,
                    device_id={"gx": lax.rem(gx + dx, NGX), "gy": lax.rem(gy + dy, NGY)},
                )
    for dz in range(1, NGZ):
        peers += 1
        pl.semaphore_signal(bar, inc=1, device_id_type=MESH, device_id={"gz": lax.rem(gz + dz, NGZ)})
    pl.semaphore_wait(bar, peers)

    lane8 = iota((8, 128), 1)
    row8 = iota((8, 128), 0)
    lane32 = iota((32, 128), 1)
    lane40 = iota((40, 128), 1)

    r1x = [
        rcopy(u.at[pl.ds(31, 1)], UR.at[0, pl.ds(39, 1), pl.ds(0, 32)], S_R1 + 0, {"gx": gxu}),
        rcopy(u.at[pl.ds(0, 1)], UR.at[0, pl.ds(32, 1), pl.ds(0, 32)], S_R1 + 1, {"gx": gxd}),
    ]
    send(r1x[0], x_up)
    send(r1x[1], x_dn)
    for p in range(32):
        R1S[0, p : p + 1, :] = u[p, 31:32, :]
        R1S[1, p : p + 1, :] = u[p, 0:1, :]
    zh = jnp.zeros((32, 128), F32)
    zl = jnp.zeros((32, 128), F32)
    for p in range(32):
        v = u[p]
        zh = jnp.where(lane32 == p, roll(v, p - 127, 1), zh)
        zl = jnp.where(lane32 == p, roll(v, p, 1), zl)
    R1S[2] = zh
    R1S[3] = zl
    devs = [{"gy": gyu}, {"gy": gyd}, {"gz": gzu}, {"gz": gzd}]
    conds = [y_up, y_dn, z_up, z_dn]
    backs = [y_dn, y_up, z_dn, z_up]
    r1 = [rcopy(R1S.at[i], R1R.at[i], S_R1 + 2 + i, devs[i]) for i in range(4)]
    for i in range(4):
        send(r1[i], conds[i])
    def mask9(rows, ny, lanes_in, hi_y, lo_y):
        row, lane = iota((rows, 128), 0), iota((rows, 128), 1)
        my = jnp.where(row < ny, F32(1.0), jnp.where(row < ny + 4, hi_y, lo_y))
        mz = jnp.where(lane < lanes_in, F32(1.0), jnp.where(lane < 96, fzu, fzd))
        return my * mz * F32(1.0 / 9.0)

    M0[0] = mask9(40, 32, 128, fyu, fyd)
    M0[1] = mask9(40, 32, 0, fyu, fyd)

    UR[0, 0:32, 0:32] = u[...]
    recv(r1x[0], x_dn)
    recv(r1x[1], x_up)
    for i in range(4):
        recv(r1[i], backs[i])
    for p in range(32):
        UR[0, p, 32:40] = jnp.where(
            row8 == 0, jnp.broadcast_to(R1R[1, p : p + 1, :], (8, 128)),
            jnp.where(row8 == 7, jnp.broadcast_to(R1R[0, p : p + 1, :], (8, 128)), F32(0.0)),
        )
        UR[1, p, 0:32] = jnp.where(
            lane32 == 0, roll(R1R[3], -p, 1), jnp.where(lane32 == 127, roll(R1R[2], 127 - p, 1), F32(0.0))
        )

    def apply_plane(ring, p):
        v = ring[0, p]
        h = ring[1, p, 0:32]
        c = v[0:32]
        ysum = (roll(v, 1, 0) + roll(v, -1, 0))[0:32]
        left = jnp.where(lane32 == 0, roll(h, 1, 1), roll(c, 1, 1))
        right = jnp.where(lane32 == 127, roll(h, -1, 1), roll(c, -1, 1))
        prev = jnp.where(p == 0, 39, p - 1)
        xsum = ring[0, prev, 0:32] + ring[0, p + 1, 0:32]
        return c, 6.0 * c - (xsum + ysum + left + right)

    def first(c, _):
        for i in range(4):
            p = 4 * c + i
            _, a = apply_plane(UR, p)
            r = rhs[p] - a
            R[p] = r
        return 0

    lax.fori_loop(0, 8, first, 0)

    kk, jj = iota((128, 128), 0), iota((128, 128), 1)

    def const(cond, value):
        return jnp.where(cond, F32(value), F32(0.0)).astype(BF16)

    rz1 = const((kk >> 1) == jj, 0.5)
    rz2 = const((kk >> 2) == jj, 0.25)
    base = lax.rem(gx, 2) * 64
    rz3 = [const((kk >> 3) + (base + 16 * i) == jj, 0.125) for i in range(4)]
    ring_k = jnp.where(kk < 96, kk >> 1, (kk >> 1) + 64)
    ring_j = jnp.where(jj < 96, jj >> 1, (jj >> 1) + 64)
    rring = const(ring_k == jj, 0.5)
    pring = const(ring_j == kk, 1.0)
    p0a = const((jj >> 1) == kk, 1.0)
    p0b = const((jj >> 1) + 64 == kk, 1.0)

    m1 = mask9(24, 16, 64, fyu, fyd)
    m2 = mask9(16, 8, 32, fyu, fyd)
    zero = F32(0.0)
    m3 = mask9(24, 16, 16, zero, zero)
    m4 = mask9(16, 8, 8, zero, zero)
    m5 = mask9(8, 4, 4, zero, zero)

    def sweep0(src, dst, g):
        def body(c, _):
            p0 = 4 * c
            prev = jnp.where(c == 0, 39, p0 - 1)
            nxt = jnp.where(c == 9, 0, p0 + 4)
            xm = jnp.where(c == 8, fxu, jnp.where(c == 9, fxd, F32(1.0)))
            idx = [prev, p0, p0 + 1, p0 + 2, p0 + 3, nxt]
            a = [src[0, i] for i in idx]
            b = [src[1, i] for i in idx]
            ma, mb = M0[0] * xm, M0[1] * xm
            for i in range(1, 5):
                va, vb = a[i], b[i]
                ra, rb = roll(va, 1, 1), roll(vb, 1, 1)
                la, lb = roll(va, -1, 1), roll(vb, -1, 1)
                na = jnp.where(lane40 == 0, rb, ra) + jnp.where(lane40 == 127, lb, la)
                nb = jnp.where(lane40 == 0, ra, rb) + jnp.where(lane40 == 127, la, lb)
                na = na + roll(va, 1, 0) + roll(va, -1, 0) + a[i - 1] + a[i + 1]
                nb = nb + roll(vb, 1, 0) + roll(vb, -1, 0) + b[i - 1] + b[i + 1]
                dst[0, p0 + i - 1] = ma * (3.0 * va + na) + g[0, p0 + i - 1]
                dst[1, p0 + i - 1] = mb * (3.0 * vb + nb) + g[1, p0 + i - 1]
            return 0

        lax.fori_loop(0, 10, body, 0)

    def plane_sweep(a, prev, nxt, m9, g):
        n = roll(a, 1, 1) + roll(a, -1, 1) + roll(a, 1, 0) + roll(a, -1, 0) + prev + nxt
        return m9 * (3.0 * a + n) + g

    def sweep12(src, dst, g, n, m9):
        total = n + 8

        def body(c, _):
            p0 = 4 * c
            prev = jnp.where(c == 0, total - 1, p0 - 1)
            nxt = jnp.where(c == total // 4 - 1, 0, p0 + 4)
            xm = jnp.where(c == n // 4, fxu, jnp.where(c == n // 4 + 1, fxd, F32(1.0)))
            a = [src[i] for i in (prev, p0, p0 + 1, p0 + 2, p0 + 3, nxt)]
            m = m9 * xm
            for i in range(1, 5):
                dst[p0 + i - 1] = plane_sweep(a[i], a[i - 1], a[i + 1], m, g[p0 + i - 1])
            return 0

        lax.fori_loop(0, total // 4, body, 0)

    def sweeps_small(g, sa, sb, n, m9):
        sa[n] = jnp.zeros_like(sa[n])
        sb[n] = jnp.zeros_like(sb[n])
        for src, dst in ((g, sa), (sa, sb), (sb, sa)):
            for p in range(n):
                dst[p] = plane_sweep(src[p], src[n if p == 0 else p - 1], src[p + 1], m9, g[p])
        return sa

    def restrict_xy(src, dst, n, rows):
        for i in range(n):
            a, b = src.at[2 * i], src.at[2 * i + 1]
            even, odd = pl.ds(0, rows, stride=2), pl.ds(1, rows, stride=2)
            dst[i, 0:rows] = 0.25 * ((a[even, :] + a[odd, :]) + (b[even, :] + b[odd, :]))

    def double_rows(dst, v):
        n = v.shape[0]
        dst[pl.ds(0, n, stride=2), :] = v
        dst[pl.ds(1, n, stride=2), :] = v

    half = row8 < 4

    def y_tile(z, rows):
        return jnp.where(half, z[rows : rows + 8], z[rows + 8 : rows + 16])

    def all_reduce_start(tile, k):
        o = S_SET + SET * k
        ARX[k, gx] = tile
        return [
            rcopy(ARX.at[k, gx], ARX.at[k, gx], o + O_ARX + d - 1, {"gx": lax.rem(gx + d, NGX)})
            for d in range(1, NGX)
        ]

    def all_reduce_x(copies, k):
        o = S_SET + SET * k
        for c in copies:
            recv(c)
        tile = ARX[k, 0]
        for i in range(1, NGX):
            tile = tile + ARX[k, i]
        ARY[k, gy] = tile
        return [
            rcopy(ARY.at[k, gy], ARY.at[k, gy], o + O_ARY + d - 1, {"gy": lax.rem(gy + d, NGY)})
            for d in range(1, NGY)
        ]

    def all_reduce_y(copies, k):
        o = S_SET + SET * k
        for c in copies:
            recv(c)
        tile = ARY[k, 0]
        for i in range(1, NGY):
            tile = tile + ARY[k, i]
        ARZ[k, gz] = tile
        return [
            rcopy(ARZ.at[k, gz], ARZ.at[k, gz], o + O_ARZ + d - 1, {"gz": lax.rem(gz + d, NGZ)})
            for d in range(1, NGZ)
        ]

    def all_reduce_z(copies, k):
        for c in copies:
            recv(c)
        tile = ARZ[k, 0]
        for i in range(1, NGZ):
            tile = tile + ARZ[k, i]
        along = jnp.sum(tile[0:1], axis=1, keepdims=True)
        curve = jnp.sum(tile[1:2], axis=1, keepdims=True)
        return along / curve

    def send_all(copies):
        for c in copies:
            send(c)

    def dots_tile(a, b):
        a = jnp.sum(a, axis=0, keepdims=True)
        b = jnp.sum(b, axis=0, keepdims=True)
        return jnp.where(row8 == 0, a, jnp.where(row8 == 1, b, F32(0.0)))

    def fold(x):
        return (x[0:8] + x[8:16]) + (x[16:24] + x[24:32])

    def precondition(rin, k, ar_copies):
        o = S_SET + SET * k
        g0, g1, g2 = G0.at[k], G1.at[k], G2.at[k]
        g0[0, 0:32, 0:32] = rin[...]
        xs = [
            (rcopy(g0.at[0, pl.ds(28, 4), pl.ds(0, 32)], g0.at[0, pl.ds(36, 4), pl.ds(0, 32)], o + O_X + 0, {"gx": gxu}), x_up, x_dn),
            (rcopy(g0.at[0, pl.ds(0, 4), pl.ds(0, 32)], g0.at[0, pl.ds(32, 4), pl.ds(0, 32)], o + O_X + 1, {"gx": gxd}), x_dn, x_up),
        ]
        for c, s, _ in xs:
            send(c, s)
        if ar_copies is not None:
            send_all(ar_copies)
        restrict_xy(rin, Q1, 16, 16)
        Q2[:, 8:16] = jnp.zeros((8, 8, 128), F32)
        restrict_xy(Q1, Q2, 8, 8)
        tile3 = jnp.zeros((8, 128), F32)
        odd_y = lax.rem(gy, 2) == 1
        for i in range(4):
            a, b = Q2.at[2 * i], Q2.at[2 * i + 1]
            even, odd = pl.ds(0, 8, stride=2), pl.ds(1, 8, stride=2)
            q3 = 0.25 * ((a[even, :] + a[odd, :]) + (b[even, :] + b[odd, :]))
            q3 = jnp.where(odd_y, roll(q3, 4, 0), q3)
            tile3 = tile3 + dotx(q3, rz3[i])
        mine = gx * NGY + gy
        C3[k, mine] = tile3
        c3 = []
        for dx in range(NGX):
            for dy in range(NGY):
                if dx or dy:
                    c3.append(rcopy(
                        C3.at[k, mine], C3.at[k, mine], o + O_C3 + dx * NGY + dy,
                        {"gx": lax.rem(gx + dx, NGX), "gy": lax.rem(gy + dy, NGY)},
                    ))
        send_all(c3)
        g2[0:8, 0:8] = dotx(Q2[:, 0:8].reshape(64, 128), rz2).reshape(8, 8, 128)
        g1[0:16, 0:16] = dotx(Q1[...].reshape(256, 128), rz1).reshape(16, 16, 128)
        more = [
            (rcopy(g1.at[pl.ds(12, 4), pl.ds(0, 16)], g1.at[pl.ds(20, 4), pl.ds(0, 16)], o + O_X + 2, {"gx": gxu}), x_up, x_dn),
            (rcopy(g1.at[pl.ds(0, 4), pl.ds(0, 16)], g1.at[pl.ds(16, 4), pl.ds(0, 16)], o + O_X + 3, {"gx": gxd}), x_dn, x_up),
            (rcopy(g2.at[pl.ds(4, 4), pl.ds(0, 8)], g2.at[pl.ds(12, 4), pl.ds(0, 8)], o + O_X + 4, {"gx": gxu}), x_up, x_dn),
            (rcopy(g2.at[pl.ds(0, 4), pl.ds(0, 8)], g2.at[pl.ds(8, 4), pl.ds(0, 8)], o + O_X + 5, {"gx": gxd}), x_dn, x_up),
        ]
        for c, s, _ in more:
            send(c, s)
        for c, _, r in xs + more:
            recv(c, r)
        parts = []
        for g, n, off, lead in ((g0.at[0], 32, 0, 20), (g1, 16, 20, 12), (g2, 8, 32, 8)):
            parts.append((g, n, off, lead))
            ah, bh = g[0:lead, n - 8 : n], g[lead : 2 * lead, n - 8 : n]
            al, bl = g[0:lead, 0:8], g[lead : 2 * lead, 0:8]
            sel = jnp.broadcast_to(half[None], (lead, 8, 128))
            YS[k, 0, off : off + lead] = jnp.where(sel, roll(ah, 4, 1), bh)
            YS[k, 1, off : off + lead] = jnp.where(sel, al, roll(bl, 4, 1))
        ys = [
            (rcopy(YS.at[k, 0], YR.at[k, 0], o + O_Y + 0, {"gy": gyu}), y_up, y_dn),
            (rcopy(YS.at[k, 1], YR.at[k, 1], o + O_Y + 1, {"gy": gyd}), y_dn, y_up),
        ]
        for c, s, _ in ys:
            send(c, s)
        ar_next = None
        if ar_copies is not None:
            ar_next = all_reduce_x(ar_copies, 0)
            send_all(ar_next)
        for c in c3:
            recv(c)
        for t in range(2):
            for rh in range(2):
                s = [C3[k, (2 * t + i) * NGY + 2 * rh + j] for i in range(2) for j in range(2)]
                H3[k, t, 8 * rh : 8 * rh + 8] = (s[0] + s[1]) + (s[2] + s[3])
        z3 = [
            (rcopy(H3.at[k], H3R.at[k, 0], o + O_Z3 + 0, {"gz": gzu}), z_up, z_dn),
            (rcopy(H3.at[k], H3R.at[k, 1], o + O_Z3 + 1, {"gz": gzd}), z_dn, z_up),
        ]
        for c, s, _ in z3:
            send(c, s)
        for c, _, r in ys:
            recv(c, r)
        for c, sc, _ in more:
            sent(c, sc)
        for g, n, off, lead in parts:
            hi, lo = YR[k, 1, off : off + lead], YR[k, 0, off : off + lead]
            sel = jnp.broadcast_to(half[None], (lead, 8, 128))
            g[0:lead, n : n + 8] = jnp.where(sel, hi, roll(lo, 4, 1))
            g[lead : 2 * lead, n : n + 8] = jnp.where(sel, roll(hi, 4, 1), lo)
        slot_id = lane40 >> 2
        slots = [(h, s) for h in range(2) for s in range(32)]

        def slot_source(h, s):
            if s < 20:
                return [(g0.at[0], 20 * h + s, 0, 40, 128)]
            i = 12 * h + s - 20
            out = [(g1, i, 0, 24, 64)]
            if i < 16:
                out.append((g2, i, 24, 16, 32))
            return out

        for h in range(2):
            up = jnp.zeros((40, 128), F32)
            dn = jnp.zeros((40, 128), F32)
            for s in range(32):
                src = slot_source(h, s)
                a = [roll(g[p], 4 * s - (nz - 4), 1) for g, p, _, _, nz in src]
                b = [roll(g[p], 4 * s, 1) for g, p, _, _, nz in src]
                if sum(x[3] for x in src) < 40:
                    a.append(jnp.zeros((16, 128), F32))
                    b.append(jnp.zeros((16, 128), F32))
                a = a[0] if len(a) == 1 else jnp.concatenate(a, axis=0)
                b = b[0] if len(b) == 1 else jnp.concatenate(b, axis=0)
                up = jnp.where(slot_id == s, a, up)
                dn = jnp.where(slot_id == s, b, dn)
            ZS[k, 0, h] = up
            ZS[k, 1, h] = dn
        zs = [
            (rcopy(ZS.at[k, 0], ZV.at[k, 0], o + O_Z + 0, {"gz": gzu}), z_up, z_dn),
            (rcopy(ZS.at[k, 1], ZV.at[k, 1], o + O_Z + 1, {"gz": gzd}), z_dn, z_up),
        ]
        for c, s, _ in zs:
            send(c, s)
        if ar_next is not None:
            ar_next = all_reduce_y(ar_next, 0)
            send_all(ar_next)
        for c, _, r in z3:
            recv(c, r)
        lane16 = iota((16, 128), 1)
        for p in range(16):
            t, off = p // 8, (p % 8) * 16
            own, lo, hi = H3[k, t], H3R[k, 0, t], H3R[k, 1, t]
            v = jnp.where(lane16 >= 112, roll(lo, 112 - off, 1), F32(0.0))
            v = jnp.where(lane16 < 32, roll(hi, 16 - off, 1), v)
            G3[p, 0:16] = jnp.where(lane16 < 16, roll(own, -off, 1), v)
            G3[p, 16:24] = jnp.zeros((8, 128), F32)
        G3[16] = jnp.zeros((24, 128), F32)

        def restrict_small(src, dst, n, rows):
            q = []
            for i in range(n):
                a, b = src.at[2 * i], src.at[2 * i + 1]
                even, odd = pl.ds(0, 8, stride=2), pl.ds(1, 8, stride=2)
                q.append(0.25 * ((a[even, :] + a[odd, :]) + (b[even, :] + b[odd, :])))
            q = dotx(jnp.concatenate(q, axis=0), rring)
            for i in range(n):
                dst[i, 0:8] = q[8 * i : 8 * i + 8]
                if rows > 8:
                    dst[i, 8:rows] = jnp.zeros((rows - 8, 128), F32)
            dst[n] = jnp.zeros((rows, 128), F32)

        restrict_small(G3, G4, 8, 16)
        restrict_small(G4, G5, 4, 8)
        s5 = sweeps_small(G5, SA5, SB5, 4, m5)
        c5 = jnp.concatenate([s5[i] for i in range(4)], axis=0) * F32(4.0**5 / 9.0)
        t5 = dotx(c5, pring)
        for i in range(4):
            double_rows(ZP4.at[i], t5[8 * i : 8 * i + 8])
        s4 = sweeps_small(G4, SA4, SB4, 8, m4)
        c4 = jnp.concatenate([s4[i] * F32(4.0**4 / 9.0) + ZP4[i // 2] for i in range(8)], axis=0)
        t4 = dotx(c4, pring)
        for i in range(8):
            double_rows(ZP3.at[i], t4[16 * i : 16 * i + 16])
        s3 = sweeps_small(G3, SA3, SB3, 16, m3)
        C3P[0] = jnp.zeros((32, 128), F32)
        C3P[17] = jnp.zeros((32, 128), F32)
        for i in range(16):
            C3P[i + 1, 0:8] = jnp.zeros((8, 128), F32)
            C3P[i + 1, 8:32] = s3[i] * F32(4.0**3 / 9.0) + ZP3[i // 2, 0:24]
        start = 8 + 4 * gy - 2
        c3l = [roll(C3P[4 * gx + i, pl.ds(start, 8), :], -2, 0) for i in range(6)]
        t3 = dotx(jnp.concatenate(c3l, axis=0), pring)
        for i in range(6):
            double_rows(ZP2.at[i], t3[8 * i : 8 * i + 8])
        for c, _, r in zs:
            recv(c, r)
        for h in range(2):
            lo, hi = ZV[k, 0, h], ZV[k, 1, h]
            for s in range(32):
                for g, p, row, rows, nz in slot_source(h, s):
                    lov, hiv = lo[row : row + rows], hi[row : row + rows]
                    lanes = lane40[0:rows]
                    left = roll(lov, 124 - 4 * s, 1)
                    if nz == 128:
                        right = roll(hiv, -4 * s, 1)
                        v = jnp.where(lanes < 4, right, jnp.where(lanes >= 124, left, F32(0.0)))
                        g0[1, p] = v
                    else:
                        right = roll(hiv, nz - 4 * s, 1)
                        v = jnp.where(lanes >= 124, left, g[p])
                        g[p] = jnp.where((lanes >= nz) & (lanes < nz + 4), right, v)
        sweep12(g2, SA2, g2, 8, m2)
        sweep12(SA2, SB2, g2, 8, m2)
        sweep12(SB2, SA2, g2, 8, m2)
        c2 = []
        for p in range(16):
            v = SA2[p] * F32(16.0 / 9.0)
            src = 1 + p // 2 if p < 8 else 5 if p == 8 else 0 if p == 15 else None
            c2.append(v if src is None else v + ZP2[src])
        t2 = dotx(jnp.concatenate(c2, axis=0), pring)
        for p in range(16):
            double_rows(ZP1.at[p], t2[16 * p : 16 * p + 16])
        sweep12(g1, SA1, g1, 16, m1)
        sweep12(SA1, SB1, g1, 16, m1)
        sweep12(SB1, SA1, g1, 16, m1)
        for p in list(range(17)) + [23]:
            src = p // 2 if p < 17 else 15
            z = ZP1[src]
            zz = jnp.concatenate([z[0:16], y_tile(z, 16)], axis=0)
            c1 = SA1[p] * F32(4.0 / 9.0) + zz
            double_rows(ZP0.at[0, p], dotx(c1, p0a))
            double_rows(ZP0.at[1, p], dotx(c1, p0b))
        sweep0(g0, SA0, g0)
        sweep0(SA0, SB0, g0)
        sweep0(SB0, SA0, g0)

        def put(p, src):
            for t in range(2):
                z = ZP0[t, src]
                zz = jnp.concatenate([z[0:32], y_tile(z, 32)], axis=0)
                ZR[t, p] = SA0[t, p] * F32(1.0 / 9.0) + zz

        def combine(c, _):
            for i in range(4):
                put(4 * c + i, 2 * c + i // 2)
            return 0

        lax.fori_loop(0, 8, combine, 0)
        put(32, 16)
        put(39, 23)
        return ar_next

    precondition(R, 0, None)

    def image0(c, acc):
        a, b = acc
        for i in range(4):
            p = 4 * c + i
            z, w = apply_plane(ZR, p)
            Z0[p] = z
            W[p] = w
            a = a + fold(R[p] * z)
            b = b + fold(z * w)
        return a, b

    zero8 = jnp.zeros((8, 128), F32)
    a, b = lax.fori_loop(0, 8, image0, (zero8, zero8))
    ar = all_reduce_start(dots_tile(a, b), 0)
    ar = precondition(W, 1, ar)
    alpha = all_reduce_z(ar, 0)

    def image1(c, acc):
        a, b = acc
        for i in range(4):
            p = 4 * c + i
            y, v = apply_plane(ZR, p)
            z = Z0[p]
            w = W[p]
            sol[p] = u[p] + alpha * z
            r1 = R[p] - alpha * w
            z1 = z - alpha * y
            w1 = w - alpha * v
            R[p] = r1
            Y0[p] = z1
            V[p] = w1
            a = a + fold(r1 * z1)
            b = b + fold(z1 * w1)
        return a, b

    a, b = lax.fori_loop(0, 8, image1, (zero8, zero8))
    ar = all_reduce_start(dots_tile(a, b), 1)
    send_all(ar)
    ar = all_reduce_x(ar, 1)
    send_all(ar)
    ar = all_reduce_y(ar, 1)
    send_all(ar)
    alpha1 = all_reduce_z(ar, 1)

    def last(c, _):
        for i in range(4):
            p = 4 * c + i
            sol[p] = sol[p] + alpha1 * Y0[p]
            res[p] = R[p] - alpha1 * V[p]
        return 0

    lax.fori_loop(0, 8, last, 0)
    for copy, cond in pending:
        if cond is None:
            copy.wait_send()
        else:
            pl.when(cond)(copy.wait_send)


def shards(rhs, u):
    v = lambda *shape: pltpu.VMEM(shape, F32)
    scratch = [
        v(2, 40, 40, 128),
        v(2, 40, 40, 128),
        v(2, 2, 40, 40, 128), v(2, 24, 24, 128), v(2, 16, 16, 128),
        v(2, 40, 40, 128), v(2, 40, 40, 128),
        v(24, 24, 128), v(24, 24, 128), v(16, 16, 128), v(16, 16, 128),
        v(32, 32, 128), v(32, 32, 128), v(32, 32, 128), v(32, 32, 128), v(32, 32, 128),
        v(16, 16, 128), v(8, 16, 128),
        v(2, 2, 40, 8, 128), v(2, 2, 40, 8, 128),
        v(2, 2, 2, 40, 128), v(2, 2, 2, 40, 128),
        v(4, 32, 128), v(4, 32, 128),
        v(2, 16, 8, 128), v(2, 2, 16, 128), v(2, 2, 2, 16, 128),
        v(17, 24, 128), v(17, 24, 128), v(17, 24, 128), v(18, 32, 128),
        v(9, 16, 128), v(9, 16, 128), v(9, 16, 128),
        v(5, 8, 128), v(5, 8, 128), v(5, 8, 128),
        v(2, 24, 48, 128), v(16, 32, 128), v(6, 16, 128), v(8, 32, 128), v(4, 16, 128),
        v(2, 40, 128),
        v(2, 4, 8, 128), v(2, 4, 8, 128), v(2, 8, 8, 128),
        pltpu.SemaphoreType.DMA((NSEM,)), pltpu.SemaphoreType.DMA((NSEM,)),
    ]
    block = jax.ShapeDtypeStruct((32, 32, 128), F32)
    return pl.pallas_call(
        kernel,
        out_shape=(block, block),
        in_specs=[pl.BlockSpec(memory_space=pltpu.VMEM)] * 2,
        out_specs=[pl.BlockSpec(memory_space=pltpu.VMEM)] * 2,
        scratch_shapes=scratch,
        compiler_params=pltpu.CompilerParams(
            collective_id=0, has_side_effects=True, vmem_limit_bytes=48 * 2**20
        ),
    )(rhs, u)


def solution(mesh):
    spec = P("gx", "gy", "gz")
    return jax.shard_map(
        shards, mesh=mesh, in_specs=(spec, spec), out_specs=(spec, spec), check_vma=False
    )
```

```python
import functools

import jax
import jax.numpy as jnp
from jax import lax
from jax.experimental import pallas as pl
from jax.experimental.pallas import tpu as pltpu
from jax.sharding import PartitionSpec as P

F32 = jnp.float32
BF16 = jnp.bfloat16
MESH = pl.DeviceIdType.MESH
NGX, NGY, NGZ = 4, 4, 8
LANES = 128

S_SET = 6
SET = 60
O_X, O_Y, O_Z, O_ZL, O_Z3, O_C3, O_ARA, O_ARB = 0, 6, 8, 10, 12, 14, 30, 38
NSEM = S_SET + 2 * SET


def roll(v, shift, axis):
    n = v.shape[axis]
    shift = shift % n
    return v if shift == 0 else pltpu.roll(v, shift, axis)


def iota(shape, axis):
    return lax.broadcasted_iota(jnp.int32, shape, axis)


def dotx(x, m):
    hi = x.astype(BF16)
    rest = x - hi.astype(F32)
    mid = rest.astype(BF16)
    low = (rest - mid.astype(F32)).astype(BF16)
    n = x.shape[0]
    y = jnp.dot(jnp.concatenate([hi, mid, low], axis=0), m, preferred_element_type=F32)
    return y[0:n] + y[n : 2 * n] + y[2 * n : 3 * n]


def kernel(
    rhs_hbm, u_hbm, sol, res,
    RHS, U, ZR, ZO, G0, G1, G2, SA0, SB0, SA1, SB1, SA2, SB2, V, Z0, Y0,
    Q1, Q2, YS, YR, ZC, ZCR, ZL, ZLR, SLA, SLB, SHA, SHB, R1S, R1R, C3, H3, H3R,
    G3, SA3, SB3, C3P, G4, SA4, SB4, G5, SA5, SB5,
    ZP0, ZPO, ZP1, ZP2, ZP3, ZP4, ARA, ARB, ss, rs, ls,
):
    gx, gy, gz = lax.axis_index("gx"), lax.axis_index("gy"), lax.axis_index("gz")
    x_up, x_dn = gx < NGX - 1, gx > 0
    y_up, y_dn = gy < NGY - 1, gy > 0
    z_up, z_dn = gz < NGZ - 1, gz > 0
    one = lambda c: jnp.where(c, F32(1.0), F32(0.0))
    fxu, fxd, fyu, fyd, fzu, fzd = map(one, (x_up, x_dn, y_up, y_dn, z_up, z_dn))
    gxu, gxd = lax.rem(gx + 1, NGX), lax.rem(gx + NGX - 1, NGX)
    gyu, gyd = lax.rem(gy + 1, NGY), lax.rem(gy + NGY - 1, NGY)
    gzu, gzd = lax.rem(gz + 1, NGZ), lax.rem(gz + NGZ - 1, NGZ)
    gx_core = gx + 1 - 2 * lax.rem(gx, 2)
    gx_far = lax.rem(gx + 2, NGX)

    pending = []

    def rcopy(src, dst, i, dev):
        return pltpu.make_async_remote_copy(
            src_ref=src, dst_ref=dst, send_sem=ss.at[i], recv_sem=rs.at[i],
            device_id=dev, device_id_type=MESH,
        )

    def send(copy, cond=None):
        if cond is None:
            copy.start()
        else:
            pl.when(cond)(lambda: copy.start())
        pending.append((copy, cond))

    def sent(copy, cond):
        pending[:] = [q for q in pending if q[0] is not copy]
        pl.when(cond)(copy.wait_send)

    def recv(copy, cond=None):
        if cond is None:
            copy.wait_recv()
        else:
            pl.when(cond)(lambda: copy.wait_recv())

    def send_all(copies):
        for c in copies:
            send(c)

    inner = (pl.ds(4, 32), pl.ds(8, 32))
    get_u = pltpu.make_async_copy(u_hbm, ZR.at[inner], ls.at[0])
    get_rhs = pltpu.make_async_copy(rhs_hbm, RHS, ls.at[1])
    keep_u = pltpu.make_async_copy(u_hbm, U, ls.at[2])
    get_u.start()
    get_rhs.start()
    keep_u.start()

    ZR[3] = jnp.zeros((48, LANES), F32)
    ZR[36] = jnp.zeros((48, LANES), F32)
    for k in range(2):
        G0[k, 0:4] = jnp.zeros((4, 48, LANES), F32)
        G0[k, 36:40] = jnp.zeros((4, 48, LANES), F32)
        G1[k, 0:4] = jnp.zeros((4, 32, LANES), F32)
        G1[k, 20:24] = jnp.zeros((4, 32, LANES), F32)
        G2[k, 0:4] = jnp.zeros((4, 24, LANES), F32)
        G2[k, 12:16] = jnp.zeros((4, 24, LANES), F32)
    for ref in (YR, ZCR, ZLR, R1R, H3R):
        ref[...] = jnp.zeros_like(ref)
    bar = pltpu.get_barrier_semaphore()
    peers = 0
    for dx in range(NGX):
        for dy in range(NGY):
            if dx or dy:
                peers += 1
                pl.semaphore_signal(
                    bar, inc=1, device_id_type=MESH,
                    device_id={"gx": lax.rem(gx + dx, NGX), "gy": lax.rem(gy + dy, NGY)},
                )
    for dz in range(1, NGZ):
        for far in range(2):
            peers += 1
            pl.semaphore_signal(
                bar, inc=1, device_id_type=MESH,
                device_id={"gx": gx_far if far else gx, "gz": lax.rem(gz + dz, NGZ)},
            )
    for ref in (G3, SA3, SB3, C3P, G4, SA4, SB4, G5, SA5, SB5, Q2):
        ref[...] = jnp.zeros_like(ref)
    get_u.wait()
    pl.semaphore_wait(bar, peers)

    lane8 = iota((8, LANES), 1)
    row8 = iota((8, LANES), 0)
    lane32 = iota((32, LANES), 1)
    lane40 = iota((40, LANES), 1)

    r1x = [
        rcopy(ZR.at[pl.ds(35, 1), pl.ds(8, 32)], ZR.at[pl.ds(3, 1), pl.ds(8, 32)], 0, {"gx": gxu}),
        rcopy(ZR.at[pl.ds(4, 1), pl.ds(8, 32)], ZR.at[pl.ds(36, 1), pl.ds(8, 32)], 1, {"gx": gxd}),
    ]
    send(r1x[0], x_up)
    send(r1x[1], x_dn)
    devs = [{"gy": gyu}, {"gy": gyd}, {"gz": gzu}, {"gz": gzd}]
    conds = [y_up, y_dn, z_up, z_dn]
    backs = [y_dn, y_up, z_dn, z_up]
    r1 = [rcopy(R1S.at[i], R1R.at[i], 2 + i, devs[i]) for i in range(4)]
    zh = jnp.zeros((32, LANES), F32)
    zl = jnp.zeros((32, LANES), F32)
    for p in range(32):
        v = ZR[p + 4, 8:40]
        zh = jnp.where(lane32 == p, roll(v, p - 127, 1), zh)
        zl = jnp.where(lane32 == p, roll(v, p, 1), zl)
    R1S[2] = zh
    R1S[3] = zl
    send(r1[2], conds[2])
    send(r1[3], conds[3])
    for p in range(32):
        R1S[0, p : p + 1, :] = ZR[p + 4, 39:40, :]
        R1S[1, p : p + 1, :] = ZR[p + 4, 8:9, :]
    send(r1[0], conds[0])
    send(r1[1], conds[1])

    kk, jj = iota((LANES, LANES), 0), iota((LANES, LANES), 1)

    def const(cond, value):
        return jnp.where(cond, F32(value), F32(0.0)).astype(BF16)

    rz1 = const((kk >> 1) == (jj & 63), 0.5)
    rz2 = const((kk >> 2) == (jj & 31), 0.25)
    base = lax.rem(gx, 2) * 64
    rz3 = jnp.concatenate([const((kk >> 3) + (base + 16 * i) == jj, 0.125) for i in range(4)], axis=0)
    ring_k = jnp.where(kk < 96, kk >> 1, (kk >> 1) + 64)
    ring_j = jnp.where(jj < 96, jj >> 1, (jj >> 1) + 64)
    rring = const(ring_k == jj, 0.5)
    pring = const(ring_j == kk, 1.0)
    p0 = jnp.concatenate([const((jj >> 1) == kk, 1.0), const((jj >> 1) + 64 == kk, 1.0)], axis=1)

    ninth = F32(1.0 / 9.0)

    def mask9(rows, lo_rows, hi_rows, lanes_in):
        row, lane = iota((rows, LANES), 0), iota((rows, LANES), 1)
        my = jnp.where(row < lo_rows, fyd, jnp.where(row < hi_rows, F32(1.0), fyu))
        mz = jnp.where(lane < lanes_in, F32(1.0), jnp.where(lane < 96, fzu, fzd))
        return my * mz * ninth

    get_rhs.wait()
    recv(r1x[0], x_dn)
    recv(r1x[1], x_up)
    for i in range(4):
        recv(r1[i], backs[i])
    for c, cond in zip(r1x, (x_up, x_dn)):
        sent(c, cond)
    for p in range(32):
        ZR[p + 4, 7:8, :] = R1R[0, p : p + 1, :]
        ZR[p + 4, 40:41, :] = R1R[1, p : p + 1, :]
        ZO[p] = jnp.where(lane32 < 64, roll(R1R[3], -p, 1), roll(R1R[2], 127 - p, 1))

    def apply_plane(p):
        c = ZR[p + 4, 8:40]
        o = ZO[p]
        left = roll(jnp.where(lane32 == 127, o, c), 1, 1)
        right = roll(jnp.where(lane32 == 0, o, c), -1, 1)
        ysum = ZR[p + 4, 7:39] + ZR[p + 4, 9:41]
        xsum = ZR[p + 3, 8:40] + ZR[p + 5, 8:40]
        return c, 6.0 * c - ((xsum + ysum) + (left + right))

    def first(c, _):
        for i in range(4):
            p = 4 * c + i
            _, a = apply_plane(p)
            G0[0, p + 4, 8:40] = RHS[p] - a
        return 0

    lax.fori_loop(0, 8, first, 0)

    m0 = mask9(40, 4, 36, 128)
    m1 = mask9(24, 4, 20, 64)
    m2 = mask9(16, 4, 12, 32)
    m3 = mask9(16, 0, 16, 16)
    m4 = mask9(8, 0, 8, 8)
    m5 = jnp.where(row8 < 4, mask9(8, 0, 8, 4), F32(0.0))
    slot_lane = lane40 - 12 * sum((lane40 >= 12 * i).astype(jnp.int32) for i in range(1, 11))
    slot_low = slot_lane < 6
    my0 = jnp.where(lane40 < 12, fxd, jnp.where(lane40 < 108, F32(1.0), fxu)) * m0
    ms_lo = my0 * jnp.where(slot_low, fzd, F32(1.0))
    ms_hi = my0 * jnp.where(slot_low, F32(1.0), fzu)

    def stencil_sum(v, up_row, dn_row, prev, nxt):
        return ((up_row + dn_row) + (prev + nxt)) + (roll(v, 1, 1) + roll(v, -1, 1))

    def sweep_plane(src, dst, g, p, r0, r1, m):
        v = src[p, r0:r1]
        n = stencil_sum(v, src[p, r0 - 1 : r1 - 1], src[p, r0 + 1 : r1 + 1], src[p - 1, r0:r1], src[p + 1, r0:r1])
        dst[p, r0:r1] = m * (3.0 * v + n) + g[p, r0:r1]

    def sweep0(src, dst, g, j):
        for p in range(j, 4):
            sweep_plane(src, dst, g, p, 4, 44, m0 * fxd)

        def body(c, _):
            for i in range(8):
                sweep_plane(src, dst, g, 8 * c + 4 + i, 4, 44, m0)
            return 0

        lax.fori_loop(0, 4, body, 0)
        for p in range(36, 40 - j):
            sweep_plane(src, dst, g, p, 4, 44, m0 * fxu)

    def sweeps12(g, sa, sb, n, m):
        lo, hi = m * fxd, m * fxu
        for j, (src, dst) in enumerate(((g, sa), (sa, sb), (sb, sa)), 1):
            for p in range(j, n + 8 - j):
                sweep_plane(src, dst, g, p, 4, 12 + n, lo if p < 4 else m if p < n + 4 else hi)

    def sweeps_small(g, sa, sb, n, rows, m):
        for src, dst in ((g, sa), (sa, sb), (sb, sa)):
            for p in range(1, n + 1):
                sweep_plane(src, dst, g, p, 8, 8 + rows, m)
        return sa

    def sweep_slab(src, dst, g, m):
        for q in range(4):
            v = src[q, 4:44]
            prev = src[q - 1, 4:44] if q else roll(src[3, 4:44], 12, 1)
            nxt = src[q + 1, 4:44] if q < 3 else roll(src[0, 4:44], -12, 1)
            n = stencil_sum(v, src[q, 3:43], src[q, 5:45], prev, nxt)
            dst[q, 4:44] = m * (3.0 * v + n) + g[q, 4:44]

    def pair_mean(a, b, first_row, rows):
        even, odd = pl.ds(first_row, rows, stride=2), pl.ds(first_row + 1, rows, stride=2)
        return 0.25 * ((a[even, :] + a[odd, :]) + (b[even, :] + b[odd, :]))

    def double_rows(dst, v):
        n = v.shape[0]
        dst[pl.ds(0, n, stride=2), :] = v
        dst[pl.ds(1, n, stride=2), :] = v

    def all_reduce_start(tile, k):
        o = S_SET + SET * k
        mine = lax.rem(gx, 2) * NGY + gy
        ARA[k, mine] = tile
        copies = []
        for dc in range(2):
            for dy in range(NGY):
                if dc or dy:
                    dev = {"gx": gx_core if dc else gx, "gy": lax.rem(gy + dy, NGY)}
                    copies.append(rcopy(ARA.at[k, mine], ARA.at[k, mine], o + O_ARA + dc * NGY + dy, dev))
        return copies

    def total(ref, k, n):
        t = [ref[k, i] for i in range(n)]
        while len(t) > 1:
            t = [t[i] + t[i + 1] for i in range(0, len(t), 2)]
        return t[0]

    def all_reduce_next(copies, k):
        o = S_SET + SET * k
        for c in copies:
            recv(c)
        mine = (gx >> 1) * NGZ + gz
        ARB[k, mine] = total(ARA, k, 8)
        out = []
        for far in range(2):
            for dz in range(NGZ):
                if far or dz:
                    dev = {"gx": gx_far if far else gx, "gz": lax.rem(gz + dz, NGZ)}
                    out.append(rcopy(ARB.at[k, mine], ARB.at[k, mine], o + O_ARB + far * NGZ + dz, dev))
        return out

    def all_reduce_end(copies, k):
        for c in copies:
            recv(c)
        tile = total(ARB, k, 16)
        along = jnp.sum(tile[0:1], axis=1, keepdims=True)
        curve = jnp.sum(tile[1:2], axis=1, keepdims=True)
        return along / curve

    def dots_tile(a, b):
        a = jnp.sum(a, axis=0, keepdims=True)
        b = jnp.sum(b, axis=0, keepdims=True)
        return jnp.where(row8 == 0, a, jnp.where(row8 == 1, b, F32(0.0)))

    def fold(x):
        return (x[0:8] + x[8:16]) + (x[16:24] + x[24:32])

    def precondition(k, ar):
        o = S_SET + SET * k
        g0, g1, g2 = G0.at[k], G1.at[k], G2.at[k]
        xs = [
            (rcopy(g0.at[pl.ds(32, 4), pl.ds(8, 32)], g0.at[pl.ds(0, 4), pl.ds(8, 32)], o + O_X + 0, {"gx": gxu}), x_up, x_dn),
            (rcopy(g0.at[pl.ds(4, 4), pl.ds(8, 32)], g0.at[pl.ds(36, 4), pl.ds(8, 32)], o + O_X + 1, {"gx": gxd}), x_dn, x_up),
        ]
        for c, s, _ in xs:
            send(c, s)
        if ar is not None:
            send_all(ar)
        for i in range(16):
            Q1[i] = pair_mean(g0.at[2 * i + 4], g0.at[2 * i + 5], 8, 16)
        for i in range(8):
            Q2[i, 0:8] = pair_mean(Q1.at[2 * i], Q1.at[2 * i + 1], 0, 8)
        q3 = jnp.concatenate([pair_mean(Q2.at[2 * i], Q2.at[2 * i + 1], 0, 8) for i in range(4)], axis=1)
        q3 = jnp.where(lax.rem(gy, 2) == 1, roll(q3, 4, 0), q3)
        mine = gx * NGY + gy
        C3[k, mine] = dotx(q3, rz3)
        c3 = []
        for dx in range(NGX):
            for dy in range(NGY):
                if dx or dy:
                    c3.append(rcopy(
                        C3.at[k, mine], C3.at[k, mine], o + O_C3 + dx * NGY + dy,
                        {"gx": lax.rem(gx + dx, NGX), "gy": lax.rem(gy + dy, NGY)},
                    ))
        send_all(c3)
        g2[4:12, 8:16] = dotx(Q2[:, 0:8].reshape(64, LANES), rz2).reshape(8, 8, LANES)
        g1[4:20, 8:24] = dotx(Q1[...].reshape(256, LANES), rz1).reshape(16, 16, LANES)
        more = [
            (rcopy(g1.at[pl.ds(16, 4), pl.ds(8, 16)], g1.at[pl.ds(0, 4), pl.ds(8, 16)], o + O_X + 2, {"gx": gxu}), x_up, x_dn),
            (rcopy(g1.at[pl.ds(4, 4), pl.ds(8, 16)], g1.at[pl.ds(20, 4), pl.ds(8, 16)], o + O_X + 3, {"gx": gxd}), x_dn, x_up),
            (rcopy(g2.at[pl.ds(8, 4), pl.ds(8, 8)], g2.at[pl.ds(0, 4), pl.ds(8, 8)], o + O_X + 4, {"gx": gxu}), x_up, x_dn),
            (rcopy(g2.at[pl.ds(4, 4), pl.ds(8, 8)], g2.at[pl.ds(12, 4), pl.ds(8, 8)], o + O_X + 5, {"gx": gxd}), x_dn, x_up),
        ]
        for c, s, _ in more:
            send(c, s)
        for c, _, r in xs + more:
            recv(c, r)
        lane4 = iota((1, 4, LANES), 2)
        quarter = [lane4 < 32, lane4 < 64, lane4 < 96]
        for d in range(2):
            r0, r1, r2 = (36, 20, 12) if d == 0 else (8, 8, 8)
            for h in range(2):
                rows = pl.ds(4 * h, 4)
                YS[k, d, 0:20, rows] = g0[20 * h : 20 * h + 20, r0 : r0 + 4]
                a, b = g1[6 * h : 6 * h + 6, r1 : r1 + 4], g1[12 + 6 * h : 18 + 6 * h, r1 : r1 + 4]
                YS[k, d, 20:26, rows] = jnp.where(quarter[1], a, b)
                v = [g2[4 * i + 2 * h : 4 * i + 2 * h + 2, r2 : r2 + 4] for i in range(4)]
                v = jnp.where(quarter[1], jnp.where(quarter[0], v[0], v[1]), jnp.where(quarter[2], v[2], v[3]))
                YS[k, d, 26:28, rows] = v
        ys = [
            (rcopy(YS.at[k, 0], YR.at[k, 0], o + O_Y + 0, {"gy": gyu}), y_up, y_dn),
            (rcopy(YS.at[k, 1], YR.at[k, 1], o + O_Y + 1, {"gy": gyd}), y_dn, y_up),
        ]
        for c, s, _ in ys:
            send(c, s)
        for c in c3:
            recv(c)
        for t in range(2):
            for rh in range(2):
                s = [C3[k, (2 * t + i) * NGY + 2 * rh + j] for i in range(2) for j in range(2)]
                H3[k, t, 8 * rh : 8 * rh + 8] = (s[0] + s[1]) + (s[2] + s[3])
        z3 = [
            (rcopy(H3.at[k], H3R.at[k, 0], o + O_Z3 + 0, {"gz": gzu}), z_up, z_dn),
            (rcopy(H3.at[k], H3R.at[k, 1], o + O_Z3 + 1, {"gz": gzd}), z_dn, z_up),
        ]
        for c, s, _ in z3:
            send(c, s)
        if ar is not None:
            ar = all_reduce_next(ar, 0)
            send_all(ar)
        for c, _, r in ys:
            recv(c, r)
        for d in range(2):
            r0, r1, r2 = (4, 4, 4) if d == 0 else (40, 24, 16)
            for h in range(2):
                rows = pl.ds(4 * h, 4)
                g0[20 * h : 20 * h + 20, r0 : r0 + 4] = YR[k, d, 0:20, rows]
                v = YR[k, d, 20:26, rows]
                w = roll(v, 64, 2)
                g1[6 * h : 6 * h + 6, r1 : r1 + 4] = jnp.where(quarter[1], v, w)
                g1[12 + 6 * h : 18 + 6 * h, r1 : r1 + 4] = jnp.where(quarter[1], w, v)
                v = YR[k, d, 26:28, rows]
                w = [roll(v, 32 * i, 2) for i in range(4)]
                for i in range(4):
                    g2[4 * i + 2 * h : 4 * i + 2 * h + 2, r2 : r2 + 4] = jnp.where(quarter[0], w[(4 - i) % 4], w[(5 - i) % 4])
        for h in range(2):
            acc = jnp.zeros((24, LANES), F32)
            for s in range(12):
                acc = jnp.where(lane40[0:24] >> 3 == s, roll(g1[12 * h + s, 4:28], 8 * s - 60, 1), acc)
            ZL[k, 24 * h : 24 * h + 24] = acc
        acc = jnp.zeros((16, LANES), F32)
        for s in range(16):
            acc = jnp.where(lane40[0:16] >> 3 == s, roll(g2[s, 4:20], 8 * s - 28, 1), acc)
        ZL[k, 48:64] = acc
        zl = [
            (rcopy(ZL.at[k], ZLR.at[k, 0], o + O_ZL + 0, {"gz": gzu}), z_up, z_dn),
            (rcopy(ZL.at[k], ZLR.at[k, 1], o + O_ZL + 1, {"gz": gzd}), z_dn, z_up),
        ]
        for c, s, _ in zl:
            send(c, s)
        for q in range(4):
            acc = jnp.zeros((40, LANES), F32)
            for s in range(10):
                in_slot = (lane40 >= 12 * s) & (lane40 < 12 * s + 12)
                acc = jnp.where(in_slot, roll(g0[4 * s + q, 4:44], 12 * s + 6, 1), acc)
            ZC[k, q] = acc
        zs = [
            (rcopy(ZC.at[k], ZCR.at[k, 0], o + O_Z + 0, {"gz": gzu}), z_up, z_dn),
            (rcopy(ZC.at[k], ZCR.at[k, 1], o + O_Z + 1, {"gz": gzd}), z_dn, z_up),
        ]
        for c, s, _ in zs:
            send(c, s)
        sweep0(g0, SA0, g0, 1)
        sweep0(SA0, SB0, g0, 2)
        sweep0(SB0, SA0, g0, 3)
        for c, _, r in z3:
            recv(c, r)
        lane16 = iota((16, LANES), 1)
        for p in range(16):
            t, off = p // 8, (p % 8) * 16
            own, lo, hi = H3[k, t], H3R[k, 0, t], H3R[k, 1, t]
            v = jnp.where(lane16 < 32, roll(hi, 16 - off, 1), roll(lo, 112 - off, 1))
            G3[p + 1, 8:24] = jnp.where(lane16 < 16, roll(own, -off, 1), v)
        q = jnp.concatenate([pair_mean(G3.at[2 * i + 1], G3.at[2 * i + 2], 8, 8) for i in range(8)], axis=0)
        q = dotx(q, rring)
        for i in range(8):
            G4[i + 1, 8:16] = q[8 * i : 8 * i + 8]
        q = jnp.concatenate([pair_mean(G4.at[2 * i + 1], G4.at[2 * i + 2], 8, 8) for i in range(4)], axis=0)
        q = dotx(q, rring)
        for i in range(4):
            G5[i + 1, 8:16] = jnp.where(row8 < 4, q[8 * i : 8 * i + 8], F32(0.0))
        s5 = sweeps_small(G5, SA5, SB5, 4, 8, m5)
        s4 = sweeps_small(G4, SA4, SB4, 8, 8, m4)
        s3 = sweeps_small(G3, SA3, SB3, 16, 16, m3)
        t5 = dotx(jnp.concatenate([s5[i + 1, 8:16] for i in range(4)], axis=0) * F32(4.0**5 / 9.0), pring)
        for i in range(4):
            double_rows(ZP4.at[i], t5[8 * i : 8 * i + 8])
        c4 = jnp.concatenate([s4[i + 1, 8:16] * F32(4.0**4 / 9.0) + ZP4[i // 2, 0:8] for i in range(8)], axis=0)
        t4 = dotx(c4, pring)
        for i in range(8):
            double_rows(ZP3.at[i], t4[8 * i : 8 * i + 8])
        for i in range(16):
            C3P[i + 1, 8:24] = s3[i + 1, 8:24] * F32(4.0**3 / 9.0) + ZP3[i // 2]
        start = 8 + 4 * gy - 2
        c3l = [C3P[4 * gx + i, pl.ds(start, 8), :] for i in range(6)]
        t3 = dotx(jnp.concatenate(c3l, axis=0), pring)
        for i in range(6):
            double_rows(ZP2.at[i], t3[8 * i : 8 * i + 8])
        for c, s, _ in more:
            sent(c, s)
        for c, _, r in zl:
            recv(c, r)
        lane24, lane16 = lane40[0:24], lane40[0:16]
        for h in range(2):
            lo, hi = ZLR[k, 0, 24 * h : 24 * h + 24], ZLR[k, 1, 24 * h : 24 * h + 24]
            for s in range(12):
                p = 12 * h + s
                v = jnp.where(lane24 < 96, roll(hi, 60 - 8 * s, 1), roll(lo, 124 - 8 * s, 1))
                g1[p, 4:28] = jnp.where(lane24 < 64, g1[p, 4:28], v)
        lo, hi = ZLR[k, 0, 48:64], ZLR[k, 1, 48:64]
        for p in range(16):
            v = jnp.where(lane16 < 96, roll(hi, 28 - 8 * p, 1), roll(lo, 124 - 8 * p, 1))
            g2[p, 4:20] = jnp.where(lane16 < 32, g2[p, 4:20], v)
        sweeps12(g2, SA2, SB2, 8, m2)
        sweeps12(g1, SA1, SB1, 16, m1)
        c2 = [SA2[p, 4:20] * F32(16.0 / 9.0) + ZP2[(p - 2) // 2] for p in range(3, 13)]
        t2 = dotx(jnp.concatenate(c2, axis=0), pring)
        for i in range(10):
            double_rows(ZP1.at[i], t2[16 * i : 16 * i + 16])
        c1 = [SA1[p, 4:28] * F32(4.0 / 9.0) + ZP1[(p - 2) // 2, 4:28] for p in range(3, 21)]
        t1 = dotx(jnp.concatenate(c1, axis=0), p0)
        for i in range(18):
            double_rows(ZP0.at[i], t1[24 * i : 24 * i + 24, 0:128])
            double_rows(ZPO.at[i], t1[24 * i : 24 * i + 24, 128:256])
        for c, _, r in zs:
            recv(c, r)
        for q in range(4):
            own = ZC[k, q]
            SLA[0, q, 4:44] = jnp.where(slot_low, ZCR[k, 0, q], own)
            SHA[0, q, 4:44] = jnp.where(slot_low, own, ZCR[k, 1, q])
        for a, b, m in ((SLA, SLB, ms_lo), (SHA, SHB, ms_hi)):
            sweep_slab(a.at[0], a.at[1], a.at[0], m)
            sweep_slab(a.at[1], b, a.at[0], m)
            sweep_slab(b, a.at[1], a.at[0], m)
        edge40 = (lane40 < 3) | (lane40 >= 125)
        merged = [jnp.where(slot_low, SHA[1, q, 4:44], SLA[1, q, 4:44]) for q in range(4)]
        for q in range(4):
            SLB[q, 4:44] = merged[q]
            SHB[q, 4:44] = jnp.where(slot_low, SLA[1, q, 4:44], SHA[1, q, 4:44])
        for p in range(3, 37):
            s, q = p // 4, p % 4
            e = roll(SLB[q, 4:44], -(12 * s + 6), 1)
            z = jnp.where(edge40, e, SA0[p, 4:44])
            ZR[p, 4:44] = z * ninth + ZP0[(p - 2) // 2, 4:44]
            if 4 <= p < 36:
                e = roll(SHB[q, 8:40], -(12 * s + 6), 1)
                ZO[p - 4] = e * ninth + ZPO[(p - 2) // 2, 8:40]
        return ar

    precondition(0, None)

    def image0(c, acc):
        a, b = acc
        for i in range(4):
            p = 4 * c + i
            z, w = apply_plane(p)
            Z0[p] = z
            G0[1, p + 4, 8:40] = w
            a = a + fold(G0[0, p + 4, 8:40] * z)
            b = b + fold(z * w)
        return a, b

    zero8 = jnp.zeros((8, LANES), F32)
    a, b = lax.fori_loop(0, 8, image0, (zero8, zero8))
    ar = all_reduce_start(dots_tile(a, b), 0)
    ar = precondition(1, ar)
    alpha = all_reduce_end(ar, 0)
    keep_u.wait()

    def image1(c, acc):
        a, b = acc
        for i in range(4):
            p = 4 * c + i
            y, v = apply_plane(p)
            z = Z0[p]
            w = G0[1, p + 4, 8:40]
            r1 = G0[0, p + 4, 8:40] - alpha * w
            z1 = z - alpha * y
            w1 = w - alpha * v
            sol[p] = U[p] + alpha * z
            res[p] = r1
            Y0[p] = z1
            V[p] = w1
            a = a + fold(r1 * z1)
            b = b + fold(z1 * w1)
        return a, b

    a, b = lax.fori_loop(0, 8, image1, (zero8, zero8))
    ar = all_reduce_start(dots_tile(a, b), 1)
    send_all(ar)
    ar = all_reduce_next(ar, 1)
    send_all(ar)
    alpha1 = all_reduce_end(ar, 1)

    def last(c, _):
        for i in range(8):
            p = 8 * c + i
            sol[p] = sol[p] + alpha1 * Y0[p]
            res[p] = res[p] - alpha1 * V[p]
        return 0

    lax.fori_loop(0, 4, last, 0)
    for copy, cond in pending:
        if cond is None:
            copy.wait_send()
        else:
            pl.when(cond)(copy.wait_send)


def shards(rhs, u):
    v = lambda *shape: pltpu.VMEM(shape, F32)
    field = v(32, 32, 128)
    scratch = [
        field, field,
        v(40, 48, 128), field,
        v(2, 40, 48, 128), v(2, 24, 32, 128), v(2, 16, 24, 128),
        v(40, 48, 128), v(40, 48, 128),
        v(24, 32, 128), v(24, 32, 128), v(16, 24, 128), v(16, 24, 128),
        field, field, field,
        v(16, 16, 128), v(8, 16, 128),
        v(2, 2, 28, 8, 128), v(2, 2, 28, 8, 128),
        v(2, 4, 40, 128), v(2, 2, 4, 40, 128),
        v(2, 64, 128), v(2, 2, 64, 128),
        v(2, 4, 48, 128), v(4, 48, 128), v(2, 4, 48, 128), v(4, 48, 128),
        v(4, 32, 128), v(4, 32, 128),
        v(2, 16, 8, 128), v(2, 2, 16, 128), v(2, 2, 2, 16, 128),
        v(18, 32, 128), v(18, 32, 128), v(18, 32, 128), v(18, 32, 128),
        v(10, 24, 128), v(10, 24, 128), v(10, 24, 128),
        v(6, 24, 128), v(6, 24, 128), v(6, 24, 128),
        v(18, 48, 128), v(18, 48, 128), v(10, 32, 128), v(6, 16, 128), v(8, 16, 128), v(4, 16, 128),
        v(2, 8, 8, 128), v(2, 16, 8, 128),
        pltpu.SemaphoreType.DMA((NSEM,)), pltpu.SemaphoreType.DMA((NSEM,)), pltpu.SemaphoreType.DMA((3,)),
    ]
    block = jax.ShapeDtypeStruct((32, 32, 128), F32)
    return pl.pallas_call(
        kernel,
        out_shape=(block, block),
        in_specs=[pl.BlockSpec(memory_space=pl.ANY)] * 2,
        out_specs=[pl.BlockSpec(memory_space=pltpu.VMEM)] * 2,
        scratch_shapes=scratch,
        compiler_params=pltpu.CompilerParams(
            collective_id=0, has_side_effects=True, vmem_limit_bytes=56 * 2**20
        ),
    )(rhs, u)


def solution(mesh):
    spec = P("gx", "gy", "gz")
    return jax.shard_map(
        shards, mesh=mesh, in_specs=(spec, spec), out_specs=(spec, spec), check_vma=False
    )
```

```python
import functools

import jax
import jax.numpy as jnp
from jax import lax
from jax.experimental import pallas as pl
from jax.experimental.pallas import tpu as pltpu
from jax.sharding import PartitionSpec as P

F32 = jnp.float32
BF16 = jnp.bfloat16
MESH = pl.DeviceIdType.MESH
NGX, NGY, NGZ = 4, 4, 8
LANES = 128

S_SET = 6
O_X, O_Y, O_D, O_Z, O_ZL, O_C3, O_ARA, O_ARB = 0, 6, 10, 14, 16, 18, 66, 74
SET = 90
NSEM = S_SET + 2 * SET


def roll(v, shift, axis):
    n = v.shape[axis]
    shift = shift % n
    return v if shift == 0 else pltpu.roll(v, shift, axis)


def iota(shape, axis):
    return lax.broadcasted_iota(jnp.int32, shape, axis)


def dotx(x, m):
    hi = x.astype(BF16)
    rest = x - hi.astype(F32)
    mid = rest.astype(BF16)
    low = (rest - mid.astype(F32)).astype(BF16)
    n = x.shape[0]
    y = jnp.dot(jnp.concatenate([hi, mid, low], axis=0), m, preferred_element_type=F32)
    return y[0:n] + y[n : 2 * n] + y[2 * n : 3 * n]


def kernel(
    rhs_hbm, u_hbm, sol, res,
    RHS, U, ZR, ZO, G0, G1, G2, SA0, SB0, SA1, SB1, SA2, SB2, V, Z0, Y0,
    Q1, Q2, YS, YR, DS, DR, ZC, ZCR, ZL, ZLR, SLA, SLB, SHA, SHB, R1S, R1R, C3, T3,
    G3, SA3, SB3, C3P, G4, SA4, SB4, G5, SA5, SB5,
    ZP0, ZPO, ZP1, ZP2, ZP3, ZP4, ARA, ARB, ss, rs, ls,
):
    gx, gy, gz = lax.axis_index("gx"), lax.axis_index("gy"), lax.axis_index("gz")
    x_up, x_dn = gx < NGX - 1, gx > 0
    y_up, y_dn = gy < NGY - 1, gy > 0
    z_up, z_dn = gz < NGZ - 1, gz > 0
    one = lambda c: jnp.where(c, F32(1.0), F32(0.0))
    fxu, fxd, fyu, fyd, fzu, fzd = map(one, (x_up, x_dn, y_up, y_dn, z_up, z_dn))
    gxu, gxd = lax.rem(gx + 1, NGX), lax.rem(gx + NGX - 1, NGX)
    gyu, gyd = lax.rem(gy + 1, NGY), lax.rem(gy + NGY - 1, NGY)
    gzu, gzd = lax.rem(gz + 1, NGZ), lax.rem(gz + NGZ - 1, NGZ)
    gx_core = gx + 1 - 2 * lax.rem(gx, 2)
    gx_far = lax.rem(gx + 2, NGX)

    pending = []

    def rcopy(src, dst, i, dev):
        return pltpu.make_async_remote_copy(
            src_ref=src, dst_ref=dst, send_sem=ss.at[i], recv_sem=rs.at[i],
            device_id=dev, device_id_type=MESH,
        )

    def send(copy, cond=None):
        if cond is None:
            copy.start()
        else:
            pl.when(cond)(lambda: copy.start())
        pending.append((copy, cond))

    def sent(copy, cond):
        pending[:] = [q for q in pending if q[0] is not copy]
        pl.when(cond)(copy.wait_send)

    def recv(copy, cond=None):
        if cond is None:
            copy.wait_recv()
        else:
            pl.when(cond)(lambda: copy.wait_recv())

    def send_all(copies):
        for c in copies:
            send(c)

    inner = (pl.ds(4, 32), pl.ds(8, 32))
    get_u = pltpu.make_async_copy(u_hbm, ZR.at[inner], ls.at[0])
    get_rhs = pltpu.make_async_copy(rhs_hbm, RHS, ls.at[1])
    keep_u = pltpu.make_async_copy(u_hbm, U, ls.at[2])
    get_u.start()
    get_rhs.start()
    keep_u.start()

    ZR[3] = jnp.zeros((48, LANES), F32)
    ZR[36] = jnp.zeros((48, LANES), F32)
    R1R[...] = jnp.zeros_like(R1R)
    bar = pltpu.get_barrier_semaphore()
    peers = 0
    for dx in range(NGX):
        for dy in range(NGY):
            if dx or dy:
                peers += 1
                pl.semaphore_signal(
                    bar, inc=1, device_id_type=MESH,
                    device_id={"gx": lax.rem(gx + dx, NGX), "gy": lax.rem(gy + dy, NGY)},
                )
    for dz in range(1, NGZ):
        if dz in (1, NGZ - 1):
            others = [(lax.rem(gx + dx, NGX), lax.rem(gy + dy, NGY)) for dx in range(NGX) for dy in range(NGY)]
        else:
            others = [(gx, gy), (gx_far, gy)]
        for ox, oy in others:
            peers += 1
            pl.semaphore_signal(
                bar, inc=1, device_id_type=MESH, device_id={"gx": ox, "gy": oy, "gz": lax.rem(gz + dz, NGZ)}
            )
    get_u.wait()
    pl.semaphore_wait(bar, peers)

    lane8 = iota((8, LANES), 1)
    row8 = iota((8, LANES), 0)
    lane32 = iota((32, LANES), 1)
    lane40 = iota((40, LANES), 1)

    diagonals = []
    for up_x in (True, False):
        for up_y in (True, False):
            diagonals.append((
                {"gx": gxu if up_x else gxd, "gy": gyu if up_y else gyd},
                (x_up if up_x else x_dn) & (y_up if up_y else y_dn),
                (x_dn if up_x else x_up) & (y_dn if up_y else y_up),
            ))

    r1x = [
        rcopy(ZR.at[pl.ds(35, 1), pl.ds(8, 32)], ZR.at[pl.ds(3, 1), pl.ds(8, 32)], 0, {"gx": gxu}),
        rcopy(ZR.at[pl.ds(4, 1), pl.ds(8, 32)], ZR.at[pl.ds(36, 1), pl.ds(8, 32)], 1, {"gx": gxd}),
    ]
    send(r1x[0], x_up)
    send(r1x[1], x_dn)
    devs = [{"gy": gyu}, {"gy": gyd}, {"gz": gzu}, {"gz": gzd}]
    conds = [y_up, y_dn, z_up, z_dn]
    backs = [y_dn, y_up, z_dn, z_up]
    r1 = [rcopy(R1S.at[min(i, 2)], R1R.at[i], 2 + i, devs[i]) for i in range(4)]
    zz = jnp.zeros((32, LANES), F32)
    for p in range(32):
        zz = jnp.where(lane32 >> 1 == p, roll(ZR[p + 4, 8:40], 2 * p + 1, 1), zz)
    R1S[2] = zz
    send(r1[2], conds[2])
    send(r1[3], conds[3])
    for p in range(32):
        R1S[0, p : p + 1, :] = ZR[p + 4, 39:40, :]
        R1S[1, p : p + 1, :] = ZR[p + 4, 8:9, :]
    send(r1[0], conds[0])
    send(r1[1], conds[1])

    for k in range(2):
        def at_x_low():
            G0[k, 0:4] = jnp.zeros((4, 48, LANES), F32)
            G1[k, 0:4] = jnp.zeros((4, 32, LANES), F32)
            G2[k, 0:4] = jnp.zeros((4, 24, LANES), F32)

        def at_x_high():
            G0[k, 36:40] = jnp.zeros((4, 48, LANES), F32)
            G1[k, 20:24] = jnp.zeros((4, 32, LANES), F32)
            G2[k, 12:16] = jnp.zeros((4, 24, LANES), F32)

        def clear(*refs):
            def run():
                for ref in refs:
                    ref[...] = jnp.zeros_like(ref)

            return run

        pl.when(jnp.logical_not(x_dn))(at_x_low)
        pl.when(jnp.logical_not(x_up))(at_x_high)
        pl.when(jnp.logical_not(y_dn))(clear(YR.at[k, 0]))
        pl.when(jnp.logical_not(y_up))(clear(YR.at[k, 1]))
        pl.when(jnp.logical_not(z_dn))(clear(ZCR.at[k, 0], ZLR.at[k, 0], C3.at[k, 1]))
        pl.when(jnp.logical_not(z_up))(clear(ZCR.at[k, 1], ZLR.at[k, 1], C3.at[k, 2]))
        for d, (_, _, from_there) in enumerate(diagonals):
            pl.when(jnp.logical_not(from_there))(clear(DR.at[k, d]))
    for ref in (G3, SA3, SB3, C3P, G4, SA4, SB4, G5, SA5, SB5, Q2):
        ref[...] = jnp.zeros_like(ref)
    kk, jj = iota((LANES, LANES), 0), iota((LANES, LANES), 1)

    def const(cond, value):
        return jnp.where(cond, F32(value), F32(0.0)).astype(BF16)

    rz1 = const((kk >> 1) == (jj & 63), 0.5)
    rz2 = const((kk >> 2) == (jj & 31), 0.25)
    rz3 = jnp.concatenate([const((kk >> 3) + 16 * i == jj, 0.125) for i in range(4)], axis=0)
    ring_k = jnp.where(kk < 96, kk >> 1, (kk >> 1) + 64)
    ring_j = jnp.where(jj < 96, jj >> 1, (jj >> 1) + 64)
    rring = const(ring_k == jj, 0.5)
    pring = const(ring_j == kk, 1.0)
    p0 = jnp.concatenate([const((jj >> 1) == kk, 1.0), const((jj >> 1) + 64 == kk, 1.0)], axis=1)

    ninth = F32(1.0 / 9.0)

    def mask9(rows, lo_rows, hi_rows, lanes_in):
        row, lane = iota((rows, LANES), 0), iota((rows, LANES), 1)
        my = jnp.where(row < lo_rows, fyd, jnp.where(row < hi_rows, F32(1.0), fyu))
        mz = jnp.where(lane < lanes_in, F32(1.0), jnp.where(lane < 96, fzu, fzd))
        return my * mz * ninth

    get_rhs.wait()
    recv(r1x[0], x_dn)
    recv(r1x[1], x_up)
    for i in range(4):
        recv(r1[i], backs[i])
    for c, cond in zip(r1x, (x_up, x_dn)):
        sent(c, cond)
    faces = jnp.where((lane32 & 1) == 0, R1R[2], R1R[3])
    for p in range(32):
        ZR[p + 4, 7:8, :] = R1R[0, p : p + 1, :]
        ZR[p + 4, 40:41, :] = R1R[1, p : p + 1, :]
        ZO[p] = roll(faces, -(2 * p + 1), 1)

    def apply_plane(p):
        c = ZR[p + 4, 8:40]
        o = ZO[p]
        left = roll(jnp.where(lane32 == 127, o, c), 1, 1)
        right = roll(jnp.where(lane32 == 0, o, c), -1, 1)
        ysum = ZR[p + 4, 7:39] + ZR[p + 4, 9:41]
        xsum = ZR[p + 3, 8:40] + ZR[p + 5, 8:40]
        return c, 6.0 * c - ((xsum + ysum) + (left + right))

    for p in range(32):
        _, a = apply_plane(p)
        G0[0, p + 4, 8:40] = RHS[p] - a

    m0 = mask9(40, 4, 36, 128)
    m1 = mask9(24, 4, 20, 64)
    m2 = mask9(16, 4, 12, 32)
    m3 = mask9(16, 0, 16, 16)
    m4 = mask9(8, 0, 8, 8)
    m5 = jnp.where(row8 < 4, mask9(8, 0, 8, 4), F32(0.0))
    slot_lane = lane40 - 12 * sum((lane40 >= 12 * i).astype(jnp.int32) for i in range(1, 11))
    slot_low = slot_lane < 6
    my0 = jnp.where(lane40 < 12, fxd, jnp.where(lane40 < 108, F32(1.0), fxu)) * m0
    ms_lo = my0 * jnp.where(slot_low, fzd, F32(1.0))
    ms_hi = my0 * jnp.where(slot_low, F32(1.0), fzu)

    def stencil_sum(v, up_row, dn_row, prev, nxt):
        return ((up_row + dn_row) + (prev + nxt)) + (roll(v, 1, 1) + roll(v, -1, 1))

    def sweep_plane(src, dst, g, p, r0, r1, m):
        v = src[p, r0:r1]
        n = stencil_sum(v, src[p, r0 - 1 : r1 - 1], src[p, r0 + 1 : r1 + 1], src[p - 1, r0:r1], src[p + 1, r0:r1])
        dst[p, r0:r1] = m * (3.0 * v + n) + g[p, r0:r1]

    def sweep0(src, dst, g, j):
        for p in range(j, 4):
            sweep_plane(src, dst, g, p, 4, 44, m0 * fxd)

        for p in range(4, 36):
            sweep_plane(src, dst, g, p, 4, 44, m0)
        for p in range(36, 40 - j):
            sweep_plane(src, dst, g, p, 4, 44, m0 * fxu)

    def sweeps12(g, sa, sb, n, m):
        lo, hi = m * fxd, m * fxu
        for j, (src, dst) in enumerate(((g, sa), (sa, sb), (sb, sa)), 1):
            for p in range(j, n + 8 - j):
                sweep_plane(src, dst, g, p, 4, 12 + n, lo if p < 4 else m if p < n + 4 else hi)

    def sweeps_small(g, sa, sb, n, rows, m):
        for src, dst in ((g, sa), (sa, sb), (sb, sa)):
            for p in range(1, n + 1):
                sweep_plane(src, dst, g, p, 8, 8 + rows, m)
        return sa

    def sweep_slab(src, dst, g, m):
        for q in range(4):
            v = src[q, 4:44]
            prev = src[q - 1, 4:44] if q else roll(src[3, 4:44], 12, 1)
            nxt = src[q + 1, 4:44] if q < 3 else roll(src[0, 4:44], -12, 1)
            n = stencil_sum(v, src[q, 3:43], src[q, 5:45], prev, nxt)
            dst[q, 4:44] = m * (3.0 * v + n) + g[q, 4:44]

    def pair_mean(a, b, first_row, rows):
        even, odd = pl.ds(first_row, rows, stride=2), pl.ds(first_row + 1, rows, stride=2)
        return 0.25 * ((a[even, :] + a[odd, :]) + (b[even, :] + b[odd, :]))

    def double_rows(dst, v):
        n = v.shape[0]
        dst[pl.ds(0, n, stride=2), :] = v
        dst[pl.ds(1, n, stride=2), :] = v

    def all_reduce_start(tile, k):
        o = S_SET + SET * k
        mine = lax.rem(gx, 2) * NGY + gy
        ARA[k, mine] = tile
        copies = []
        for dc in range(2):
            for dy in range(NGY):
                if dc or dy:
                    dev = {"gx": gx_core if dc else gx, "gy": lax.rem(gy + dy, NGY)}
                    copies.append(rcopy(ARA.at[k, mine], ARA.at[k, mine], o + O_ARA + dc * NGY + dy, dev))
        return copies

    def total(ref, k, n):
        t = [ref[k, i] for i in range(n)]
        while len(t) > 1:
            t = [t[i] + t[i + 1] for i in range(0, len(t), 2)]
        return t[0]

    def all_reduce_next(copies, k):
        o = S_SET + SET * k
        for c in copies:
            recv(c)
        mine = (gx >> 1) * NGZ + gz
        ARB[k, mine] = total(ARA, k, 8)
        out = []
        for far in range(2):
            for dz in range(NGZ):
                if far or dz:
                    dev = {"gx": gx_far if far else gx, "gz": lax.rem(gz + dz, NGZ)}
                    out.append(rcopy(ARB.at[k, mine], ARB.at[k, mine], o + O_ARB + far * NGZ + dz, dev))
        return out

    def all_reduce_end(copies, k):
        for c in copies:
            recv(c)
        tile = total(ARB, k, 16)
        along = jnp.sum(tile[0:1], axis=1, keepdims=True)
        curve = jnp.sum(tile[1:2], axis=1, keepdims=True)
        return along / curve

    def dots_tile(a, b):
        a = jnp.sum(a, axis=0, keepdims=True)
        b = jnp.sum(b, axis=0, keepdims=True)
        return jnp.where(row8 == 0, a, jnp.where(row8 == 1, b, F32(0.0)))

    def fold(x):
        return (x[0:8] + x[8:16]) + (x[16:24] + x[24:32])

    def precondition(k, ar):
        o = S_SET + SET * k
        g0, g1, g2 = G0.at[k], G1.at[k], G2.at[k]
        if ar is not None:
            send_all(ar)
        for i in range(16):
            Q1[i] = pair_mean(g0.at[2 * i + 4], g0.at[2 * i + 5], 8, 16)
        for i in range(8):
            Q2[i, 0:8] = pair_mean(Q1.at[2 * i], Q1.at[2 * i + 1], 0, 8)
        q3 = jnp.concatenate([pair_mean(Q2.at[2 * i], Q2.at[2 * i + 1], 0, 8) for i in range(4)], axis=1)
        T3[...] = dotx(q3, rz3)
        t3 = jnp.where(lane40[0:4] < 64, T3[pl.ds(0, 4, stride=2), :], roll(T3[pl.ds(1, 4, stride=2), :], 64, 1))
        mine = gx * NGY + gy
        C3[k, 0, mine] = t3[0:2]
        c3 = []
        for dz, dev_z, s, r in ((0, gz, None, None), (1, gzu, z_up, z_dn), (2, gzd, z_dn, z_up)):
            for dx in range(NGX):
                for dy in range(NGY):
                    if dz or dx or dy:
                        c3.append((rcopy(
                            C3.at[k, 0, mine], C3.at[k, dz, mine], o + O_C3 + 16 * dz + dx * NGY + dy,
                            {"gx": lax.rem(gx + dx, NGX), "gy": lax.rem(gy + dy, NGY), "gz": dev_z},
                        ), s, r))
        for c, s, _ in c3:
            send(c, s)
        g2[4:12, 8:16] = dotx(Q2[:, 0:8].reshape(64, LANES), rz2).reshape(8, 8, LANES)
        g1[4:20, 8:24] = dotx(Q1[...].reshape(256, LANES), rz1).reshape(16, 16, LANES)
        xs = [
            (rcopy(g0.at[pl.ds(32, 4), pl.ds(8, 32)], g0.at[pl.ds(0, 4), pl.ds(8, 32)], o + O_X + 0, {"gx": gxu}), x_up, x_dn),
            (rcopy(g0.at[pl.ds(4, 4), pl.ds(8, 32)], g0.at[pl.ds(36, 4), pl.ds(8, 32)], o + O_X + 1, {"gx": gxd}), x_dn, x_up),
        ]
        more = [
            (rcopy(g1.at[pl.ds(16, 4), pl.ds(8, 16)], g1.at[pl.ds(0, 4), pl.ds(8, 16)], o + O_X + 2, {"gx": gxu}), x_up, x_dn),
            (rcopy(g1.at[pl.ds(4, 4), pl.ds(8, 16)], g1.at[pl.ds(20, 4), pl.ds(8, 16)], o + O_X + 3, {"gx": gxd}), x_dn, x_up),
            (rcopy(g2.at[pl.ds(8, 4), pl.ds(8, 8)], g2.at[pl.ds(0, 4), pl.ds(8, 8)], o + O_X + 4, {"gx": gxu}), x_up, x_dn),
            (rcopy(g2.at[pl.ds(4, 4), pl.ds(8, 8)], g2.at[pl.ds(12, 4), pl.ds(8, 8)], o + O_X + 5, {"gx": gxd}), x_dn, x_up),
        ]
        lane4 = iota((1, 4, LANES), 2)
        quarter = [lane4 < 32, lane4 < 64, lane4 < 96]

        def four(v):
            return jnp.where(quarter[1], jnp.where(quarter[0], v[0], v[1]), jnp.where(quarter[2], v[2], v[3]))

        ys, ds = [], []
        for d in range(2):
            r0, r1, r2 = (36, 20, 12) if d == 0 else (8, 8, 8)
            for h in range(2):
                rows = pl.ds(4 * h, 4)
                YS[k, d, 0:16, rows] = g0[4 + 16 * h : 20 + 16 * h, r0 : r0 + 4]
                a, b = g1[4 + 4 * h : 8 + 4 * h, r1 : r1 + 4], g1[12 + 4 * h : 16 + 4 * h, r1 : r1 + 4]
                YS[k, d, 16:20, rows] = jnp.where(quarter[1], a, b)
                YS[k, d, 20:21, rows] = four([g2[4 + 2 * i + h : 5 + 2 * i + h, r2 : r2 + 4] for i in range(4)])
            dev, s, r = (({"gy": gyu}, y_up, y_dn), ({"gy": gyd}, y_dn, y_up))[d]
            ys.append((rcopy(YS.at[k, d], YR.at[k, d], o + O_Y + d, dev), s, r))
        for d, (dev, s, r) in enumerate(diagonals):
            up_x, up_y = d < 2, d % 2 == 0
            p0_, p1, p2 = (32, 16, 8) if up_x else (4, 4, 4)
            r0, r1, r2 = (36, 20, 12) if up_y else (8, 8, 8)
            for h in range(2):
                rows = pl.ds(4 * h, 4)
                DS[k, d, 0:2, rows] = g0[p0_ + 2 * h : p0_ + 2 * h + 2, r0 : r0 + 4]
                a, b = g1[p1 + h : p1 + h + 1, r1 : r1 + 4], g1[p1 + 2 + h : p1 + 3 + h, r1 : r1 + 4]
                DS[k, d, 2:3, rows] = jnp.where(quarter[1], a, b)
                DS[k, d, 3:4, rows] = four([g2[p2 + i : p2 + i + 1, r2 : r2 + 4] for i in range(4)])
            ds.append((rcopy(DS.at[k, d], DR.at[k, d], o + O_D + d, dev), s, r))
        for c, s, _ in ds + ys + xs + more:
            send(c, s)
        if ar is not None:
            ar = all_reduce_next(ar, 0)
            send_all(ar)
        for c, _, r in xs + more + ys + ds:
            recv(c, r)
        for d in range(2):
            r0, r1, r2 = (4, 4, 4) if d == 0 else (40, 24, 16)
            for h in range(2):
                rows = pl.ds(4 * h, 4)
                g0[4 + 16 * h : 20 + 16 * h, r0 : r0 + 4] = YR[k, d, 0:16, rows]
                v = YR[k, d, 16:20, rows]
                w = roll(v, 64, 2)
                g1[4 + 4 * h : 8 + 4 * h, r1 : r1 + 4] = jnp.where(quarter[1], v, w)
                g1[12 + 4 * h : 16 + 4 * h, r1 : r1 + 4] = jnp.where(quarter[1], w, v)
                v = YR[k, d, 20:21, rows]
                w = [roll(v, 32 * i, 2) for i in range(4)]
                for i in range(4):
                    g2[4 + 2 * i + h : 5 + 2 * i + h, r2 : r2 + 4] = jnp.where(quarter[0], w[(4 - i) % 4], w[(5 - i) % 4])
        for d in range(4):
            up_x, up_y = d < 2, d % 2 == 0
            p0_, p1, p2 = (0, 0, 0) if up_x else (36, 20, 12)
            r0, r1, r2 = (4, 4, 4) if up_y else (40, 24, 16)
            for h in range(2):
                rows = pl.ds(4 * h, 4)
                g0[p0_ + 2 * h : p0_ + 2 * h + 2, r0 : r0 + 4] = DR[k, d, 0:2, rows]
                v = DR[k, d, 2:3, rows]
                w = roll(v, 64, 2)
                g1[p1 + h : p1 + h + 1, r1 : r1 + 4] = jnp.where(quarter[1], v, w)
                g1[p1 + 2 + h : p1 + 3 + h, r1 : r1 + 4] = jnp.where(quarter[1], w, v)
            v = DR[k, d, 3:4, 0:4]
            w = [roll(v, 32 * i, 2) for i in range(4)]
            for i in range(4):
                g2[p2 + i : p2 + i + 1, r2 : r2 + 4] = jnp.where(quarter[0], w[(4 - i) % 4], w[(5 - i) % 4])
        for h in range(2):
            acc = jnp.zeros((24, LANES), F32)
            for s in range(12):
                acc = jnp.where(lane40[0:24] >> 3 == s, roll(g1[12 * h + s, 4:28], 8 * s - 60, 1), acc)
            ZL[k, 24 * h : 24 * h + 24] = acc
        acc = jnp.zeros((16, LANES), F32)
        for s in range(16):
            acc = jnp.where(lane40[0:16] >> 3 == s, roll(g2[s, 4:20], 8 * s - 28, 1), acc)
        ZL[k, 48:64] = acc
        zl = [
            (rcopy(ZL.at[k], ZLR.at[k, 0], o + O_ZL + 0, {"gz": gzu}), z_up, z_dn),
            (rcopy(ZL.at[k], ZLR.at[k, 1], o + O_ZL + 1, {"gz": gzd}), z_dn, z_up),
        ]
        for c, s, _ in zl:
            send(c, s)
        for q in range(4):
            acc = jnp.zeros((40, LANES), F32)
            for s in range(10):
                in_slot = (lane40 >= 12 * s) & (lane40 < 12 * s + 12)
                acc = jnp.where(in_slot, roll(g0[4 * s + q, 4:44], 12 * s + 6, 1), acc)
            ZC[k, q] = acc
        zs = [
            (rcopy(ZC.at[k], ZCR.at[k, 0], o + O_Z + 0, {"gz": gzu}), z_up, z_dn),
            (rcopy(ZC.at[k], ZCR.at[k, 1], o + O_Z + 1, {"gz": gzd}), z_dn, z_up),
        ]
        for c, s, _ in zs:
            send(c, s)
        sweep0(g0, SA0, g0, 1)
        sweep0(SA0, SB0, g0, 2)
        sweep0(SB0, SA0, g0, 3)
        for c, _, r in c3:
            recv(c, r)
        for g in range(4):
            own, lo, hi = (jnp.concatenate([C3[k, i, 4 * g + j] for j in range(4)], axis=0) for i in range(3))
            for px in range(4):
                for odd in range(2):
                    off = 16 * px + 64 * odd
                    v = jnp.where(lane8 < 32, roll(hi, 16 - off, 1), roll(lo, 112 - off, 1))
                    v = jnp.where(lane8 < 16, roll(own, -off, 1), v)
                    G3.at[4 * g + px + 1][pl.ds(8 + odd, 8, stride=2), :] = v
        q = jnp.concatenate([pair_mean(G3.at[2 * i + 1], G3.at[2 * i + 2], 8, 8) for i in range(8)], axis=0)
        q = dotx(q, rring)
        for i in range(8):
            G4[i + 1, 8:16] = q[8 * i : 8 * i + 8]
        q = jnp.concatenate([pair_mean(G4.at[2 * i + 1], G4.at[2 * i + 2], 8, 8) for i in range(4)], axis=0)
        q = dotx(q, rring)
        for i in range(4):
            G5[i + 1, 8:16] = jnp.where(row8 < 4, q[8 * i : 8 * i + 8], F32(0.0))
        s5 = sweeps_small(G5, SA5, SB5, 4, 8, m5)
        s4 = sweeps_small(G4, SA4, SB4, 8, 8, m4)
        s3 = sweeps_small(G3, SA3, SB3, 16, 16, m3)
        t5 = dotx(jnp.concatenate([s5[i + 1, 8:16] for i in range(4)], axis=0) * F32(4.0**5 / 9.0), pring)
        for i in range(4):
            double_rows(ZP4.at[i], t5[8 * i : 8 * i + 8])
        c4 = jnp.concatenate([s4[i + 1, 8:16] * F32(4.0**4 / 9.0) + ZP4[i // 2, 0:8] for i in range(8)], axis=0)
        t4 = dotx(c4, pring)
        for i in range(8):
            double_rows(ZP3.at[i], t4[8 * i : 8 * i + 8])
        for i in range(16):
            C3P[i + 1, 8:24] = s3[i + 1, 8:24] * F32(4.0**3 / 9.0) + ZP3[i // 2]
        start = 8 + 4 * gy - 2
        c3l = [C3P[4 * gx + i, pl.ds(start, 8), :] for i in range(6)]
        t3 = dotx(jnp.concatenate(c3l, axis=0), pring)
        for i in range(6):
            double_rows(ZP2.at[i], t3[8 * i : 8 * i + 8])
        for c, s, _ in more:
            sent(c, s)
        for c, _, r in zl:
            recv(c, r)
        lane24, lane16 = lane40[0:24], lane40[0:16]
        for h in range(2):
            lo, hi = ZLR[k, 0, 24 * h : 24 * h + 24], ZLR[k, 1, 24 * h : 24 * h + 24]
            for s in range(12):
                p = 12 * h + s
                v = jnp.where(lane24 < 96, roll(hi, 60 - 8 * s, 1), roll(lo, 124 - 8 * s, 1))
                g1[p, 4:28] = jnp.where(lane24 < 64, g1[p, 4:28], v)
        lo, hi = ZLR[k, 0, 48:64], ZLR[k, 1, 48:64]
        for p in range(16):
            v = jnp.where(lane16 < 96, roll(hi, 28 - 8 * p, 1), roll(lo, 124 - 8 * p, 1))
            g2[p, 4:20] = jnp.where(lane16 < 32, g2[p, 4:20], v)
        sweeps12(g2, SA2, SB2, 8, m2)
        sweeps12(g1, SA1, SB1, 16, m1)
        c2 = [SA2[p, 4:20] * F32(16.0 / 9.0) + ZP2[(p - 2) // 2] for p in range(3, 13)]
        t2 = dotx(jnp.concatenate(c2, axis=0), pring)
        for i in range(10):
            double_rows(ZP1.at[i], t2[16 * i : 16 * i + 16])
        c1 = [SA1[p, 4:28] * F32(4.0 / 9.0) + ZP1[(p - 2) // 2, 4:28] for p in range(3, 21)]
        t1 = dotx(jnp.concatenate(c1, axis=0), p0)
        for i in range(18):
            double_rows(ZP0.at[i], t1[24 * i : 24 * i + 24, 0:128])
            double_rows(ZPO.at[i], t1[24 * i : 24 * i + 24, 128:256])
        for c, _, r in zs:
            recv(c, r)
        for q in range(4):
            own = ZC[k, q]
            SLA[0, q, 4:44] = jnp.where(slot_low, ZCR[k, 0, q], own)
            SHA[0, q, 4:44] = jnp.where(slot_low, own, ZCR[k, 1, q])
        for a, b, m in ((SLA, SLB, ms_lo), (SHA, SHB, ms_hi)):
            sweep_slab(a.at[0], a.at[1], a.at[0], m)
            sweep_slab(a.at[1], b, a.at[0], m)
            sweep_slab(b, a.at[1], a.at[0], m)
        edge40 = (lane40 < 3) | (lane40 >= 125)
        merged = [jnp.where(slot_low, SHA[1, q, 4:44], SLA[1, q, 4:44]) for q in range(4)]
        for q in range(4):
            SLB[q, 4:44] = merged[q]
            SHB[q, 4:44] = jnp.where(slot_low, SLA[1, q, 4:44], SHA[1, q, 4:44])
        for p in range(3, 37):
            s, q = p // 4, p % 4
            e = roll(SLB[q, 4:44], -(12 * s + 6), 1)
            z = jnp.where(edge40, e, SA0[p, 4:44])
            ZR[p, 4:44] = z * ninth + ZP0[(p - 2) // 2, 4:44]
            if 4 <= p < 36:
                e = roll(SHB[q, 8:40], -(12 * s + 6), 1)
                ZO[p - 4] = e * ninth + ZPO[(p - 2) // 2, 8:40]
        return ar

    precondition(0, None)

    zero8 = jnp.zeros((8, LANES), F32)
    a = b = zero8
    for p in range(32):
        z, w = apply_plane(p)
        Z0[p] = z
        G0[1, p + 4, 8:40] = w
        a = a + fold(G0[0, p + 4, 8:40] * z)
        b = b + fold(z * w)
    ar = all_reduce_start(dots_tile(a, b), 0)
    ar = precondition(1, ar)
    alpha = all_reduce_end(ar, 0)
    keep_u.wait()

    a = b = zero8
    for p in range(32):
        y, v = apply_plane(p)
        z = Z0[p]
        w = G0[1, p + 4, 8:40]
        r1 = G0[0, p + 4, 8:40] - alpha * w
        z1 = z - alpha * y
        w1 = w - alpha * v
        sol[p] = U[p] + alpha * z
        res[p] = r1
        Y0[p] = z1
        V[p] = w1
        a = a + fold(r1 * z1)
        b = b + fold(z1 * w1)
    ar = all_reduce_start(dots_tile(a, b), 1)
    send_all(ar)
    ar = all_reduce_next(ar, 1)
    send_all(ar)
    alpha1 = all_reduce_end(ar, 1)

    def last(c, _):
        for i in range(8):
            p = 8 * c + i
            sol[p] = sol[p] + alpha1 * Y0[p]
            res[p] = res[p] - alpha1 * V[p]
        return 0

    lax.fori_loop(0, 4, last, 0)
    for copy, cond in pending:
        if cond is None:
            copy.wait_send()
        else:
            pl.when(cond)(copy.wait_send)


def shards(rhs, u):
    v = lambda *shape: pltpu.VMEM(shape, F32)
    field = v(32, 32, 128)
    scratch = [
        field, field,
        v(40, 48, 128), field,
        v(2, 40, 48, 128), v(2, 24, 32, 128), v(2, 16, 24, 128),
        v(40, 48, 128), v(40, 48, 128),
        v(24, 32, 128), v(24, 32, 128), v(16, 24, 128), v(16, 24, 128),
        field, field, field,
        v(16, 16, 128), v(8, 16, 128),
        v(2, 2, 21, 8, 128), v(2, 2, 21, 8, 128), v(2, 4, 4, 8, 128), v(2, 4, 4, 8, 128),
        v(2, 4, 40, 128), v(2, 2, 4, 40, 128),
        v(2, 64, 128), v(2, 2, 64, 128),
        v(2, 4, 48, 128), v(4, 48, 128), v(2, 4, 48, 128), v(4, 48, 128),
        v(4, 32, 128), v(4, 32, 128),
        v(2, 3, 16, 2, 128), v(8, 128),
        v(18, 32, 128), v(18, 32, 128), v(18, 32, 128), v(18, 32, 128),
        v(10, 24, 128), v(10, 24, 128), v(10, 24, 128),
        v(6, 24, 128), v(6, 24, 128), v(6, 24, 128),
        v(18, 48, 128), v(18, 48, 128), v(10, 32, 128), v(6, 16, 128), v(8, 16, 128), v(4, 16, 128),
        v(2, 8, 8, 128), v(2, 16, 8, 128),
        pltpu.SemaphoreType.DMA((NSEM,)), pltpu.SemaphoreType.DMA((NSEM,)), pltpu.SemaphoreType.DMA((3,)),
    ]
    block = jax.ShapeDtypeStruct((32, 32, 128), F32)
    return pl.pallas_call(
        kernel,
        out_shape=(block, block),
        in_specs=[pl.BlockSpec(memory_space=pl.ANY)] * 2,
        out_specs=[pl.BlockSpec(memory_space=pltpu.VMEM)] * 2,
        scratch_shapes=scratch,
        compiler_params=pltpu.CompilerParams(
            collective_id=0, has_side_effects=True, vmem_limit_bytes=56 * 2**20
        ),
    )(rhs, u)


def solution(mesh):
    spec = P("gx", "gy", "gz")
    return jax.shard_map(
        shards, mesh=mesh, in_specs=(spec, spec), out_specs=(spec, spec), check_vma=False
    )
```

```python
import functools

import jax
import jax.numpy as jnp
from jax import lax
from jax.experimental import pallas as pl
from jax.experimental.pallas import tpu as pltpu
from jax.sharding import PartitionSpec as P

F32 = jnp.float32
BF16 = jnp.bfloat16
MESH = pl.DeviceIdType.MESH
NGX, NGY, NGZ = 4, 4, 8
LANES = 128

S_SET = 6
O_X, O_Y, O_D, O_Z, O_ZL, O_C3, O_ARA, O_ARB = 0, 6, 10, 14, 16, 18, 66, 74
SET = 90
NSEM = S_SET + 2 * SET


def roll(v, shift, axis):
    n = v.shape[axis]
    shift = shift % n
    return v if shift == 0 else pltpu.roll(v, shift, axis)


def iota(shape, axis):
    return lax.broadcasted_iota(jnp.int32, shape, axis)


def dotx(x, m):
    hi = x.astype(BF16)
    rest = x - hi.astype(F32)
    mid = rest.astype(BF16)
    low = (rest - mid.astype(F32)).astype(BF16)
    n = x.shape[0]
    y = jnp.dot(jnp.concatenate([hi, mid, low], axis=0), m, preferred_element_type=F32)
    return y[0:n] + y[n : 2 * n] + y[2 * n : 3 * n]


def kernel(
    rhs_hbm, u_hbm, sol, res,
    RHS, U, ZR, ZO, G0, G1, G2, SA0, SB0, SA1, SB1, SA2, SB2, V, Z0, Y0,
    Q1, Q2, YS, YR, DS, DR, XS, XR, ZC, ZCS, ZCR, ZL, ZLR, SLA, SLB, SHA, SHB, R1S, R1R, C3, T3,
    G3, SA3, SB3, C3P, G4, SA4, SB4, G5, SA5, SB5,
    ZP0, ZPO, ZP1, ZP2, ZP3, ZP4, ARA, ARB, ss, rs, ls,
):
    gx, gy, gz = lax.axis_index("gx"), lax.axis_index("gy"), lax.axis_index("gz")
    x_up, x_dn = gx < NGX - 1, gx > 0
    y_up, y_dn = gy < NGY - 1, gy > 0
    z_up, z_dn = gz < NGZ - 1, gz > 0
    one = lambda c: jnp.where(c, F32(1.0), F32(0.0))
    fxu, fxd, fyu, fyd, fzu, fzd = map(one, (x_up, x_dn, y_up, y_dn, z_up, z_dn))
    gxu, gxd = lax.rem(gx + 1, NGX), lax.rem(gx + NGX - 1, NGX)
    gyu, gyd = lax.rem(gy + 1, NGY), lax.rem(gy + NGY - 1, NGY)
    gzu, gzd = lax.rem(gz + 1, NGZ), lax.rem(gz + NGZ - 1, NGZ)
    gx_core = gx + 1 - 2 * lax.rem(gx, 2)
    gx_far = lax.rem(gx + 2, NGX)

    pending = []

    def rcopy(src, dst, i, dev):
        return pltpu.make_async_remote_copy(
            src_ref=src, dst_ref=dst, send_sem=ss.at[i], recv_sem=rs.at[i],
            device_id=dev, device_id_type=MESH,
        )

    def send(copy, cond=None):
        if cond is None:
            copy.start()
        else:
            pl.when(cond)(lambda: copy.start())
        pending.append((copy, cond))

    def sent(copy, cond):
        pending[:] = [q for q in pending if q[0] is not copy]
        pl.when(cond)(copy.wait_send)

    def recv(copy, cond=None):
        if cond is None:
            copy.wait_recv()
        else:
            pl.when(cond)(lambda: copy.wait_recv())

    def send_all(copies):
        for c in copies:
            send(c)

    inner = (pl.ds(4, 32), pl.ds(8, 32))
    get_u = pltpu.make_async_copy(u_hbm, ZR.at[inner], ls.at[0])
    get_rhs = pltpu.make_async_copy(rhs_hbm, RHS, ls.at[1])
    keep_u = pltpu.make_async_copy(u_hbm, U, ls.at[2])
    get_u.start()
    get_rhs.start()
    keep_u.start()

    ZR[3] = jnp.zeros((48, LANES), F32)
    ZR[36] = jnp.zeros((48, LANES), F32)
    R1R[...] = jnp.zeros_like(R1R)
    bar = pltpu.get_barrier_semaphore()
    peers = 0
    for dx in range(NGX):
        for dy in range(NGY):
            if dx or dy:
                peers += 1
                pl.semaphore_signal(
                    bar, inc=1, device_id_type=MESH,
                    device_id={"gx": lax.rem(gx + dx, NGX), "gy": lax.rem(gy + dy, NGY)},
                )
    for dz in range(1, NGZ):
        if dz in (1, NGZ - 1):
            others = [(lax.rem(gx + dx, NGX), lax.rem(gy + dy, NGY)) for dx in range(NGX) for dy in range(NGY)]
        else:
            others = [(gx, gy), (gx_far, gy)]
        for ox, oy in others:
            peers += 1
            pl.semaphore_signal(
                bar, inc=1, device_id_type=MESH, device_id={"gx": ox, "gy": oy, "gz": lax.rem(gz + dz, NGZ)}
            )
    get_u.wait()

    lane8 = iota((8, LANES), 1)
    row8 = iota((8, LANES), 0)
    lane32 = iota((32, LANES), 1)
    lane40 = iota((40, LANES), 1)

    diagonals = []
    for up_x in (True, False):
        for up_y in (True, False):
            diagonals.append((
                {"gx": gxu if up_x else gxd, "gy": gyu if up_y else gyd},
                (x_up if up_x else x_dn) & (y_up if up_y else y_dn),
                (x_dn if up_x else x_up) & (y_dn if up_y else y_up),
            ))

    r1x = [
        rcopy(ZR.at[pl.ds(35, 1), pl.ds(8, 32)], ZR.at[pl.ds(3, 1), pl.ds(8, 32)], 0, {"gx": gxu}),
        rcopy(ZR.at[pl.ds(4, 1), pl.ds(8, 32)], ZR.at[pl.ds(36, 1), pl.ds(8, 32)], 1, {"gx": gxd}),
    ]
    devs = [{"gy": gyu}, {"gy": gyd}, {"gz": gzu}, {"gz": gzd}]
    conds = [y_up, y_dn, z_up, z_dn]
    backs = [y_dn, y_up, z_dn, z_up]
    r1 = [rcopy(R1S.at[min(i, 2)], R1R.at[i], 2 + i, devs[i]) for i in range(4)]
    zz = jnp.zeros((32, LANES), F32)
    for p in range(32):
        zz = jnp.where(lane32 >> 1 == p, roll(ZR[p + 4, 8:40], 2 * p + 1, 1), zz)
    R1S[2] = zz
    for p in range(32):
        R1S[0, p : p + 1, :] = ZR[p + 4, 39:40, :]
        R1S[1, p : p + 1, :] = ZR[p + 4, 8:9, :]
    pl.semaphore_wait(bar, peers)
    send(r1[2], conds[2])
    send(r1[3], conds[3])
    send(r1x[0], x_up)
    send(r1x[1], x_dn)
    send(r1[0], conds[0])
    send(r1[1], conds[1])

    for k in range(2):
        def clear(*refs):
            def run():
                for ref in refs:
                    ref[...] = jnp.zeros_like(ref)

            return run

        pl.when(jnp.logical_not(x_dn))(clear(G0.at[k, pl.ds(0, 4)], XR.at[k, 0]))
        pl.when(jnp.logical_not(x_up))(clear(G0.at[k, pl.ds(36, 4)], XR.at[k, 1]))
        pl.when(jnp.logical_not(y_dn))(clear(YR.at[k, 0]))
        pl.when(jnp.logical_not(y_up))(clear(YR.at[k, 1]))
        pl.when(jnp.logical_not(z_dn))(clear(ZCR.at[k, 0], ZLR.at[k, 0], C3.at[k, 1]))
        pl.when(jnp.logical_not(z_up))(clear(ZCR.at[k, 1], ZLR.at[k, 1], C3.at[k, 2]))
        for d, (_, _, from_there) in enumerate(diagonals):
            pl.when(jnp.logical_not(from_there))(clear(DR.at[k, d]))
    for ref in (G3, SA3, SB3, C3P, G4, SA4, SB4, G5, SA5, SB5, Q2):
        ref[...] = jnp.zeros_like(ref)
    kk, jj = iota((LANES, LANES), 0), iota((LANES, LANES), 1)

    def const(cond, value):
        return jnp.where(cond, F32(value), F32(0.0)).astype(BF16)

    rz1 = const((kk >> 1) == (jj & 63), 0.5)
    rz2 = const((kk >> 2) == (jj & 31), 0.25)
    rz3 = jnp.concatenate([const((kk >> 3) + 16 * i == jj, 0.125) for i in range(4)], axis=0)
    ring_k = jnp.where(kk < 96, kk >> 1, (kk >> 1) + 64)
    ring_j = jnp.where(jj < 96, jj >> 1, (jj >> 1) + 64)
    rring = const(ring_k == jj, 0.5)
    pring = const(ring_j == kk, 1.0)
    p0 = jnp.concatenate([const((jj >> 1) == kk, 1.0), const((jj >> 1) + 64 == kk, 1.0)], axis=1)

    ninth = F32(1.0 / 9.0)

    def mask9(rows, lo_rows, hi_rows, lanes_in):
        row, lane = iota((rows, LANES), 0), iota((rows, LANES), 1)
        my = jnp.where(row < lo_rows, fyd, jnp.where(row < hi_rows, F32(1.0), fyu))
        mz = jnp.where(lane < lanes_in, F32(1.0), jnp.where(lane < 96, fzu, fzd))
        return my * mz * ninth

    get_rhs.wait()
    recv(r1x[0], x_dn)
    recv(r1x[1], x_up)
    for i in range(4):
        recv(r1[i], backs[i])
    for c, cond in zip(r1x, (x_up, x_dn)):
        sent(c, cond)
    faces = jnp.where((lane32 & 1) == 0, R1R[2], R1R[3])
    for p in range(32):
        ZR[p + 4, 7:8, :] = R1R[0, p : p + 1, :]
        ZR[p + 4, 40:41, :] = R1R[1, p : p + 1, :]
        ZO[p] = roll(faces, -(2 * p + 1), 1)

    def apply_plane(p):
        c = ZR[p + 4, 8:40]
        o = ZO[p]
        left = roll(jnp.where(lane32 == 127, o, c), 1, 1)
        right = roll(jnp.where(lane32 == 0, o, c), -1, 1)
        ysum = ZR[p + 4, 7:39] + ZR[p + 4, 9:41]
        xsum = ZR[p + 3, 8:40] + ZR[p + 5, 8:40]
        return c, 6.0 * c - ((xsum + ysum) + (left + right))

    for p in range(32):
        _, a = apply_plane(p)
        G0[0, p + 4, 8:40] = RHS[p] - a

    m0 = mask9(40, 4, 36, 128)
    m1 = mask9(24, 4, 20, 64)
    m2 = mask9(16, 4, 12, 32)
    m3 = mask9(16, 0, 16, 16)
    m4 = mask9(8, 0, 8, 8)
    m5 = jnp.where(row8 < 4, mask9(8, 0, 8, 4), F32(0.0))
    slot_lane = lane40 - 12 * sum((lane40 >= 12 * i).astype(jnp.int32) for i in range(1, 11))
    slot_low = slot_lane < 6
    my0 = jnp.where(lane40 < 12, fxd, jnp.where(lane40 < 108, F32(1.0), fxu)) * m0
    ms_lo = my0 * jnp.where(slot_low, fzd, F32(1.0))
    ms_hi = my0 * jnp.where(slot_low, F32(1.0), fzu)

    def stencil_sum(v, up_row, dn_row, prev, nxt):
        return ((up_row + dn_row) + (prev + nxt)) + (roll(v, 1, 1) + roll(v, -1, 1))

    def sweep_plane(src, dst, g, p, r0, r1, m):
        v = src[p, r0:r1]
        n = stencil_sum(v, src[p, r0 - 1 : r1 - 1], src[p, r0 + 1 : r1 + 1], src[p - 1, r0:r1], src[p + 1, r0:r1])
        dst[p, r0:r1] = m * (3.0 * v + n) + g[p, r0:r1]

    def sweep0(src, dst, g, j):
        for p in range(j, 4):
            sweep_plane(src, dst, g, p, 4, 44, m0 * fxd)

        for p in range(4, 36):
            sweep_plane(src, dst, g, p, 4, 44, m0)
        for p in range(36, 40 - j):
            sweep_plane(src, dst, g, p, 4, 44, m0 * fxu)

    def sweeps12(g, sa, sb, n, m):
        lo, hi = m * fxd, m * fxu
        for j, (src, dst) in enumerate(((g, sa), (sa, sb), (sb, sa)), 1):
            for p in range(j, n + 8 - j):
                sweep_plane(src, dst, g, p, 4, 12 + n, lo if p < 4 else m if p < n + 4 else hi)

    def sweeps_small(g, sa, sb, n, rows, m):
        for src, dst in ((g, sa), (sa, sb), (sb, sa)):
            for p in range(1, n + 1):
                sweep_plane(src, dst, g, p, 8, 8 + rows, m)
        return sa

    def sweep_slab(src, dst, g, m):
        for q in range(4):
            v = src[q, 4:44]
            prev = src[q - 1, 4:44] if q else roll(src[3, 4:44], 12, 1)
            nxt = src[q + 1, 4:44] if q < 3 else roll(src[0, 4:44], -12, 1)
            n = stencil_sum(v, src[q, 3:43], src[q, 5:45], prev, nxt)
            dst[q, 4:44] = m * (3.0 * v + n) + g[q, 4:44]

    def pair_mean(a, b, first_row, rows):
        even, odd = pl.ds(first_row, rows, stride=2), pl.ds(first_row + 1, rows, stride=2)
        return 0.25 * ((a[even, :] + a[odd, :]) + (b[even, :] + b[odd, :]))

    def double_rows(dst, v):
        n = v.shape[0]
        dst[pl.ds(0, n, stride=2), :] = v
        dst[pl.ds(1, n, stride=2), :] = v

    def all_reduce_start(tile, k):
        o = S_SET + SET * k
        mine = lax.rem(gx, 2) * NGY + gy
        ARA[k, mine] = tile
        copies = []
        for dc in range(2):
            for dy in range(NGY):
                if dc or dy:
                    dev = {"gx": gx_core if dc else gx, "gy": lax.rem(gy + dy, NGY)}
                    copies.append(rcopy(ARA.at[k, mine], ARA.at[k, mine], o + O_ARA + dc * NGY + dy, dev))
        return copies

    def total(ref, k, n):
        t = [ref[k, i] for i in range(n)]
        while len(t) > 1:
            t = [t[i] + t[i + 1] for i in range(0, len(t), 2)]
        return t[0]

    def all_reduce_next(copies, k):
        o = S_SET + SET * k
        for c in copies:
            recv(c)
        mine = (gx >> 1) * NGZ + gz
        ARB[k, mine] = total(ARA, k, 8)
        out = []
        for far in range(2):
            for dz in range(NGZ):
                if far or dz:
                    dev = {"gx": gx_far if far else gx, "gz": lax.rem(gz + dz, NGZ)}
                    out.append(rcopy(ARB.at[k, mine], ARB.at[k, mine], o + O_ARB + far * NGZ + dz, dev))
        return out

    def all_reduce_end(copies, k):
        for c in copies:
            recv(c)
        tile = total(ARB, k, 16)
        along = jnp.sum(tile[0:1], axis=1, keepdims=True)
        curve = jnp.sum(tile[1:2], axis=1, keepdims=True)
        return along / curve

    def dots_tile(a, b):
        a = jnp.sum(a, axis=0, keepdims=True)
        b = jnp.sum(b, axis=0, keepdims=True)
        return jnp.where(row8 == 0, a, jnp.where(row8 == 1, b, F32(0.0)))

    def fold(x):
        return (x[0:8] + x[8:16]) + (x[16:24] + x[24:32])

    def precondition(k, ar):
        o = S_SET + SET * k
        g0, g1, g2 = G0.at[k], G1.at[k], G2.at[k]
        if ar is not None:
            send_all(ar)
        for i in range(16):
            Q1[i] = pair_mean(g0.at[2 * i + 4], g0.at[2 * i + 5], 8, 16)
        for i in range(8):
            Q2[i, 0:8] = pair_mean(Q1.at[2 * i], Q1.at[2 * i + 1], 0, 8)
        q3 = jnp.concatenate([pair_mean(Q2.at[2 * i], Q2.at[2 * i + 1], 0, 8) for i in range(4)], axis=1)
        T3[...] = dotx(q3, rz3)
        t3 = jnp.where(lane40[0:4] < 64, T3[pl.ds(0, 4, stride=2), :], roll(T3[pl.ds(1, 4, stride=2), :], 64, 1))
        mine = gx * NGY + gy
        C3[k, 0, mine] = t3[0:2]
        c3 = []
        for dz, dev_z, s, r in ((0, gz, None, None), (1, gzu, z_up, z_dn), (2, gzd, z_dn, z_up)):
            for dx in range(NGX):
                for dy in range(NGY):
                    if dz or dx or dy:
                        c3.append((rcopy(
                            C3.at[k, 0, mine], C3.at[k, dz, mine], o + O_C3 + 16 * dz + dx * NGY + dy,
                            {"gx": lax.rem(gx + dx, NGX), "gy": lax.rem(gy + dy, NGY), "gz": dev_z},
                        ), s, r))
        for c, s, _ in c3:
            send(c, s)
        g2[4:12, 8:16] = dotx(Q2[:, 0:8].reshape(64, LANES), rz2).reshape(8, 8, LANES)
        g1[4:20, 8:24] = dotx(Q1[...].reshape(256, LANES), rz1).reshape(16, 16, LANES)
        xs = [
            (rcopy(g0.at[pl.ds(32, 4), pl.ds(8, 32)], g0.at[pl.ds(0, 4), pl.ds(8, 32)], o + O_X + 0, {"gx": gxu}), x_up, x_dn),
            (rcopy(g0.at[pl.ds(4, 4), pl.ds(8, 32)], g0.at[pl.ds(36, 4), pl.ds(8, 32)], o + O_X + 1, {"gx": gxd}), x_dn, x_up),
        ]
        lane4 = iota((1, 4, LANES), 2)
        quarter = [lane4 < 32, lane4 < 64, lane4 < 96]

        def four(v):
            return jnp.where(quarter[1], jnp.where(quarter[0], v[0], v[1]), jnp.where(quarter[2], v[2], v[3]))

        ys, ds = [], []
        for d in range(2):
            r0, r1, r2 = (36, 20, 12) if d == 0 else (8, 8, 8)
            for h in range(2):
                rows = pl.ds(4 * h, 4)
                YS[k, d, 0:16, rows] = g0[4 + 16 * h : 20 + 16 * h, r0 : r0 + 4]
                a, b = g1[4 + 4 * h : 8 + 4 * h, r1 : r1 + 4], g1[12 + 4 * h : 16 + 4 * h, r1 : r1 + 4]
                YS[k, d, 16:20, rows] = jnp.where(quarter[1], a, b)
                YS[k, d, 20:21, rows] = four([g2[4 + 2 * i + h : 5 + 2 * i + h, r2 : r2 + 4] for i in range(4)])
            dev, s, r = (({"gy": gyu}, y_up, y_dn), ({"gy": gyd}, y_dn, y_up))[d]
            ys.append((rcopy(YS.at[k, d], YR.at[k, d], o + O_Y + d, dev), s, r))
        for d, (dev, s, r) in enumerate(diagonals):
            up_x, up_y = d < 2, d % 2 == 0
            p0_, p1, p2 = (32, 16, 8) if up_x else (4, 4, 4)
            r0, r1, r2 = (36, 20, 12) if up_y else (8, 8, 8)
            for h in range(2):
                rows = pl.ds(4 * h, 4)
                DS[k, d, 0:2, rows] = g0[p0_ + 2 * h : p0_ + 2 * h + 2, r0 : r0 + 4]
                a, b = g1[p1 + h : p1 + h + 1, r1 : r1 + 4], g1[p1 + 2 + h : p1 + 3 + h, r1 : r1 + 4]
                DS[k, d, 2:3, rows] = jnp.where(quarter[1], a, b)
                DS[k, d, 3:4, rows] = four([g2[p2 + i : p2 + i + 1, r2 : r2 + 4] for i in range(4)])
            ds.append((rcopy(DS.at[k, d], DR.at[k, d], o + O_D + d, dev), s, r))
        lane16 = iota((16, LANES), 1)
        eighth = [lane8 < 32, lane8 < 64, lane8 < 96]
        more = []
        for d in range(2):
            p1, p2 = (16, 8) if d == 0 else (4, 4)
            for h in range(2):
                XS[k, d, 16 * h : 16 * h + 16] = jnp.where(lane16 < 64, g1[p1 + h, 8:24], g1[p1 + 2 + h, 8:24])
            v = [g2[p2 + i, 8:16] for i in range(4)]
            XS[k, d, 32:40] = jnp.where(eighth[1], jnp.where(eighth[0], v[0], v[1]), jnp.where(eighth[2], v[2], v[3]))
            dev, s, r = (({"gx": gxu}, x_up, x_dn), ({"gx": gxd}, x_dn, x_up))[d]
            more.append((rcopy(XS.at[k, d], XR.at[k, d], o + O_X + 2 + d, dev), s, r))
        for c, s, _ in ds + ys + xs + more:
            send(c, s)
        if ar is not None:
            ar = all_reduce_next(ar, 0)
            send_all(ar)
        for c, _, r in xs + more + ys + ds:
            recv(c, r)
        for d in range(2):
            p1, p2 = (0, 0) if d == 0 else (20, 12)
            for h in range(2):
                v = XR[k, d, 16 * h : 16 * h + 16]
                w = roll(v, 64, 1)
                g1[p1 + h, 8:24] = jnp.where(lane16 < 64, v, w)
                g1[p1 + 2 + h, 8:24] = jnp.where(lane16 < 64, w, v)
            v = XR[k, d, 32:40]
            w = [roll(v, 32 * i, 1) for i in range(4)]
            for i in range(4):
                g2[p2 + i, 8:16] = jnp.where(eighth[0], w[(4 - i) % 4], w[(5 - i) % 4])
        for d in range(2):
            r0, r1, r2 = (4, 4, 4) if d == 0 else (40, 24, 16)
            for h in range(2):
                rows = pl.ds(4 * h, 4)
                g0[4 + 16 * h : 20 + 16 * h, r0 : r0 + 4] = YR[k, d, 0:16, rows]
                v = YR[k, d, 16:20, rows]
                w = roll(v, 64, 2)
                g1[4 + 4 * h : 8 + 4 * h, r1 : r1 + 4] = jnp.where(quarter[1], v, w)
                g1[12 + 4 * h : 16 + 4 * h, r1 : r1 + 4] = jnp.where(quarter[1], w, v)
                v = YR[k, d, 20:21, rows]
                w = [roll(v, 32 * i, 2) for i in range(4)]
                for i in range(4):
                    g2[4 + 2 * i + h : 5 + 2 * i + h, r2 : r2 + 4] = jnp.where(quarter[0], w[(4 - i) % 4], w[(5 - i) % 4])
        for d in range(4):
            up_x, up_y = d < 2, d % 2 == 0
            p0_, p1, p2 = (0, 0, 0) if up_x else (36, 20, 12)
            r0, r1, r2 = (4, 4, 4) if up_y else (40, 24, 16)
            for h in range(2):
                rows = pl.ds(4 * h, 4)
                g0[p0_ + 2 * h : p0_ + 2 * h + 2, r0 : r0 + 4] = DR[k, d, 0:2, rows]
                v = DR[k, d, 2:3, rows]
                w = roll(v, 64, 2)
                g1[p1 + h : p1 + h + 1, r1 : r1 + 4] = jnp.where(quarter[1], v, w)
                g1[p1 + 2 + h : p1 + 3 + h, r1 : r1 + 4] = jnp.where(quarter[1], w, v)
            v = DR[k, d, 3:4, 0:4]
            w = [roll(v, 32 * i, 2) for i in range(4)]
            for i in range(4):
                g2[p2 + i : p2 + i + 1, r2 : r2 + 4] = jnp.where(quarter[0], w[(4 - i) % 4], w[(5 - i) % 4])
        half_slots = []
        for h in range(2):
            acc = jnp.zeros((24, LANES), F32)
            for s in range(12):
                acc = jnp.where(lane40[0:24] >> 3 == s, roll(g1[12 * h + s, 4:28], 8 * s - 60, 1), acc)
            half_slots.append(acc)
        acc = jnp.zeros((16, LANES), F32)
        for s in range(16):
            acc = jnp.where(lane40[0:16] >> 3 == s, roll(g2[s, 4:20], 8 * s - 28, 1), acc)
        half_slots += [acc[0:8], acc[8:16]]
        for i, n in ((0, 24), (2, 8)):
            a, b = half_slots[i : i + 2]
            first_four = (lane40[0:n] & 4) == 0
            rows = pl.ds(12 * i, n)
            ZL[k, 0, rows] = jnp.where(first_four, a, roll(b, 4, 1))
            ZL[k, 1, rows] = jnp.where(first_four, roll(a, -4, 1), b)
        zl = [
            (rcopy(ZL.at[k, 0], ZLR.at[k, 0], o + O_ZL + 0, {"gz": gzu}), z_up, z_dn),
            (rcopy(ZL.at[k, 1], ZLR.at[k, 1], o + O_ZL + 1, {"gz": gzd}), z_dn, z_up),
        ]
        for c, s, _ in zl:
            send(c, s)
        for q in range(4):
            acc = jnp.zeros((40, LANES), F32)
            for s in range(10):
                in_slot = (lane40 >= 12 * s) & (lane40 < 12 * s + 12)
                acc = jnp.where(in_slot, roll(g0[4 * s + q, 4:44], 12 * s + 6, 1), acc)
            ZC[k, q] = acc
        for i in range(2):
            a, b = ZC[k, 2 * i], ZC[k, 2 * i + 1]
            ZCS[k, 0, i] = jnp.where(slot_low, a, roll(b, 6, 1))
            ZCS[k, 1, i] = jnp.where(slot_low, roll(a, -6, 1), b)
        zs = [
            (rcopy(ZCS.at[k, 0], ZCR.at[k, 0], o + O_Z + 0, {"gz": gzu}), z_up, z_dn),
            (rcopy(ZCS.at[k, 1], ZCR.at[k, 1], o + O_Z + 1, {"gz": gzd}), z_dn, z_up),
        ]
        for c, s, _ in zs:
            send(c, s)
        sweep0(g0, SA0, g0, 1)
        sweep0(SA0, SB0, g0, 2)
        sweep0(SB0, SA0, g0, 3)
        for c, _, r in c3:
            recv(c, r)
        for g in range(4):
            own, lo, hi = (jnp.concatenate([C3[k, i, 4 * g + j] for j in range(4)], axis=0) for i in range(3))
            for px in range(4):
                for odd in range(2):
                    off = 16 * px + 64 * odd
                    v = jnp.where(lane8 < 32, roll(hi, 16 - off, 1), roll(lo, 112 - off, 1))
                    v = jnp.where(lane8 < 16, roll(own, -off, 1), v)
                    G3.at[4 * g + px + 1][pl.ds(8 + odd, 8, stride=2), :] = v
        q = jnp.concatenate([pair_mean(G3.at[2 * i + 1], G3.at[2 * i + 2], 8, 8) for i in range(8)], axis=0)
        q = dotx(q, rring)
        for i in range(8):
            G4[i + 1, 8:16] = q[8 * i : 8 * i + 8]
        q = jnp.concatenate([pair_mean(G4.at[2 * i + 1], G4.at[2 * i + 2], 8, 8) for i in range(4)], axis=0)
        q = dotx(q, rring)
        for i in range(4):
            G5[i + 1, 8:16] = jnp.where(row8 < 4, q[8 * i : 8 * i + 8], F32(0.0))
        s5 = sweeps_small(G5, SA5, SB5, 4, 8, m5)
        s4 = sweeps_small(G4, SA4, SB4, 8, 8, m4)
        s3 = sweeps_small(G3, SA3, SB3, 16, 16, m3)
        t5 = dotx(jnp.concatenate([s5[i + 1, 8:16] for i in range(4)], axis=0) * F32(4.0**5 / 9.0), pring)
        for i in range(4):
            double_rows(ZP4.at[i], t5[8 * i : 8 * i + 8])
        c4 = jnp.concatenate([s4[i + 1, 8:16] * F32(4.0**4 / 9.0) + ZP4[i // 2, 0:8] for i in range(8)], axis=0)
        t4 = dotx(c4, pring)
        for i in range(8):
            double_rows(ZP3.at[i], t4[8 * i : 8 * i + 8])
        for i in range(16):
            C3P[i + 1, 8:24] = s3[i + 1, 8:24] * F32(4.0**3 / 9.0) + ZP3[i // 2]
        start = 8 + 4 * gy - 2
        c3l = [C3P[4 * gx + i, pl.ds(start, 8), :] for i in range(6)]
        t3 = dotx(jnp.concatenate(c3l, axis=0), pring)
        for i in range(6):
            double_rows(ZP2.at[i], t3[8 * i : 8 * i + 8])
        for c, _, r in zl:
            recv(c, r)
        lane24, lane16 = lane40[0:24], lane40[0:16]
        lo, hi = ZLR[k, 0, 0:24], ZLR[k, 1, 0:24]
        for p in range(24):
            at = 8 * (p % 12) + 4 * (p // 12)
            v = jnp.where(lane24 < 96, roll(hi, 64 - at, 1), roll(lo, 124 - at, 1))
            g1[p, 4:28] = jnp.where(lane24 < 64, g1[p, 4:28], v)
        lo = jnp.concatenate([ZLR[k, 0, 24:32], roll(ZLR[k, 0, 24:32], -4, 1)], axis=0)
        hi = jnp.concatenate([ZLR[k, 1, 24:32], roll(ZLR[k, 1, 24:32], -4, 1)], axis=0)
        for p in range(16):
            v = jnp.where(lane16 < 96, roll(hi, 32 - 8 * p, 1), roll(lo, 124 - 8 * p, 1))
            g2[p, 4:20] = jnp.where(lane16 < 32, g2[p, 4:20], v)
        sweeps12(g2, SA2, SB2, 8, m2)
        sweeps12(g1, SA1, SB1, 16, m1)
        c2 = [SA2[p, 4:20] * F32(16.0 / 9.0) + ZP2[(p - 2) // 2] for p in range(3, 13)]
        t2 = dotx(jnp.concatenate(c2, axis=0), pring)
        for i in range(10):
            double_rows(ZP1.at[i], t2[16 * i : 16 * i + 16])
        c1 = [SA1[p, 4:28] * F32(4.0 / 9.0) + ZP1[(p - 2) // 2, 4:28] for p in range(3, 21)]
        t1 = dotx(jnp.concatenate(c1, axis=0), p0)
        for i in range(18):
            double_rows(ZP0.at[i], t1[24 * i : 24 * i + 24, 0:128])
            double_rows(ZPO.at[i], t1[24 * i : 24 * i + 24, 128:256])
        for c, _, r in zs:
            recv(c, r)
        for i in range(2):
            below, above = ZCR[k, 0, i], ZCR[k, 1, i]
            a, b = ZC[k, 2 * i], ZC[k, 2 * i + 1]
            SLA[0, 2 * i, 4:44] = jnp.where(slot_low, below, a)
            SLA[0, 2 * i + 1, 4:44] = jnp.where(slot_low, roll(below, -6, 1), b)
            SHA[0, 2 * i, 4:44] = jnp.where(slot_low, a, roll(above, 6, 1))
            SHA[0, 2 * i + 1, 4:44] = jnp.where(slot_low, b, above)
        for a, b, m in ((SLA, SLB, ms_lo), (SHA, SHB, ms_hi)):
            sweep_slab(a.at[0], a.at[1], a.at[0], m)
            sweep_slab(a.at[1], b, a.at[0], m)
            sweep_slab(b, a.at[1], a.at[0], m)
        edge40 = (lane40 < 3) | (lane40 >= 125)
        merged = [jnp.where(slot_low, SHA[1, q, 4:44], SLA[1, q, 4:44]) for q in range(4)]
        for q in range(4):
            SLB[q, 4:44] = merged[q]
            SHB[q, 4:44] = jnp.where(slot_low, SLA[1, q, 4:44], SHA[1, q, 4:44])
        for p in range(3, 37):
            s, q = p // 4, p % 4
            e = roll(SLB[q, 4:44], -(12 * s + 6), 1)
            z = jnp.where(edge40, e, SA0[p, 4:44])
            ZR[p, 4:44] = z * ninth + ZP0[(p - 2) // 2, 4:44]
            if 4 <= p < 36:
                e = roll(SHB[q, 8:40], -(12 * s + 6), 1)
                ZO[p - 4] = e * ninth + ZPO[(p - 2) // 2, 8:40]
        return ar

    precondition(0, None)

    zero8 = jnp.zeros((8, LANES), F32)
    a = b = zero8
    for p in range(32):
        z, w = apply_plane(p)
        Z0[p] = z
        G0[1, p + 4, 8:40] = w
        a = a + fold(G0[0, p + 4, 8:40] * z)
        b = b + fold(z * w)
    ar = all_reduce_start(dots_tile(a, b), 0)
    ar = precondition(1, ar)
    alpha = all_reduce_end(ar, 0)
    keep_u.wait()

    a = b = zero8
    for p in range(32):
        y, v = apply_plane(p)
        z = Z0[p]
        w = G0[1, p + 4, 8:40]
        r1 = G0[0, p + 4, 8:40] - alpha * w
        z1 = z - alpha * y
        w1 = w - alpha * v
        sol[p] = U[p] + alpha * z
        res[p] = r1
        Y0[p] = z1
        V[p] = w1
        a = a + fold(r1 * z1)
        b = b + fold(z1 * w1)
    ar = all_reduce_start(dots_tile(a, b), 1)
    send_all(ar)
    ar = all_reduce_next(ar, 1)
    send_all(ar)
    alpha1 = all_reduce_end(ar, 1)

    def last(c, _):
        for i in range(8):
            p = 8 * c + i
            sol[p] = sol[p] + alpha1 * Y0[p]
            res[p] = res[p] - alpha1 * V[p]
        return 0

    lax.fori_loop(0, 4, last, 0)
    for copy, cond in pending:
        if cond is None:
            copy.wait_send()
        else:
            pl.when(cond)(copy.wait_send)


def shards(rhs, u):
    v = lambda *shape: pltpu.VMEM(shape, F32)
    field = v(32, 32, 128)
    scratch = [
        field, field,
        v(40, 48, 128), field,
        v(2, 40, 48, 128), v(2, 24, 32, 128), v(2, 16, 24, 128),
        v(40, 48, 128), v(40, 48, 128),
        v(24, 32, 128), v(24, 32, 128), v(16, 24, 128), v(16, 24, 128),
        field, field, field,
        v(16, 16, 128), v(8, 16, 128),
        v(2, 2, 21, 8, 128), v(2, 2, 21, 8, 128), v(2, 4, 4, 8, 128), v(2, 4, 4, 8, 128), v(2, 2, 40, 128), v(2, 2, 40, 128),
        v(2, 4, 40, 128), v(2, 2, 2, 40, 128), v(2, 2, 2, 40, 128),
        v(2, 2, 32, 128), v(2, 2, 32, 128),
        v(2, 4, 48, 128), v(4, 48, 128), v(2, 4, 48, 128), v(4, 48, 128),
        v(4, 32, 128), v(4, 32, 128),
        v(2, 3, 16, 2, 128), v(8, 128),
        v(18, 32, 128), v(18, 32, 128), v(18, 32, 128), v(18, 32, 128),
        v(10, 24, 128), v(10, 24, 128), v(10, 24, 128),
        v(6, 24, 128), v(6, 24, 128), v(6, 24, 128),
        v(18, 48, 128), v(18, 48, 128), v(10, 32, 128), v(6, 16, 128), v(8, 16, 128), v(4, 16, 128),
        v(2, 8, 8, 128), v(2, 16, 8, 128),
        pltpu.SemaphoreType.DMA((NSEM,)), pltpu.SemaphoreType.DMA((NSEM,)), pltpu.SemaphoreType.DMA((3,)),
    ]
    block = jax.ShapeDtypeStruct((32, 32, 128), F32)
    return pl.pallas_call(
        kernel,
        out_shape=(block, block),
        in_specs=[pl.BlockSpec(memory_space=pltpu.HBM)] * 2,
        out_specs=[pl.BlockSpec(memory_space=pltpu.VMEM)] * 2,
        scratch_shapes=scratch,
        compiler_params=pltpu.CompilerParams(
            collective_id=0, has_side_effects=True, vmem_limit_bytes=24 * 2**20
        ),
    )(pltpu.with_memory_space_constraint(rhs, pltpu.HBM), pltpu.with_memory_space_constraint(u, pltpu.HBM))


def solution(mesh):
    spec = P("gx", "gy", "gz")
    return jax.shard_map(
        shards, mesh=mesh, in_specs=(spec, spec), out_specs=(spec, spec), check_vma=False
    )
```

```python
import functools

import jax
import jax.numpy as jnp
from jax import lax
from jax.experimental import pallas as pl
from jax.experimental.pallas import tpu as pltpu
from jax.sharding import PartitionSpec as P

F32 = jnp.float32
BF16 = jnp.bfloat16
MESH = pl.DeviceIdType.MESH
NGX, NGY, NGZ = 4, 4, 8
LANES = 128

S_SET = 6
O_X, O_Y, O_D, O_Z, O_ZL, O_C3, O_ARA, O_ARB = 0, 6, 10, 14, 16, 18, 66, 74
SET = 90
NSEM = S_SET + 2 * SET


def roll(v, shift, axis):
    n = v.shape[axis]
    shift = shift % n
    return v if shift == 0 else pltpu.roll(v, shift, axis)


def iota(shape, axis):
    return lax.broadcasted_iota(jnp.int32, shape, axis)


def dotx(x, m):
    hi = x.astype(BF16)
    rest = x - hi.astype(F32)
    mid = rest.astype(BF16)
    low = (rest - mid.astype(F32)).astype(BF16)
    n = x.shape[0]
    y = jnp.dot(jnp.concatenate([hi, mid, low], axis=0), m, preferred_element_type=F32)
    return y[0:n] + y[n : 2 * n] + y[2 * n : 3 * n]


def kernel(
    rhs_hbm, u_hbm, sol, res,
    RHS, U, ZR, ZO, G0, G1, G2, SA0, SB0, SA1, SB1, SA2, SB2, V, Z0, Y0,
    Q1, Q2, YS, YR, DS, DR, XS, XR, ZC, ZCS, ZCR, ZL, ZLR, SLA, SLB, SHA, SHB, R1S, R1R, C3, T3,
    G3, SA3, SB3, C3P, G4, SA4, SB4, G5, SA5, SB5,
    ZP0, ZPO, ZP1, ZP2, ZP3, ZP4, ARA, ARB, ss, rs, ls,
):
    gx, gy, gz = lax.axis_index("gx"), lax.axis_index("gy"), lax.axis_index("gz")
    x_up, x_dn = gx < NGX - 1, gx > 0
    y_up, y_dn = gy < NGY - 1, gy > 0
    z_up, z_dn = gz < NGZ - 1, gz > 0
    one = lambda c: jnp.where(c, F32(1.0), F32(0.0))
    fxu, fxd, fyu, fyd, fzu, fzd = map(one, (x_up, x_dn, y_up, y_dn, z_up, z_dn))
    gxu, gxd = lax.rem(gx + 1, NGX), lax.rem(gx + NGX - 1, NGX)
    gyu, gyd = lax.rem(gy + 1, NGY), lax.rem(gy + NGY - 1, NGY)
    gzu, gzd = lax.rem(gz + 1, NGZ), lax.rem(gz + NGZ - 1, NGZ)
    gx_core = gx + 1 - 2 * lax.rem(gx, 2)
    gx_far = lax.rem(gx + 2, NGX)

    pending = []

    def rcopy(src, dst, i, dev):
        return pltpu.make_async_remote_copy(
            src_ref=src, dst_ref=dst, send_sem=ss.at[i], recv_sem=rs.at[i],
            device_id=dev, device_id_type=MESH,
        )

    def send(copy, cond=None):
        if cond is None:
            copy.start()
        else:
            pl.when(cond)(lambda: copy.start())
        pending.append((copy, cond))

    def sent(copy, cond):
        pending[:] = [q for q in pending if q[0] is not copy]
        pl.when(cond)(copy.wait_send)

    def recv(copy, cond=None):
        if cond is None:
            copy.wait_recv()
        else:
            pl.when(cond)(lambda: copy.wait_recv())

    def finish(copies):
        for copy, cond in copies:
            if cond is None:
                copy.wait_send()
            else:
                pl.when(cond)(copy.wait_send)

    def send_all(copies):
        for c in copies:
            send(c)

    inner = (pl.ds(4, 32), pl.ds(8, 32))
    get_u = pltpu.make_async_copy(u_hbm, ZR.at[inner], ls.at[0])
    get_rhs = pltpu.make_async_copy(rhs_hbm, RHS, ls.at[1])
    keep_u = pltpu.make_async_copy(u_hbm, U, ls.at[2])
    get_u.start()
    get_rhs.start()
    keep_u.start()

    ZR[3] = jnp.zeros((48, LANES), F32)
    ZR[36] = jnp.zeros((48, LANES), F32)
    R1R[...] = jnp.zeros_like(R1R)
    bar = pltpu.get_barrier_semaphore()
    greet = [(1, 0, 0), (3, 0, 0), (0, 1, 0), (0, 3, 0), (0, 0, 1), (0, 0, 7)]
    greet += [(dx, dy, dz) for dz in (0, 1, 7) for dx in range(NGX) for dy in range(NGY)]
    greet += [(dx, 0, dz) for dz in range(2, 7) for dx in (0, 2)]
    greet = list(dict.fromkeys(g for g in greet if any(g)))
    near = {
        "gx": [gx, gxu, gx_far, gxd],
        "gy": [gy, gyu, lax.rem(gy + 2, NGY), gyd],
        "gz": [lax.rem(gz + dz, NGZ) for dz in range(NGZ)],
    }
    for dx, dy, dz in greet:
        pl.semaphore_signal(
            bar, inc=1, device_id_type=MESH, device_id={"gx": near["gx"][dx], "gy": near["gy"][dy], "gz": near["gz"][dz]}
        )
    get_u.wait()

    lane8 = iota((8, LANES), 1)
    row8 = iota((8, LANES), 0)
    lane32 = iota((32, LANES), 1)
    lane40 = iota((40, LANES), 1)

    diagonals = []
    for up_x in (True, False):
        for up_y in (True, False):
            diagonals.append((
                {"gx": gxu if up_x else gxd, "gy": gyu if up_y else gyd},
                (x_up if up_x else x_dn) & (y_up if up_y else y_dn),
                (x_dn if up_x else x_up) & (y_dn if up_y else y_up),
            ))

    r1x = [
        rcopy(ZR.at[pl.ds(35, 1), pl.ds(8, 32)], ZR.at[pl.ds(3, 1), pl.ds(8, 32)], 0, {"gx": gxu}),
        rcopy(ZR.at[pl.ds(4, 1), pl.ds(8, 32)], ZR.at[pl.ds(36, 1), pl.ds(8, 32)], 1, {"gx": gxd}),
    ]
    devs = [{"gy": gyu}, {"gy": gyd}, {"gz": gzu}, {"gz": gzd}]
    conds = [y_up, y_dn, z_up, z_dn]
    backs = [y_dn, y_up, z_dn, z_up]
    r1 = [rcopy(R1S.at[min(i, 2)], R1R.at[i], 2 + i, devs[i]) for i in range(4)]
    zz = jnp.zeros((32, LANES), F32)
    for p in range(32):
        zz = jnp.where(lane32 >> 1 == p, roll(ZR[p + 4, 8:40], 2 * p + 1, 1), zz)
    R1S[2] = zz
    for p in range(32):
        R1S[0, p : p + 1, :] = ZR[p + 4, 39:40, :]
        R1S[1, p : p + 1, :] = ZR[p + 4, 8:9, :]
    pl.semaphore_wait(bar, len(greet))
    send(r1[2], conds[2])
    send(r1[3], conds[3])
    send(r1x[0], x_up)
    send(r1x[1], x_dn)
    send(r1[0], conds[0])
    send(r1[1], conds[1])

    for k in range(2):
        def clear(*refs):
            def run():
                for ref in refs:
                    ref[...] = jnp.zeros_like(ref)

            return run

        pl.when(jnp.logical_not(x_dn))(clear(G0.at[k, pl.ds(0, 4)], XR.at[k, 0]))
        pl.when(jnp.logical_not(x_up))(clear(G0.at[k, pl.ds(36, 4)], XR.at[k, 1]))
        pl.when(jnp.logical_not(y_dn))(clear(YR.at[k, 0]))
        pl.when(jnp.logical_not(y_up))(clear(YR.at[k, 1]))
        pl.when(jnp.logical_not(z_dn))(clear(ZCR.at[k, 0], ZLR.at[k, 0], C3.at[k, 1]))
        pl.when(jnp.logical_not(z_up))(clear(ZCR.at[k, 1], ZLR.at[k, 1], C3.at[k, 2]))
        for d, (_, _, from_there) in enumerate(diagonals):
            pl.when(jnp.logical_not(from_there))(clear(DR.at[k, d]))
    for ref in (G3, SA3, SB3, C3P, G4, SA4, SB4, G5, SA5, SB5, Q2):
        ref[...] = jnp.zeros_like(ref)
    kk, jj = iota((LANES, LANES), 0), iota((LANES, LANES), 1)

    def const(cond, value):
        return jnp.where(cond, F32(value), F32(0.0)).astype(BF16)

    rz1 = const((kk >> 1) == (jj & 63), 0.5)
    rz2 = const((kk >> 2) == (jj & 31), 0.25)
    rz3 = jnp.concatenate([const((kk >> 3) + 16 * i == jj, 0.125) for i in range(4)], axis=0)
    ring_k = jnp.where(kk < 96, kk >> 1, (kk >> 1) + 64)
    ring_j = jnp.where(jj < 96, jj >> 1, (jj >> 1) + 64)
    rring = const(ring_k == jj, 0.5)
    pring = const(ring_j == kk, 1.0)
    p0 = jnp.concatenate([const((jj >> 1) == kk, 1.0), const((jj >> 1) + 64 == kk, 1.0)], axis=1)

    ninth = F32(1.0 / 9.0)

    def mask9(rows, lo_rows, hi_rows, lanes_in):
        row, lane = iota((rows, LANES), 0), iota((rows, LANES), 1)
        my = jnp.where(row < lo_rows, fyd, jnp.where(row < hi_rows, F32(1.0), fyu))
        mz = jnp.where(lane < lanes_in, F32(1.0), jnp.where(lane < 96, fzu, fzd))
        return my * mz * ninth

    get_rhs.wait()
    recv(r1x[0], x_dn)
    recv(r1x[1], x_up)
    for i in range(4):
        recv(r1[i], backs[i])
    for c, cond in zip(r1x, (x_up, x_dn)):
        sent(c, cond)
    faces = jnp.where((lane32 & 1) == 0, R1R[2], R1R[3])
    for p in range(32):
        ZR[p + 4, 7:8, :] = R1R[0, p : p + 1, :]
        ZR[p + 4, 40:41, :] = R1R[1, p : p + 1, :]
        ZO[p] = roll(faces, -(2 * p + 1), 1)

    def apply_plane(p):
        c = ZR[p + 4, 8:40]
        o = ZO[p]
        left = roll(jnp.where(lane32 == 127, o, c), 1, 1)
        right = roll(jnp.where(lane32 == 0, o, c), -1, 1)
        ysum = ZR[p + 4, 7:39] + ZR[p + 4, 9:41]
        xsum = ZR[p + 3, 8:40] + ZR[p + 5, 8:40]
        return c, 6.0 * c - ((xsum + ysum) + (left + right))

    for p in range(32):
        _, a = apply_plane(p)
        G0[0, p + 4, 8:40] = RHS[p] - a

    m0 = mask9(40, 4, 36, 128)
    m1 = mask9(24, 4, 20, 64)
    m2 = mask9(16, 4, 12, 32)
    m3 = mask9(16, 0, 16, 16)
    m4 = mask9(8, 0, 8, 8)
    m5 = jnp.where(row8 < 4, mask9(8, 0, 8, 4), F32(0.0))
    slot_lane = lane40 - 12 * sum((lane40 >= 12 * i).astype(jnp.int32) for i in range(1, 11))
    slot_low = slot_lane < 6
    my0 = jnp.where(lane40 < 12, fxd, jnp.where(lane40 < 108, F32(1.0), fxu)) * m0
    ms_lo = my0 * jnp.where(slot_low, fzd, F32(1.0))
    ms_hi = my0 * jnp.where(slot_low, F32(1.0), fzu)

    def stencil_sum(v, up_row, dn_row, prev, nxt):
        return ((up_row + dn_row) + (prev + nxt)) + (roll(v, 1, 1) + roll(v, -1, 1))

    def sweep_plane(src, dst, g, p, r0, r1, m):
        v = src[p, r0:r1]
        n = stencil_sum(v, src[p, r0 - 1 : r1 - 1], src[p, r0 + 1 : r1 + 1], src[p - 1, r0:r1], src[p + 1, r0:r1])
        dst[p, r0:r1] = m * (3.0 * v + n) + g[p, r0:r1]

    def sweep0(src, dst, g, j):
        for p in range(j, 4):
            sweep_plane(src, dst, g, p, 4, 44, m0 * fxd)

        for p in range(4, 36):
            sweep_plane(src, dst, g, p, 4, 44, m0)
        for p in range(36, 40 - j):
            sweep_plane(src, dst, g, p, 4, 44, m0 * fxu)

    def sweeps12(g, sa, sb, n, m):
        lo, hi = m * fxd, m * fxu
        for j, (src, dst) in enumerate(((g, sa), (sa, sb), (sb, sa)), 1):
            for p in range(j, n + 8 - j):
                sweep_plane(src, dst, g, p, 4, 12 + n, lo if p < 4 else m if p < n + 4 else hi)

    def sweeps_small(g, sa, sb, n, rows, m):
        for src, dst in ((g, sa), (sa, sb), (sb, sa)):
            for p in range(1, n + 1):
                sweep_plane(src, dst, g, p, 8, 8 + rows, m)
        return sa

    def sweep_slab(src, dst, g, m):
        for q in range(4):
            v = src[q, 4:44]
            prev = src[q - 1, 4:44] if q else roll(src[3, 4:44], 12, 1)
            nxt = src[q + 1, 4:44] if q < 3 else roll(src[0, 4:44], -12, 1)
            n = stencil_sum(v, src[q, 3:43], src[q, 5:45], prev, nxt)
            dst[q, 4:44] = m * (3.0 * v + n) + g[q, 4:44]

    def pair_mean(a, b, first_row, rows):
        even, odd = pl.ds(first_row, rows, stride=2), pl.ds(first_row + 1, rows, stride=2)
        return 0.25 * ((a[even, :] + a[odd, :]) + (b[even, :] + b[odd, :]))

    def double_rows(dst, v):
        n = v.shape[0]
        dst[pl.ds(0, n, stride=2), :] = v
        dst[pl.ds(1, n, stride=2), :] = v

    def all_reduce_start(tile, k):
        o = S_SET + SET * k
        mine = lax.rem(gx, 2) * NGY + gy
        ARA[k, mine] = tile
        copies = []
        for dc in range(2):
            for dy in range(NGY):
                if dc or dy:
                    dev = {"gx": gx_core if dc else gx, "gy": lax.rem(gy + dy, NGY)}
                    copies.append(rcopy(ARA.at[k, mine], ARA.at[k, mine], o + O_ARA + dc * NGY + dy, dev))
        return copies

    def total(ref, k, n):
        t = [ref[k, i] for i in range(n)]
        while len(t) > 1:
            t = [t[i] + t[i + 1] for i in range(0, len(t), 2)]
        return t[0]

    def all_reduce_next(copies, k):
        o = S_SET + SET * k
        for c in copies:
            recv(c)
        mine = (gx >> 1) * NGZ + gz
        ARB[k, mine] = total(ARA, k, 8)
        out = []
        for far in range(2):
            for dz in range(NGZ):
                if far or dz:
                    dev = {"gx": gx_far if far else gx, "gz": lax.rem(gz + dz, NGZ)}
                    out.append(rcopy(ARB.at[k, mine], ARB.at[k, mine], o + O_ARB + far * NGZ + dz, dev))
        return out

    def all_reduce_end(copies, k):
        for c in copies:
            recv(c)
        tile = total(ARB, k, 16)
        along = jnp.sum(tile[0:1], axis=1, keepdims=True)
        curve = jnp.sum(tile[1:2], axis=1, keepdims=True)
        return along / curve

    def dots_tile(a, b):
        a = jnp.sum(a, axis=0, keepdims=True)
        b = jnp.sum(b, axis=0, keepdims=True)
        return jnp.concatenate([a, b], axis=0)

    def fold(x):
        return (x[0:8] + x[8:16]) + (x[16:24] + x[24:32])

    def precondition(k, ar):
        o = S_SET + SET * k
        g0, g1, g2 = G0.at[k], G1.at[k], G2.at[k]
        xs = [
            (rcopy(g0.at[pl.ds(32, 4), pl.ds(8, 32)], g0.at[pl.ds(0, 4), pl.ds(8, 32)], o + O_X + 0, {"gx": gxu}), x_up, x_dn),
            (rcopy(g0.at[pl.ds(4, 4), pl.ds(8, 32)], g0.at[pl.ds(36, 4), pl.ds(8, 32)], o + O_X + 1, {"gx": gxd}), x_dn, x_up),
        ]
        ys = []
        for d in range(2):
            r0 = 36 if d == 0 else 8
            for h in range(2):
                YS[k, d, 0:16, pl.ds(4 * h, 4)] = g0[4 + 16 * h : 20 + 16 * h, r0 : r0 + 4]
            dev, s, r = (({"gy": gyu}, y_up, y_dn), ({"gy": gyd}, y_dn, y_up))[d]
            ys.append((rcopy(YS.at[k, d, pl.ds(0, 16)], YR.at[k, d, pl.ds(0, 16)], o + O_Y + d, dev), s, r))
        if ar is not None:
            send_all(ar)
        for c, s, _ in ys + xs:
            send(c, s)
        for i in range(16):
            Q1[i] = pair_mean(g0.at[2 * i + 4], g0.at[2 * i + 5], 8, 16)
        for i in range(8):
            Q2[i, 0:8] = pair_mean(Q1.at[2 * i], Q1.at[2 * i + 1], 0, 8)
        q3 = jnp.concatenate([pair_mean(Q2.at[2 * i], Q2.at[2 * i + 1], 0, 8) for i in range(4)], axis=1)
        T3[...] = dotx(q3, rz3)
        t3 = jnp.where(lane40[0:4] < 64, T3[pl.ds(0, 4, stride=2), :], roll(T3[pl.ds(1, 4, stride=2), :], 64, 1))
        mine = gx * NGY + gy
        C3[k, 0, mine] = t3[0:2]
        c3 = []
        for dz, dev_z, s, r in ((0, gz, None, None), (1, gzu, z_up, z_dn), (2, gzd, z_dn, z_up)):
            for dx in range(NGX):
                for dy in range(NGY):
                    if dz or dx or dy:
                        c3.append((rcopy(
                            C3.at[k, 0, mine], C3.at[k, dz, mine], o + O_C3 + 16 * dz + dx * NGY + dy,
                            {"gx": lax.rem(gx + dx, NGX), "gy": lax.rem(gy + dy, NGY), "gz": dev_z},
                        ), s, r))
        for c, s, _ in c3:
            send(c, s)
        g2[4:12, 8:16] = dotx(Q2[:, 0:8].reshape(64, LANES), rz2).reshape(8, 8, LANES)
        g1[4:20, 8:24] = dotx(Q1[...].reshape(256, LANES), rz1).reshape(16, 16, LANES)
        lane4 = iota((1, 4, LANES), 2)
        quarter = [lane4 < 32, lane4 < 64, lane4 < 96]

        def four(v):
            return jnp.where(quarter[1], jnp.where(quarter[0], v[0], v[1]), jnp.where(quarter[2], v[2], v[3]))

        ds = []
        for d in range(2):
            r1, r2 = (20, 12) if d == 0 else (8, 8)
            for h in range(2):
                rows = pl.ds(4 * h, 4)
                a, b = g1[4 + 4 * h : 8 + 4 * h, r1 : r1 + 4], g1[12 + 4 * h : 16 + 4 * h, r1 : r1 + 4]
                YS[k, d, 16:20, rows] = jnp.where(quarter[1], a, b)
                YS[k, d, 20:21, rows] = four([g2[4 + 2 * i + h : 5 + 2 * i + h, r2 : r2 + 4] for i in range(4)])
            dev, s, r = (({"gy": gyu}, y_up, y_dn), ({"gy": gyd}, y_dn, y_up))[d]
            ys.append((rcopy(YS.at[k, d, pl.ds(16, 5)], YR.at[k, d, pl.ds(16, 5)], o + O_Y + 2 + d, dev), s, r))
        for d, (dev, s, r) in enumerate(diagonals):
            up_x, up_y = d < 2, d % 2 == 0
            at = lambda n, i: 3 + n - (i - 1) if up_x else 4 + i - 1
            row = lambda n, m: 8 + n - m if up_y else 8
            for i, m, to in ((1, 3, 0), (2, 2, 3), (3, 1, 5)):
                DS[k, d, to : to + m] = g0[at(32, i), pl.ds(row(32, m), m)]
            low3 = lane40[0:3] < 64
            DS[k, d, 8:11] = jnp.where(low3, g1[at(16, 1), pl.ds(row(16, 3), 3)], g1[at(16, 2), pl.ds(row(16, 3), 3)])
            DS[k, d, 11:12] = g1[at(16, 3), pl.ds(row(16, 1), 1)]
            v = [g2[at(8, i), pl.ds(row(8, 3), 3)] for i in (1, 2, 3)]
            DS[k, d, 12:15] = jnp.where(low3, jnp.where(lane40[0:3] < 32, v[0], v[1]), v[2])
            ds.append((rcopy(DS.at[k, d], DR.at[k, d], o + O_D + d, dev), s, r))
        lane16 = iota((16, LANES), 1)
        eighth = [lane8 < 32, lane8 < 64, lane8 < 96]
        more = []
        for d in range(2):
            p1, p2 = (16, 8) if d == 0 else (4, 4)
            for h in range(2):
                XS[k, d, 16 * h : 16 * h + 16] = jnp.where(lane16 < 64, g1[p1 + h, 8:24], g1[p1 + 2 + h, 8:24])
            v = [g2[p2 + i, 8:16] for i in range(4)]
            XS[k, d, 32:40] = jnp.where(eighth[1], jnp.where(eighth[0], v[0], v[1]), jnp.where(eighth[2], v[2], v[3]))
            dev, s, r = (({"gx": gxu}, x_up, x_dn), ({"gx": gxd}, x_dn, x_up))[d]
            more.append((rcopy(XS.at[k, d], XR.at[k, d], o + O_X + 2 + d, dev), s, r))
        for c, s, _ in ys[2:] + ds + more:
            send(c, s)
        if ar is not None:
            ar = all_reduce_next(ar, 0)
            send_all(ar)
        for c, _, r in xs + more + ys + ds:
            recv(c, r)
        for d in range(2):
            p1, p2 = (0, 0) if d == 0 else (20, 12)
            for h in range(2):
                v = XR[k, d, 16 * h : 16 * h + 16]
                w = roll(v, 64, 1)
                g1[p1 + h, 8:24] = jnp.where(lane16 < 64, v, w)
                g1[p1 + 2 + h, 8:24] = jnp.where(lane16 < 64, w, v)
            v = XR[k, d, 32:40]
            w = [roll(v, 32 * i, 1) for i in range(4)]
            for i in range(4):
                g2[p2 + i, 8:16] = jnp.where(eighth[0], w[(4 - i) % 4], w[(5 - i) % 4])
        for d in range(2):
            r0, r1, r2 = (4, 4, 4) if d == 0 else (40, 24, 16)
            for h in range(2):
                rows = pl.ds(4 * h, 4)
                g0[4 + 16 * h : 20 + 16 * h, r0 : r0 + 4] = YR[k, d, 0:16, rows]
                v = YR[k, d, 16:20, rows]
                w = roll(v, 64, 2)
                g1[4 + 4 * h : 8 + 4 * h, r1 : r1 + 4] = jnp.where(quarter[1], v, w)
                g1[12 + 4 * h : 16 + 4 * h, r1 : r1 + 4] = jnp.where(quarter[1], w, v)
                v = YR[k, d, 20:21, rows]
                w = [roll(v, 32 * i, 2) for i in range(4)]
                for i in range(4):
                    g2[4 + 2 * i + h : 5 + 2 * i + h, r2 : r2 + 4] = jnp.where(quarter[0], w[(4 - i) % 4], w[(5 - i) % 4])
        for d in range(4):
            up_x, up_y = d < 2, d % 2 == 0
            at = lambda n, i: 4 - i if up_x else 3 + n + i
            row = lambda n, m: 8 - m if up_y else 8 + n
            for i, m, to in ((1, 3, 0), (2, 2, 3), (3, 1, 5)):
                g0[at(32, i), pl.ds(row(32, m), m)] = DR[k, d, to : to + m]
            low3 = lane40[0:3] < 64
            v = DR[k, d, 8:11]
            w = roll(v, 64, 1)
            g1[at(16, 1), pl.ds(row(16, 3), 3)] = jnp.where(low3, v, w)
            g1[at(16, 2), pl.ds(row(16, 3), 3)] = jnp.where(low3, w, v)
            g1[at(16, 3), pl.ds(row(16, 1), 1)] = DR[k, d, 11:12]
            v = DR[k, d, 12:15]
            w = [roll(v, 32 * i, 1) for i in range(4)]
            for i in range(3):
                g2[at(8, i + 1), pl.ds(row(8, 3), 3)] = jnp.where(lane40[0:3] < 32, w[(4 - i) % 4], w[(5 - i) % 4])
        half_slots = []
        for h in range(2):
            acc = jnp.zeros((24, LANES), F32)
            for s in range(12):
                acc = jnp.where(lane40[0:24] >> 3 == s, roll(g1[12 * h + s, 4:28], 8 * s - 60, 1), acc)
            half_slots.append(acc)
        acc = jnp.zeros((16, LANES), F32)
        for s in range(16):
            acc = jnp.where(lane40[0:16] >> 3 == s, roll(g2[s, 4:20], 8 * s - 28, 1), acc)
        half_slots += [acc[0:8], acc[8:16]]
        for i, n in ((0, 24), (2, 8)):
            a, b = half_slots[i : i + 2]
            first_four = (lane40[0:n] & 4) == 0
            rows = pl.ds(12 * i, n)
            ZL[k, 0, rows] = jnp.where(first_four, a, roll(b, 4, 1))
            ZL[k, 1, rows] = jnp.where(first_four, roll(a, -4, 1), b)
        zl = [
            (rcopy(ZL.at[k, 0], ZLR.at[k, 0], o + O_ZL + 0, {"gz": gzu}), z_up, z_dn),
            (rcopy(ZL.at[k, 1], ZLR.at[k, 1], o + O_ZL + 1, {"gz": gzd}), z_dn, z_up),
        ]
        for c, s, _ in zl:
            send(c, s)
        for q in range(4):
            acc = jnp.zeros((40, LANES), F32)
            for s in range(10):
                in_slot = (lane40 >= 12 * s) & (lane40 < 12 * s + 12)
                acc = jnp.where(in_slot, roll(g0[4 * s + q, 4:44], 12 * s + 6, 1), acc)
            ZC[k, q] = acc
        for i in range(2):
            a, b = ZC[k, 2 * i], ZC[k, 2 * i + 1]
            ZCS[k, 0, i] = jnp.where(slot_low, a, roll(b, 6, 1))
            ZCS[k, 1, i] = jnp.where(slot_low, roll(a, -6, 1), b)
        zs = [
            (rcopy(ZCS.at[k, 0], ZCR.at[k, 0], o + O_Z + 0, {"gz": gzu}), z_up, z_dn),
            (rcopy(ZCS.at[k, 1], ZCR.at[k, 1], o + O_Z + 1, {"gz": gzd}), z_dn, z_up),
        ]
        for c, s, _ in zs:
            send(c, s)
        sweep0(g0, SA0, g0, 1)
        sweep0(SA0, SB0, g0, 2)
        sweep0(SB0, SA0, g0, 3)
        for c, _, r in c3:
            recv(c, r)
        for g in range(4):
            own, lo, hi = (jnp.concatenate([C3[k, i, 4 * g + j] for j in range(4)], axis=0) for i in range(3))
            for px in range(4):
                for odd in range(2):
                    off = 16 * px + 64 * odd
                    v = jnp.where(lane8 < 32, roll(hi, 16 - off, 1), roll(lo, 112 - off, 1))
                    v = jnp.where(lane8 < 16, roll(own, -off, 1), v)
                    G3.at[4 * g + px + 1][pl.ds(8 + odd, 8, stride=2), :] = v
        q = jnp.concatenate([pair_mean(G3.at[2 * i + 1], G3.at[2 * i + 2], 8, 8) for i in range(8)], axis=0)
        q = dotx(q, rring)
        for i in range(8):
            G4[i + 1, 8:16] = q[8 * i : 8 * i + 8]
        q = jnp.concatenate([pair_mean(G4.at[2 * i + 1], G4.at[2 * i + 2], 8, 8) for i in range(4)], axis=0)
        q = dotx(q, rring)
        for i in range(4):
            G5[i + 1, 8:16] = jnp.where(row8 < 4, q[8 * i : 8 * i + 8], F32(0.0))
        s5 = sweeps_small(G5, SA5, SB5, 4, 8, m5)
        s4 = sweeps_small(G4, SA4, SB4, 8, 8, m4)
        s3 = sweeps_small(G3, SA3, SB3, 16, 16, m3)
        t5 = dotx(jnp.concatenate([s5[i + 1, 8:16] for i in range(4)], axis=0) * F32(4.0**5 / 9.0), pring)
        for i in range(4):
            double_rows(ZP4.at[i], t5[8 * i : 8 * i + 8])
        c4 = jnp.concatenate([s4[i + 1, 8:16] * F32(4.0**4 / 9.0) + ZP4[i // 2, 0:8] for i in range(8)], axis=0)
        t4 = dotx(c4, pring)
        for i in range(8):
            double_rows(ZP3.at[i], t4[8 * i : 8 * i + 8])
        for i in range(16):
            C3P[i + 1, 8:24] = s3[i + 1, 8:24] * F32(4.0**3 / 9.0) + ZP3[i // 2]
        start = 8 + 4 * gy - 2
        c3l = [C3P[4 * gx + i, pl.ds(start, 8), :] for i in range(6)]
        t3 = dotx(jnp.concatenate(c3l, axis=0), pring)
        for i in range(6):
            double_rows(ZP2.at[i], t3[8 * i : 8 * i + 8])
        for c, _, r in zl:
            recv(c, r)
        lane24, lane16 = lane40[0:24], lane40[0:16]
        lo, hi = ZLR[k, 0, 0:24], ZLR[k, 1, 0:24]
        for p in range(24):
            at = 8 * (p % 12) + 4 * (p // 12)
            v = jnp.where(lane24 < 96, roll(hi, 64 - at, 1), roll(lo, 124 - at, 1))
            g1[p, 4:28] = jnp.where(lane24 < 64, g1[p, 4:28], v)
        lo = jnp.concatenate([ZLR[k, 0, 24:32], roll(ZLR[k, 0, 24:32], -4, 1)], axis=0)
        hi = jnp.concatenate([ZLR[k, 1, 24:32], roll(ZLR[k, 1, 24:32], -4, 1)], axis=0)
        for p in range(16):
            v = jnp.where(lane16 < 96, roll(hi, 32 - 8 * p, 1), roll(lo, 124 - 8 * p, 1))
            g2[p, 4:20] = jnp.where(lane16 < 32, g2[p, 4:20], v)
        sweeps12(g2, SA2, SB2, 8, m2)
        sweeps12(g1, SA1, SB1, 16, m1)
        for c, _, r in zs:
            recv(c, r)
        for i in range(2):
            below, above = ZCR[k, 0, i], ZCR[k, 1, i]
            a, b = ZC[k, 2 * i], ZC[k, 2 * i + 1]
            SLA[0, 2 * i, 4:44] = jnp.where(slot_low, below, a)
            SLA[0, 2 * i + 1, 4:44] = jnp.where(slot_low, roll(below, -6, 1), b)
            SHA[0, 2 * i, 4:44] = jnp.where(slot_low, a, roll(above, 6, 1))
            SHA[0, 2 * i + 1, 4:44] = jnp.where(slot_low, b, above)
        slabs = ((SLA, SLB, ms_lo), (SHA, SHB, ms_hi))
        c2 = [SA2[p, 4:20] * F32(16.0 / 9.0) + ZP2[(p - 2) // 2] for p in range(3, 13)]
        t2 = dotx(jnp.concatenate(c2, axis=0), pring)
        for a, b, m in slabs:
            sweep_slab(a.at[0], a.at[1], a.at[0], m)
        for i in range(10):
            double_rows(ZP1.at[i], t2[16 * i : 16 * i + 16])
        c1 = [SA1[p, 4:28] * F32(4.0 / 9.0) + ZP1[(p - 2) // 2, 4:28] for p in range(3, 21)]
        t1 = dotx(jnp.concatenate(c1, axis=0), p0)
        for a, b, m in slabs:
            sweep_slab(a.at[1], b, a.at[0], m)
            sweep_slab(b, a.at[1], a.at[0], m)
        for i in range(18):
            double_rows(ZP0.at[i], t1[24 * i : 24 * i + 24, 0:128])
            double_rows(ZPO.at[i], t1[24 * i : 24 * i + 24, 128:256])
        edge40 = (lane40 < 3) | (lane40 >= 125)
        merged = [jnp.where(slot_low, SHA[1, q, 4:44], SLA[1, q, 4:44]) for q in range(4)]
        for q in range(4):
            SLB[q, 4:44] = merged[q]
            SHB[q, 4:44] = jnp.where(slot_low, SLA[1, q, 4:44], SHA[1, q, 4:44])
        for p in range(3, 37):
            s, q = p // 4, p % 4
            e = roll(SLB[q, 4:44], -(12 * s + 6), 1)
            z = jnp.where(edge40, e, SA0[p, 4:44])
            ZR[p, 4:44] = z * ninth + ZP0[(p - 2) // 2, 4:44]
            if 4 <= p < 36:
                e = roll(SHB[q, 8:40], -(12 * s + 6), 1)
                ZO[p - 4] = e * ninth + ZPO[(p - 2) // 2, 8:40]
        return ar

    precondition(0, None)

    zero8 = jnp.zeros((8, LANES), F32)
    a = b = zero8
    for p in range(32):
        z, w = apply_plane(p)
        Z0[p] = z
        G0[1, p + 4, 8:40] = w
        a = a + fold(G0[0, p + 4, 8:40] * z)
        b = b + fold(z * w)
    ar = all_reduce_start(dots_tile(a, b), 0)
    ar = precondition(1, ar)
    alpha = all_reduce_end(ar, 0)
    keep_u.wait()

    a = b = zero8
    for p in range(32):
        y, v = apply_plane(p)
        z = Z0[p]
        w = G0[1, p + 4, 8:40]
        r1 = G0[0, p + 4, 8:40] - alpha * w
        z1 = z - alpha * y
        w1 = w - alpha * v
        sol[p] = U[p] + alpha * z
        res[p] = r1
        Y0[p] = z1
        V[p] = w1
        a = a + fold(r1 * z1)
        b = b + fold(z1 * w1)
    ar = all_reduce_start(dots_tile(a, b), 1)
    send_all(ar)
    early = pending[: -len(ar)]
    pending[:] = pending[-len(ar) :]
    finish(early)
    ar = all_reduce_next(ar, 1)
    send_all(ar)
    alpha1 = all_reduce_end(ar, 1)

    def last(c, _):
        for i in range(8):
            p = 8 * c + i
            sol[p] = sol[p] + alpha1 * Y0[p]
            res[p] = res[p] - alpha1 * V[p]
        return 0

    lax.fori_loop(0, 4, last, 0)
    finish(pending)


def shards(rhs, u):
    v = lambda *shape: pltpu.VMEM(shape, F32)
    field = v(32, 32, 128)
    scratch = [
        field, field,
        v(40, 48, 128), field,
        v(2, 40, 48, 128), v(2, 24, 32, 128), v(2, 16, 24, 128),
        v(40, 48, 128), v(40, 48, 128),
        v(24, 32, 128), v(24, 32, 128), v(16, 24, 128), v(16, 24, 128),
        field, field, field,
        v(16, 16, 128), v(8, 16, 128),
        v(2, 2, 21, 8, 128), v(2, 2, 21, 8, 128), v(2, 4, 16, 128), v(2, 4, 16, 128), v(2, 2, 40, 128), v(2, 2, 40, 128),
        v(2, 4, 40, 128), v(2, 2, 2, 40, 128), v(2, 2, 2, 40, 128),
        v(2, 2, 32, 128), v(2, 2, 32, 128),
        v(2, 4, 48, 128), v(4, 48, 128), v(2, 4, 48, 128), v(4, 48, 128),
        v(4, 32, 128), v(4, 32, 128),
        v(2, 3, 16, 2, 128), v(8, 128),
        v(18, 32, 128), v(18, 32, 128), v(18, 32, 128), v(18, 32, 128),
        v(10, 24, 128), v(10, 24, 128), v(10, 24, 128),
        v(6, 24, 128), v(6, 24, 128), v(6, 24, 128),
        v(18, 48, 128), v(18, 48, 128), v(10, 32, 128), v(6, 16, 128), v(8, 16, 128), v(4, 16, 128),
        v(2, 8, 2, 128), v(2, 16, 2, 128),
        pltpu.SemaphoreType.DMA((NSEM,)), pltpu.SemaphoreType.DMA((NSEM,)), pltpu.SemaphoreType.DMA((3,)),
    ]
    block = jax.ShapeDtypeStruct((32, 32, 128), F32)
    return pl.pallas_call(
        kernel,
        out_shape=(block, block),
        in_specs=[pl.BlockSpec(memory_space=pltpu.HBM)] * 2,
        out_specs=[pl.BlockSpec(memory_space=pltpu.VMEM)] * 2,
        scratch_shapes=scratch,
        compiler_params=pltpu.CompilerParams(
            collective_id=0, has_side_effects=True, vmem_limit_bytes=24 * 2**20
        ),
    )(pltpu.with_memory_space_constraint(rhs, pltpu.HBM), pltpu.with_memory_space_constraint(u, pltpu.HBM))


def solution(mesh):
    spec = P("gx", "gy", "gz")
    return jax.shard_map(
        shards, mesh=mesh, in_specs=(spec, spec), out_specs=(spec, spec), check_vma=False
    )
```

```python
import functools

import jax
import jax.numpy as jnp
from jax import lax
from jax.experimental import pallas as pl
from jax.experimental.pallas import tpu as pltpu
from jax.sharding import PartitionSpec as P

F32 = jnp.float32
BF16 = jnp.bfloat16
MESH = pl.DeviceIdType.MESH
NGX, NGY, NGZ = 4, 4, 8
LANES = 128

S_SET = 6
O_X, O_Y, O_D, O_Z, O_ZL, O_C3, O_ARA, O_ARB = 0, 6, 10, 14, 16, 18, 66, 74
SET = 90
NSEM = S_SET + 2 * SET


def roll(v, shift, axis):
    n = v.shape[axis]
    shift = shift % n
    return v if shift == 0 else pltpu.roll(v, shift, axis)


def iota(shape, axis):
    return lax.broadcasted_iota(jnp.int32, shape, axis)


def dotx(x, m):
    hi = x.astype(BF16)
    rest = x - hi.astype(F32)
    mid = rest.astype(BF16)
    low = (rest - mid.astype(F32)).astype(BF16)
    n = x.shape[0]
    y = jnp.dot(jnp.concatenate([hi, mid, low], axis=0), m, preferred_element_type=F32)
    return y[0:n] + y[n : 2 * n] + y[2 * n : 3 * n]


def kernel(
    rhs_hbm, u_hbm, sol, res, Y0, V, last_alpha,
    RHS, U, ZR, ZO, G0, G1, G2, SA0, SB0, SA1, SB1, SA2, SB2, Z0,
    Q1, Q2, YS, YR, DS, DR, XS, XR, ZC, ZCS, ZCR, ZL, ZLR, SLA, SLB, SHA, SHB, R1S, R1R, C3, T3,
    G3, SA3, SB3, C3P, G4, SA4, SB4, G5, SA5, SB5,
    ZP0, ZPO, ZP1, ZP2, ZP3, ZP4, ARA, ARB, ss, rs, ls,
):
    gx, gy, gz = lax.axis_index("gx"), lax.axis_index("gy"), lax.axis_index("gz")
    x_up, x_dn = gx < NGX - 1, gx > 0
    y_up, y_dn = gy < NGY - 1, gy > 0
    z_up, z_dn = gz < NGZ - 1, gz > 0
    one = lambda c: jnp.where(c, F32(1.0), F32(0.0))
    fxu, fxd, fyu, fyd, fzu, fzd = map(one, (x_up, x_dn, y_up, y_dn, z_up, z_dn))
    gxu, gxd = lax.rem(gx + 1, NGX), lax.rem(gx + NGX - 1, NGX)
    gyu, gyd = lax.rem(gy + 1, NGY), lax.rem(gy + NGY - 1, NGY)
    gzu, gzd = lax.rem(gz + 1, NGZ), lax.rem(gz + NGZ - 1, NGZ)
    gx_core = gx + 1 - 2 * lax.rem(gx, 2)
    gx_far = lax.rem(gx + 2, NGX)

    pending = []

    def rcopy(src, dst, i, dev):
        return pltpu.make_async_remote_copy(
            src_ref=src, dst_ref=dst, send_sem=ss.at[i], recv_sem=rs.at[i],
            device_id=dev, device_id_type=MESH,
        )

    def send(copy, cond=None):
        if cond is None:
            copy.start()
        else:
            pl.when(cond)(lambda: copy.start())
        pending.append((copy, cond))

    def sent(copy, cond):
        pending[:] = [q for q in pending if q[0] is not copy]
        pl.when(cond)(copy.wait_send)

    def recv(copy, cond=None):
        if cond is None:
            copy.wait_recv()
        else:
            pl.when(cond)(lambda: copy.wait_recv())

    def finish(copies):
        for copy, cond in copies:
            if cond is None:
                copy.wait_send()
            else:
                pl.when(cond)(copy.wait_send)

    def send_all(copies):
        for c in copies:
            send(c)

    inner = (pl.ds(4, 32), pl.ds(8, 32))
    get_u = pltpu.make_async_copy(u_hbm, ZR.at[inner], ls.at[0])
    get_rhs = pltpu.make_async_copy(rhs_hbm, RHS, ls.at[1])
    keep_u = pltpu.make_async_copy(u_hbm, U, ls.at[2])
    get_u.start()
    get_rhs.start()
    keep_u.start()

    ZR[3] = jnp.zeros((48, LANES), F32)
    ZR[36] = jnp.zeros((48, LANES), F32)
    R1R[...] = jnp.zeros_like(R1R)
    bar = pltpu.get_barrier_semaphore()
    greet = [(1, 0, 0), (3, 0, 0), (0, 1, 0), (0, 3, 0), (0, 0, 1), (0, 0, 7)]
    greet += [(dx, dy, dz) for dz in (0, 1, 7) for dx in range(NGX) for dy in range(NGY)]
    greet += [(dx, 0, dz) for dz in range(2, 7) for dx in (0, 2)]
    greet = list(dict.fromkeys(g for g in greet if any(g)))
    near = {
        "gx": [gx, gxu, gx_far, gxd],
        "gy": [gy, gyu, lax.rem(gy + 2, NGY), gyd],
        "gz": [lax.rem(gz + dz, NGZ) for dz in range(NGZ)],
    }
    for dx, dy, dz in greet:
        pl.semaphore_signal(
            bar, inc=1, device_id_type=MESH, device_id={"gx": near["gx"][dx], "gy": near["gy"][dy], "gz": near["gz"][dz]}
        )
    get_u.wait()

    lane8 = iota((8, LANES), 1)
    row8 = iota((8, LANES), 0)
    lane32 = iota((32, LANES), 1)
    lane40 = iota((40, LANES), 1)

    diagonals = []
    for up_x in (True, False):
        for up_y in (True, False):
            diagonals.append((
                {"gx": gxu if up_x else gxd, "gy": gyu if up_y else gyd},
                (x_up if up_x else x_dn) & (y_up if up_y else y_dn),
                (x_dn if up_x else x_up) & (y_dn if up_y else y_up),
            ))

    r1x = [
        rcopy(ZR.at[pl.ds(35, 1), pl.ds(8, 32)], ZR.at[pl.ds(3, 1), pl.ds(8, 32)], 0, {"gx": gxu}),
        rcopy(ZR.at[pl.ds(4, 1), pl.ds(8, 32)], ZR.at[pl.ds(36, 1), pl.ds(8, 32)], 1, {"gx": gxd}),
    ]
    devs = [{"gy": gyu}, {"gy": gyd}, {"gz": gzu}, {"gz": gzd}]
    conds = [y_up, y_dn, z_up, z_dn]
    backs = [y_dn, y_up, z_dn, z_up]
    r1 = [rcopy(R1S.at[min(i, 2)], R1R.at[i], 2 + i, devs[i]) for i in range(4)]
    zz = jnp.zeros((32, LANES), F32)
    for p in range(32):
        zz = jnp.where(lane32 >> 1 == p, roll(ZR[p + 4, 8:40], 2 * p + 1, 1), zz)
    R1S[2] = zz
    for p in range(32):
        R1S[0, p : p + 1, :] = ZR[p + 4, 39:40, :]
        R1S[1, p : p + 1, :] = ZR[p + 4, 8:9, :]
    pl.semaphore_wait(bar, len(greet))
    send(r1[2], conds[2])
    send(r1[3], conds[3])
    send(r1x[0], x_up)
    send(r1x[1], x_dn)
    send(r1[0], conds[0])
    send(r1[1], conds[1])

    for k in range(2):
        def clear(*refs):
            def run():
                for ref in refs:
                    ref[...] = jnp.zeros_like(ref)

            return run

        pl.when(jnp.logical_not(x_dn))(clear(G0.at[k, pl.ds(0, 4)], XR.at[k, 0]))
        pl.when(jnp.logical_not(x_up))(clear(G0.at[k, pl.ds(36, 4)], XR.at[k, 1]))
        pl.when(jnp.logical_not(y_dn))(clear(YR.at[k, 0]))
        pl.when(jnp.logical_not(y_up))(clear(YR.at[k, 1]))
        pl.when(jnp.logical_not(z_dn))(clear(ZCR.at[k, 0], ZLR.at[k, 0], C3.at[k, 1]))
        pl.when(jnp.logical_not(z_up))(clear(ZCR.at[k, 1], ZLR.at[k, 1], C3.at[k, 2]))
        for d, (_, _, from_there) in enumerate(diagonals):
            pl.when(jnp.logical_not(from_there))(clear(DR.at[k, d]))
    for ref in (G3, SA3, SB3, C3P, G4, SA4, SB4, G5, SA5, SB5, Q2):
        ref[...] = jnp.zeros_like(ref)
    kk, jj = iota((LANES, LANES), 0), iota((LANES, LANES), 1)

    def const(cond, value):
        return jnp.where(cond, F32(value), F32(0.0)).astype(BF16)

    rz1 = const((kk >> 1) == (jj & 63), 0.5)
    rz2 = const((kk >> 2) == (jj & 31), 0.25)
    rz3 = jnp.concatenate([const((kk >> 3) + 16 * i == jj, 0.125) for i in range(4)], axis=0)
    ring_k = jnp.where(kk < 96, kk >> 1, (kk >> 1) + 64)
    ring_j = jnp.where(jj < 96, jj >> 1, (jj >> 1) + 64)
    rring = const(ring_k == jj, 0.5)
    pring = const(ring_j == kk, 1.0)
    p0 = jnp.concatenate([const((jj >> 1) == kk, 1.0), const((jj >> 1) + 64 == kk, 1.0)], axis=1)

    ninth = F32(1.0 / 9.0)

    def mask9(rows, lo_rows, hi_rows, lanes_in):
        row, lane = iota((rows, LANES), 0), iota((rows, LANES), 1)
        my = jnp.where(row < lo_rows, fyd, jnp.where(row < hi_rows, F32(1.0), fyu))
        mz = jnp.where(lane < lanes_in, F32(1.0), jnp.where(lane < 96, fzu, fzd))
        return my * mz * ninth

    get_rhs.wait()
    recv(r1x[0], x_dn)
    recv(r1x[1], x_up)
    for i in range(4):
        recv(r1[i], backs[i])
    for c, cond in zip(r1x, (x_up, x_dn)):
        sent(c, cond)
    faces = jnp.where((lane32 & 1) == 0, R1R[2], R1R[3])
    for p in range(32):
        ZR[p + 4, 7:8, :] = R1R[0, p : p + 1, :]
        ZR[p + 4, 40:41, :] = R1R[1, p : p + 1, :]
        ZO[p] = roll(faces, -(2 * p + 1), 1)

    def apply_plane(p):
        c = ZR[p + 4, 8:40]
        o = ZO[p]
        left = roll(jnp.where(lane32 == 127, o, c), 1, 1)
        right = roll(jnp.where(lane32 == 0, o, c), -1, 1)
        ysum = ZR[p + 4, 7:39] + ZR[p + 4, 9:41]
        xsum = ZR[p + 3, 8:40] + ZR[p + 5, 8:40]
        return c, 6.0 * c - ((xsum + ysum) + (left + right))

    for p in range(32):
        _, a = apply_plane(p)
        G0[0, p + 4, 8:40] = RHS[p] - a

    m0 = mask9(40, 4, 36, 128)
    m1 = mask9(24, 4, 20, 64)
    m2 = mask9(16, 4, 12, 32)
    m3 = mask9(16, 0, 16, 16)
    m4 = mask9(8, 0, 8, 8)
    m5 = jnp.where(row8 < 4, mask9(8, 0, 8, 4), F32(0.0))
    slot_lane = lane40 - 12 * sum((lane40 >= 12 * i).astype(jnp.int32) for i in range(1, 11))
    slot_low = slot_lane < 6
    my0 = jnp.where(lane40 < 12, fxd, jnp.where(lane40 < 108, F32(1.0), fxu)) * m0
    ms_lo = my0 * jnp.where(slot_low, fzd, F32(1.0))
    ms_hi = my0 * jnp.where(slot_low, F32(1.0), fzu)

    def in_slot(lane, s):
        return (lane >= 12 * s) & (lane < 12 * s + 12)

    def stencil_sum(v, up_row, dn_row, prev, nxt):
        return ((up_row + dn_row) + (prev + nxt)) + (roll(v, 1, 1) + roll(v, -1, 1))

    def sweep_plane(src, dst, g, p, r0, r1, m):
        v = src[p, r0:r1]
        n = stencil_sum(v, src[p, r0 - 1 : r1 - 1], src[p, r0 + 1 : r1 + 1], src[p - 1, r0:r1], src[p + 1, r0:r1])
        dst[p, r0:r1] = m * (3.0 * v + n) + g[p, r0:r1]

    def sweep0(src, dst, g, j):
        for p in range(j, 4):
            sweep_plane(src, dst, g, p, 4, 44, m0 * fxd)

        for p in range(4, 36):
            sweep_plane(src, dst, g, p, 4, 44, m0)
        for p in range(36, 40 - j):
            sweep_plane(src, dst, g, p, 4, 44, m0 * fxu)

    def sweeps12(g, sa, sb, n, m):
        lo, hi = m * fxd, m * fxu
        for j, (src, dst) in enumerate(((g, sa), (sa, sb), (sb, sa)), 1):
            for p in range(j, n + 8 - j):
                sweep_plane(src, dst, g, p, 4, 12 + n, lo if p < 4 else m if p < n + 4 else hi)

    def sweeps_small(g, sa, sb, n, rows, m):
        for src, dst in ((g, sa), (sa, sb), (sb, sa)):
            for p in range(1, n + 1):
                sweep_plane(src, dst, g, p, 8, 8 + rows, m)
        return sa

    def sweep_slab(src, dst, g, m):
        for q in range(4):
            v = src[q, 4:44]
            prev = src[q - 1, 4:44] if q else roll(src[3, 4:44], 12, 1)
            nxt = src[q + 1, 4:44] if q < 3 else roll(src[0, 4:44], -12, 1)
            n = stencil_sum(v, src[q, 3:43], src[q, 5:45], prev, nxt)
            dst[q, 4:44] = m * (3.0 * v + n) + g[q, 4:44]

    def pair_mean(a, b, first_row, rows):
        even, odd = pl.ds(first_row, rows, stride=2), pl.ds(first_row + 1, rows, stride=2)
        return 0.25 * ((a[even, :] + a[odd, :]) + (b[even, :] + b[odd, :]))

    def double_rows(dst, v):
        n = v.shape[0]
        dst[pl.ds(0, n, stride=2), :] = v
        dst[pl.ds(1, n, stride=2), :] = v

    def all_reduce_start(tile, k):
        o = S_SET + SET * k
        mine = lax.rem(gx, 2) * NGY + gy
        ARA[k, mine] = tile
        copies = []
        for dc in range(2):
            for dy in range(NGY):
                if dc or dy:
                    dev = {"gx": gx_core if dc else gx, "gy": lax.rem(gy + dy, NGY)}
                    copies.append(rcopy(ARA.at[k, mine], ARA.at[k, mine], o + O_ARA + dc * NGY + dy, dev))
        return copies

    def total(ref, k, n):
        t = [ref[k, i] for i in range(n)]
        while len(t) > 1:
            t = [t[i] + t[i + 1] for i in range(0, len(t), 2)]
        return t[0]

    def all_reduce_next(copies, k):
        o = S_SET + SET * k
        for c in copies:
            recv(c)
        mine = (gx >> 1) * NGZ + gz
        ARB[k, mine] = total(ARA, k, 8)
        out = []
        for far in range(2):
            for dz in range(NGZ):
                if far or dz:
                    dev = {"gx": gx_far if far else gx, "gz": lax.rem(gz + dz, NGZ)}
                    out.append(rcopy(ARB.at[k, mine], ARB.at[k, mine], o + O_ARB + far * NGZ + dz, dev))
        return out

    def all_reduce_end(copies, k):
        for c in copies:
            recv(c)
        tile = total(ARB, k, 16)
        along = jnp.sum(tile[0:1], axis=1, keepdims=True)
        curve = jnp.sum(tile[1:2], axis=1, keepdims=True)
        return along / curve

    def dots_tile(a, b):
        a = jnp.sum(a, axis=0, keepdims=True)
        b = jnp.sum(b, axis=0, keepdims=True)
        return jnp.concatenate([a, b], axis=0)

    def fold(x):
        return (x[0:8] + x[8:16]) + (x[16:24] + x[24:32])

    def precondition(k, ar):
        o = S_SET + SET * k
        g0, g1, g2 = G0.at[k], G1.at[k], G2.at[k]
        xs = [
            (rcopy(g0.at[pl.ds(32, 4), pl.ds(8, 32)], g0.at[pl.ds(0, 4), pl.ds(8, 32)], o + O_X + 0, {"gx": gxu}), x_up, x_dn),
            (rcopy(g0.at[pl.ds(4, 4), pl.ds(8, 32)], g0.at[pl.ds(36, 4), pl.ds(8, 32)], o + O_X + 1, {"gx": gxd}), x_dn, x_up),
        ]
        ys = []
        for d in range(2):
            r0 = 36 if d == 0 else 8
            for h in range(2):
                YS[k, d, 0:16, pl.ds(4 * h, 4)] = g0[4 + 16 * h : 20 + 16 * h, r0 : r0 + 4]
            dev, s, r = (({"gy": gyu}, y_up, y_dn), ({"gy": gyd}, y_dn, y_up))[d]
            ys.append((rcopy(YS.at[k, d, pl.ds(0, 16)], YR.at[k, d, pl.ds(0, 16)], o + O_Y + d, dev), s, r))
        if ar is not None:
            send_all(ar)
        for c, s, _ in ys + xs:
            send(c, s)
        for i in range(16):
            Q1[i] = pair_mean(g0.at[2 * i + 4], g0.at[2 * i + 5], 8, 16)
        for i in range(8):
            Q2[i, 0:8] = pair_mean(Q1.at[2 * i], Q1.at[2 * i + 1], 0, 8)
        q3 = jnp.concatenate([pair_mean(Q2.at[2 * i], Q2.at[2 * i + 1], 0, 8) for i in range(4)], axis=1)
        T3[...] = dotx(q3, rz3)
        t3 = jnp.where(lane40[0:4] < 64, T3[pl.ds(0, 4, stride=2), :], roll(T3[pl.ds(1, 4, stride=2), :], 64, 1))
        mine = gx * NGY + gy
        C3[k, 0, mine] = t3[0:2]
        c3 = []
        for dz, dev_z, s, r in ((0, gz, None, None), (1, gzu, z_up, z_dn), (2, gzd, z_dn, z_up)):
            for dx in range(NGX):
                for dy in range(NGY):
                    if dz or dx or dy:
                        c3.append((rcopy(
                            C3.at[k, 0, mine], C3.at[k, dz, mine], o + O_C3 + 16 * dz + dx * NGY + dy,
                            {"gx": lax.rem(gx + dx, NGX), "gy": lax.rem(gy + dy, NGY), "gz": dev_z},
                        ), s, r))
        for c, s, _ in c3:
            send(c, s)
        g2[4:12, 8:16] = dotx(Q2[:, 0:8].reshape(64, LANES), rz2).reshape(8, 8, LANES)
        g1[4:20, 8:24] = dotx(Q1[...].reshape(256, LANES), rz1).reshape(16, 16, LANES)
        lane4 = iota((1, 4, LANES), 2)
        quarter = [lane4 < 32, lane4 < 64, lane4 < 96]

        def four(v):
            return jnp.where(quarter[1], jnp.where(quarter[0], v[0], v[1]), jnp.where(quarter[2], v[2], v[3]))

        ds = []
        for d in range(2):
            r1, r2 = (20, 12) if d == 0 else (8, 8)
            for h in range(2):
                rows = pl.ds(4 * h, 4)
                a, b = g1[4 + 4 * h : 8 + 4 * h, r1 : r1 + 4], g1[12 + 4 * h : 16 + 4 * h, r1 : r1 + 4]
                YS[k, d, 16:20, rows] = jnp.where(quarter[1], a, b)
                YS[k, d, 20:21, rows] = four([g2[4 + 2 * i + h : 5 + 2 * i + h, r2 : r2 + 4] for i in range(4)])
            dev, s, r = (({"gy": gyu}, y_up, y_dn), ({"gy": gyd}, y_dn, y_up))[d]
            ys.append((rcopy(YS.at[k, d, pl.ds(16, 5)], YR.at[k, d, pl.ds(16, 5)], o + O_Y + 2 + d, dev), s, r))
        for d, (dev, s, r) in enumerate(diagonals):
            up_x, up_y = d < 2, d % 2 == 0
            at = lambda n, i: 3 + n - (i - 1) if up_x else 4 + i - 1
            row = lambda n, m: 8 + n - m if up_y else 8
            for i, m, to in ((1, 3, 0), (2, 2, 3), (3, 1, 5)):
                DS[k, d, to : to + m] = g0[at(32, i), pl.ds(row(32, m), m)]
            low3 = lane40[0:3] < 64
            DS[k, d, 8:11] = jnp.where(low3, g1[at(16, 1), pl.ds(row(16, 3), 3)], g1[at(16, 2), pl.ds(row(16, 3), 3)])
            DS[k, d, 11:12] = g1[at(16, 3), pl.ds(row(16, 1), 1)]
            v = [g2[at(8, i), pl.ds(row(8, 3), 3)] for i in (1, 2, 3)]
            DS[k, d, 12:15] = jnp.where(low3, jnp.where(lane40[0:3] < 32, v[0], v[1]), v[2])
            ds.append((rcopy(DS.at[k, d], DR.at[k, d], o + O_D + d, dev), s, r))
        lane16 = iota((16, LANES), 1)
        eighth = [lane8 < 32, lane8 < 64, lane8 < 96]
        more = []
        for d in range(2):
            p1, p2 = (16, 8) if d == 0 else (4, 4)
            for h in range(2):
                XS[k, d, 16 * h : 16 * h + 16] = jnp.where(lane16 < 64, g1[p1 + h, 8:24], g1[p1 + 2 + h, 8:24])
            v = [g2[p2 + i, 8:16] for i in range(4)]
            XS[k, d, 32:40] = jnp.where(eighth[1], jnp.where(eighth[0], v[0], v[1]), jnp.where(eighth[2], v[2], v[3]))
            dev, s, r = (({"gx": gxu}, x_up, x_dn), ({"gx": gxd}, x_dn, x_up))[d]
            more.append((rcopy(XS.at[k, d], XR.at[k, d], o + O_X + 2 + d, dev), s, r))
        for c, s, _ in ys[2:] + ds + more:
            send(c, s)
        for q in range(4):
            acc = jnp.zeros((32, LANES), F32)
            for s in range(1, 9):
                acc = jnp.where(in_slot(lane32, s), roll(g0[4 * s + q, 8:40], 12 * s + 6, 1), acc)
            ZC[k, q, 4:36] = acc
        if ar is not None:
            ar = all_reduce_next(ar, 0)
            send_all(ar)
        for c, _, r in xs + more + ys + ds:
            recv(c, r)
        for d in range(2):
            p1, p2 = (0, 0) if d == 0 else (20, 12)
            for h in range(2):
                v = XR[k, d, 16 * h : 16 * h + 16]
                w = roll(v, 64, 1)
                g1[p1 + h, 8:24] = jnp.where(lane16 < 64, v, w)
                g1[p1 + 2 + h, 8:24] = jnp.where(lane16 < 64, w, v)
            v = XR[k, d, 32:40]
            w = [roll(v, 32 * i, 1) for i in range(4)]
            for i in range(4):
                g2[p2 + i, 8:16] = jnp.where(eighth[0], w[(4 - i) % 4], w[(5 - i) % 4])
        for d in range(2):
            r0, r1, r2 = (4, 4, 4) if d == 0 else (40, 24, 16)
            for h in range(2):
                rows = pl.ds(4 * h, 4)
                g0[4 + 16 * h : 20 + 16 * h, r0 : r0 + 4] = YR[k, d, 0:16, rows]
                v = YR[k, d, 16:20, rows]
                w = roll(v, 64, 2)
                g1[4 + 4 * h : 8 + 4 * h, r1 : r1 + 4] = jnp.where(quarter[1], v, w)
                g1[12 + 4 * h : 16 + 4 * h, r1 : r1 + 4] = jnp.where(quarter[1], w, v)
                v = YR[k, d, 20:21, rows]
                w = [roll(v, 32 * i, 2) for i in range(4)]
                for i in range(4):
                    g2[4 + 2 * i + h : 5 + 2 * i + h, r2 : r2 + 4] = jnp.where(quarter[0], w[(4 - i) % 4], w[(5 - i) % 4])
        for d in range(4):
            up_x, up_y = d < 2, d % 2 == 0
            at = lambda n, i: 4 - i if up_x else 3 + n + i
            row = lambda n, m: 8 - m if up_y else 8 + n
            for i, m, to in ((1, 3, 0), (2, 2, 3), (3, 1, 5)):
                g0[at(32, i), pl.ds(row(32, m), m)] = DR[k, d, to : to + m]
            low3 = lane40[0:3] < 64
            v = DR[k, d, 8:11]
            w = roll(v, 64, 1)
            g1[at(16, 1), pl.ds(row(16, 3), 3)] = jnp.where(low3, v, w)
            g1[at(16, 2), pl.ds(row(16, 3), 3)] = jnp.where(low3, w, v)
            g1[at(16, 3), pl.ds(row(16, 1), 1)] = DR[k, d, 11:12]
            v = DR[k, d, 12:15]
            w = [roll(v, 32 * i, 1) for i in range(4)]
            for i in range(3):
                g2[at(8, i + 1), pl.ds(row(8, 3), 3)] = jnp.where(lane40[0:3] < 32, w[(4 - i) % 4], w[(5 - i) % 4])
        half_slots = []
        for h in range(2):
            acc = jnp.zeros((24, LANES), F32)
            for s in range(12):
                acc = jnp.where(lane40[0:24] >> 3 == s, roll(g1[12 * h + s, 4:28], 8 * s - 60, 1), acc)
            half_slots.append(acc)
        acc = jnp.zeros((16, LANES), F32)
        for s in range(16):
            acc = jnp.where(lane40[0:16] >> 3 == s, roll(g2[s, 4:20], 8 * s - 28, 1), acc)
        half_slots += [acc[0:8], acc[8:16]]
        for i, n in ((0, 24), (2, 8)):
            a, b = half_slots[i : i + 2]
            first_four = (lane40[0:n] & 4) == 0
            rows = pl.ds(12 * i, n)
            ZL[k, 0, rows] = jnp.where(first_four, a, roll(b, 4, 1))
            ZL[k, 1, rows] = jnp.where(first_four, roll(a, -4, 1), b)
        zl = [
            (rcopy(ZL.at[k, 0], ZLR.at[k, 0], o + O_ZL + 0, {"gz": gzu}), z_up, z_dn),
            (rcopy(ZL.at[k, 1], ZLR.at[k, 1], o + O_ZL + 1, {"gz": gzd}), z_dn, z_up),
        ]
        for c, s, _ in zl:
            send(c, s)
        for q in range(4):
            mid = ZC[k, q, 4:36]
            for s in (0, 9):
                mid = jnp.where(in_slot(lane32, s), roll(g0[4 * s + q, 8:40], 12 * s + 6, 1), mid)
            ZC[k, q, 4:36] = mid
            acc = jnp.zeros((8, LANES), F32)
            for s in range(10):
                g = g0.at[4 * s + q]
                v = jnp.concatenate([g[4:8], g[40:44]], axis=0)
                acc = jnp.where(in_slot(lane8, s), roll(v, 12 * s + 6, 1), acc)
            ZC[k, q, 0:4] = acc[0:4]
            ZC[k, q, 36:40] = acc[4:8]
        for i in range(2):
            a, b = ZC[k, 2 * i], ZC[k, 2 * i + 1]
            ZCS[k, 0, i] = jnp.where(slot_low, a, roll(b, 6, 1))
            ZCS[k, 1, i] = jnp.where(slot_low, roll(a, -6, 1), b)
        zs = [
            (rcopy(ZCS.at[k, 0], ZCR.at[k, 0], o + O_Z + 0, {"gz": gzu}), z_up, z_dn),
            (rcopy(ZCS.at[k, 1], ZCR.at[k, 1], o + O_Z + 1, {"gz": gzd}), z_dn, z_up),
        ]
        for c, s, _ in zs:
            send(c, s)
        sweep0(g0, SA0, g0, 1)
        sweep0(SA0, SB0, g0, 2)
        sweep0(SB0, SA0, g0, 3)
        for c, _, r in c3:
            recv(c, r)
        for g in range(4):
            own, lo, hi = (jnp.concatenate([C3[k, i, 4 * g + j] for j in range(4)], axis=0) for i in range(3))
            for px in range(4):
                for odd in range(2):
                    off = 16 * px + 64 * odd
                    v = jnp.where(lane8 < 32, roll(hi, 16 - off, 1), roll(lo, 112 - off, 1))
                    v = jnp.where(lane8 < 16, roll(own, -off, 1), v)
                    G3.at[4 * g + px + 1][pl.ds(8 + odd, 8, stride=2), :] = v
        q = jnp.concatenate([pair_mean(G3.at[2 * i + 1], G3.at[2 * i + 2], 8, 8) for i in range(8)], axis=0)
        q = dotx(q, rring)
        for i in range(8):
            G4[i + 1, 8:16] = q[8 * i : 8 * i + 8]
        q = jnp.concatenate([pair_mean(G4.at[2 * i + 1], G4.at[2 * i + 2], 8, 8) for i in range(4)], axis=0)
        q = dotx(q, rring)
        for i in range(4):
            G5[i + 1, 8:16] = jnp.where(row8 < 4, q[8 * i : 8 * i + 8], F32(0.0))
        s5 = sweeps_small(G5, SA5, SB5, 4, 8, m5)
        s4 = sweeps_small(G4, SA4, SB4, 8, 8, m4)
        s3 = sweeps_small(G3, SA3, SB3, 16, 16, m3)
        t5 = dotx(jnp.concatenate([s5[i + 1, 8:16] for i in range(4)], axis=0) * F32(4.0**5 / 9.0), pring)
        for i in range(4):
            double_rows(ZP4.at[i], t5[8 * i : 8 * i + 8])
        c4 = jnp.concatenate([s4[i + 1, 8:16] * F32(4.0**4 / 9.0) + ZP4[i // 2, 0:8] for i in range(8)], axis=0)
        t4 = dotx(c4, pring)
        for i in range(8):
            double_rows(ZP3.at[i], t4[8 * i : 8 * i + 8])
        for i in range(16):
            C3P[i + 1, 8:24] = s3[i + 1, 8:24] * F32(4.0**3 / 9.0) + ZP3[i // 2]
        start = 8 + 4 * gy - 2
        c3l = [C3P[4 * gx + i, pl.ds(start, 8), :] for i in range(6)]
        t3 = dotx(jnp.concatenate(c3l, axis=0), pring)
        for i in range(6):
            double_rows(ZP2.at[i], t3[8 * i : 8 * i + 8])
        for c, _, r in zl:
            recv(c, r)
        lane24, lane16 = lane40[0:24], lane40[0:16]
        lo, hi = ZLR[k, 0, 0:24], ZLR[k, 1, 0:24]
        for p in range(24):
            at = 8 * (p % 12) + 4 * (p // 12)
            v = jnp.where(lane24 < 96, roll(hi, 64 - at, 1), roll(lo, 124 - at, 1))
            g1[p, 4:28] = jnp.where(lane24 < 64, g1[p, 4:28], v)
        lo = jnp.concatenate([ZLR[k, 0, 24:32], roll(ZLR[k, 0, 24:32], -4, 1)], axis=0)
        hi = jnp.concatenate([ZLR[k, 1, 24:32], roll(ZLR[k, 1, 24:32], -4, 1)], axis=0)
        for p in range(16):
            v = jnp.where(lane16 < 96, roll(hi, 32 - 8 * p, 1), roll(lo, 124 - 8 * p, 1))
            g2[p, 4:20] = jnp.where(lane16 < 32, g2[p, 4:20], v)
        sweeps12(g2, SA2, SB2, 8, m2)
        sweeps12(g1, SA1, SB1, 16, m1)
        for c, _, r in zs:
            recv(c, r)
        for i in range(2):
            below, above = ZCR[k, 0, i], ZCR[k, 1, i]
            a, b = ZC[k, 2 * i], ZC[k, 2 * i + 1]
            SLA[0, 2 * i, 4:44] = jnp.where(slot_low, below, a)
            SLA[0, 2 * i + 1, 4:44] = jnp.where(slot_low, roll(below, -6, 1), b)
            SHA[0, 2 * i, 4:44] = jnp.where(slot_low, a, roll(above, 6, 1))
            SHA[0, 2 * i + 1, 4:44] = jnp.where(slot_low, b, above)
        slabs = ((SLA, SLB, ms_lo), (SHA, SHB, ms_hi))
        c2 = [SA2[p, 4:20] * F32(16.0 / 9.0) + ZP2[(p - 2) // 2] for p in range(3, 13)]
        t2 = dotx(jnp.concatenate(c2, axis=0), pring)
        for a, b, m in slabs:
            sweep_slab(a.at[0], a.at[1], a.at[0], m)
        for i in range(10):
            double_rows(ZP1.at[i], t2[16 * i : 16 * i + 16])
        c1 = [SA1[p, 4:28] * F32(4.0 / 9.0) + ZP1[(p - 2) // 2, 4:28] for p in range(3, 21)]
        t1 = dotx(jnp.concatenate(c1, axis=0), p0)
        for a, b, m in slabs:
            sweep_slab(a.at[1], b, a.at[0], m)
            sweep_slab(b, a.at[1], a.at[0], m)
        for i in range(18):
            double_rows(ZP0.at[i], t1[24 * i : 24 * i + 24, 0:128])
            double_rows(ZPO.at[i], t1[24 * i : 24 * i + 24, 128:256])
        edge40 = (lane40 < 3) | (lane40 >= 125)
        merged = [jnp.where(slot_low, SHA[1, q, 4:44], SLA[1, q, 4:44]) for q in range(4)]
        for q in range(4):
            SLB[q, 4:44] = merged[q]
            SHB[q, 4:44] = jnp.where(slot_low, SLA[1, q, 4:44], SHA[1, q, 4:44])
        for p in range(3, 37):
            s, q = p // 4, p % 4
            e = roll(SLB[q, 4:44], -(12 * s + 6), 1)
            z = jnp.where(edge40, e, SA0[p, 4:44])
            ZR[p, 4:44] = z * ninth + ZP0[(p - 2) // 2, 4:44]
            if 4 <= p < 36:
                e = roll(SHB[q, 8:40], -(12 * s + 6), 1)
                ZO[p - 4] = e * ninth + ZPO[(p - 2) // 2, 8:40]
        return ar

    precondition(0, None)

    zero8 = jnp.zeros((8, LANES), F32)
    a = b = zero8
    for p in range(32):
        z, w = apply_plane(p)
        Z0[p] = z
        G0[1, p + 4, 8:40] = w
        a = a + fold(G0[0, p + 4, 8:40] * z)
        b = b + fold(z * w)
    ar = all_reduce_start(dots_tile(a, b), 0)
    ar = precondition(1, ar)
    alpha = all_reduce_end(ar, 0)
    keep_u.wait()

    a = b = zero8
    for p in range(32):
        y, v = apply_plane(p)
        z = Z0[p]
        w = G0[1, p + 4, 8:40]
        r1 = G0[0, p + 4, 8:40] - alpha * w
        z1 = z - alpha * y
        w1 = w - alpha * v
        sol[p] = U[p] + alpha * z
        res[p] = r1
        Y0[p] = z1
        V[p] = w1
        a = a + fold(r1 * z1)
        b = b + fold(z1 * w1)
    ar = all_reduce_start(dots_tile(a, b), 1)
    send_all(ar)
    early = pending[: -len(ar)]
    pending[:] = pending[-len(ar) :]
    finish(early)
    ar = all_reduce_next(ar, 1)
    send_all(ar)
    alpha1 = all_reduce_end(ar, 1)

    last_alpha[...] = jnp.broadcast_to(alpha1, (8, LANES))
    finish(pending)


def update_kernel(sol, res, z, w, alpha, sol_out, res_out, new_sol, new_res, sems):
    a = alpha[0:1]
    copies = []
    for c in range(4):
        for p in range(8 * c, 8 * c + 8):
            new_sol[p] = sol[p] + a * z[p]
            new_res[p] = res[p] - a * w[p]
        part = pl.ds(8 * c, 8)
        copies.append(pltpu.make_async_copy(new_sol.at[part], sol_out.at[part], sems.at[2 * c]))
        copies.append(pltpu.make_async_copy(new_res.at[part], res_out.at[part], sems.at[2 * c + 1]))
        copies[-2].start()
        copies[-1].start()
    for copy in copies:
        copy.wait()


def shards(rhs, u):
    v = lambda *shape: pltpu.VMEM(shape, F32)
    field = v(32, 32, 128)
    scratch = [
        field, field,
        v(40, 48, 128), field,
        v(2, 40, 48, 128), v(2, 24, 32, 128), v(2, 16, 24, 128),
        v(40, 48, 128), v(40, 48, 128),
        v(24, 32, 128), v(24, 32, 128), v(16, 24, 128), v(16, 24, 128),
        field,
        v(16, 16, 128), v(8, 16, 128),
        v(2, 2, 21, 8, 128), v(2, 2, 21, 8, 128), v(2, 4, 16, 128), v(2, 4, 16, 128), v(2, 2, 40, 128), v(2, 2, 40, 128),
        v(2, 4, 40, 128), v(2, 2, 2, 40, 128), v(2, 2, 2, 40, 128),
        v(2, 2, 32, 128), v(2, 2, 32, 128),
        v(2, 4, 48, 128), v(4, 48, 128), v(2, 4, 48, 128), v(4, 48, 128),
        v(4, 32, 128), v(4, 32, 128),
        v(2, 3, 16, 2, 128), v(8, 128),
        v(18, 32, 128), v(18, 32, 128), v(18, 32, 128), v(18, 32, 128),
        v(10, 24, 128), v(10, 24, 128), v(10, 24, 128),
        v(6, 24, 128), v(6, 24, 128), v(6, 24, 128),
        v(18, 48, 128), v(18, 48, 128), v(10, 32, 128), v(6, 16, 128), v(8, 16, 128), v(4, 16, 128),
        v(2, 8, 2, 128), v(2, 16, 2, 128),
        pltpu.SemaphoreType.DMA((NSEM,)), pltpu.SemaphoreType.DMA((NSEM,)), pltpu.SemaphoreType.DMA((3,)),
    ]
    block = jax.ShapeDtypeStruct((32, 32, 128), F32)
    fields = pl.pallas_call(
        kernel,
        out_shape=(block,) * 4 + (jax.ShapeDtypeStruct((8, 128), F32),),
        in_specs=[pl.BlockSpec(memory_space=pltpu.HBM)] * 2,
        out_specs=[pl.BlockSpec(memory_space=pltpu.VMEM)] * 5,
        scratch_shapes=scratch,
        compiler_params=pltpu.CompilerParams(
            collective_id=0, has_side_effects=True, vmem_limit_bytes=24 * 2**20
        ),
    )(pltpu.with_memory_space_constraint(rhs, pltpu.HBM), pltpu.with_memory_space_constraint(u, pltpu.HBM))
    return pl.pallas_call(
        update_kernel,
        out_shape=(block, block),
        in_specs=[pl.BlockSpec(memory_space=pltpu.VMEM)] * 5,
        out_specs=[pl.BlockSpec(memory_space=pltpu.HBM)] * 2,
        scratch_shapes=[v(32, 32, 128), v(32, 32, 128), pltpu.SemaphoreType.DMA((8,))],
        compiler_params=pltpu.CompilerParams(vmem_limit_bytes=4 * 2**20),
    )(*fields)


def solution(mesh):
    spec = P("gx", "gy", "gz")
    return jax.shard_map(
        shards, mesh=mesh, in_specs=(spec, spec), out_specs=(spec, spec), check_vma=False
    )
```

```python
import functools

import jax
import jax.numpy as jnp
from jax import lax
from jax.experimental import pallas as pl
from jax.experimental.pallas import tpu as pltpu
from jax.sharding import PartitionSpec as P

F32 = jnp.float32
BF16 = jnp.bfloat16
MESH = pl.DeviceIdType.MESH
NGX, NGY, NGZ = 4, 4, 8
LANES = 128

S_SET = 6
O_X, O_Y, O_D, O_Z, O_ZL, O_C3, O_ARA, O_ARB = 0, 6, 10, 14, 16, 18, 66, 74
SET = 90
NSEM = S_SET + 2 * SET


def roll(v, shift, axis):
    n = v.shape[axis]
    shift = shift % n
    return v if shift == 0 else pltpu.roll(v, shift, axis)


def iota(shape, axis):
    return lax.broadcasted_iota(jnp.int32, shape, axis)


def dotx(x, m):
    hi = x.astype(BF16)
    rest = x - hi.astype(F32)
    mid = rest.astype(BF16)
    low = (rest - mid.astype(F32)).astype(BF16)
    n = x.shape[0]
    y = jnp.dot(jnp.concatenate([hi, mid, low], axis=0), m, preferred_element_type=F32)
    return y[0:n] + y[n : 2 * n] + y[2 * n : 3 * n]


def kernel(
    rhs_hbm, u_hbm, sol, res, Y0, V, last_alpha,
    RHS, U, ZR, ZO, G0, G1, G2, SA0, SB0, SA1, SB1, SA2, SB2, Z0,
    Q1, Q2, YS, YR, DS, DR, XS, XR, ZC, ZCS, ZCR, ZL, ZLR, SLA, SLB, SHA, SHB, R1S, R1R, C3, T3,
    G3, SA3, SB3, C3P, G4, SA4, SB4, G5, SA5, SB5,
    ZP0, ZPO, ZP1, ZP2, ZP3, ZP4, ARA, ARB, ss, rs, ls,
):
    gx, gy, gz = lax.axis_index("gx"), lax.axis_index("gy"), lax.axis_index("gz")
    x_up, x_dn = gx < NGX - 1, gx > 0
    y_up, y_dn = gy < NGY - 1, gy > 0
    z_up, z_dn = gz < NGZ - 1, gz > 0
    one = lambda c: jnp.where(c, F32(1.0), F32(0.0))
    fxu, fxd, fyu, fyd, fzu, fzd = map(one, (x_up, x_dn, y_up, y_dn, z_up, z_dn))
    gxu, gxd = lax.rem(gx + 1, NGX), lax.rem(gx + NGX - 1, NGX)
    gyu, gyd = lax.rem(gy + 1, NGY), lax.rem(gy + NGY - 1, NGY)
    gzu, gzd = lax.rem(gz + 1, NGZ), lax.rem(gz + NGZ - 1, NGZ)
    gx_core = gx + 1 - 2 * lax.rem(gx, 2)
    gx_far = lax.rem(gx + 2, NGX)

    pending = []

    def rcopy(src, dst, i, dev):
        return pltpu.make_async_remote_copy(
            src_ref=src, dst_ref=dst, send_sem=ss.at[i], recv_sem=rs.at[i],
            device_id=dev, device_id_type=MESH,
        )

    def send(copy, cond=None):
        if cond is None:
            copy.start()
        else:
            pl.when(cond)(lambda: copy.start())
        pending.append((copy, cond))

    def sent(copy, cond):
        pending[:] = [q for q in pending if q[0] is not copy]
        pl.when(cond)(copy.wait_send)

    def recv(copy, cond=None):
        if cond is None:
            copy.wait_recv()
        else:
            pl.when(cond)(lambda: copy.wait_recv())

    def finish(copies):
        for copy, cond in copies:
            if cond is None:
                copy.wait_send()
            else:
                pl.when(cond)(copy.wait_send)

    def send_all(copies):
        for c in copies:
            send(c)

    inner = (pl.ds(4, 32), pl.ds(8, 32))
    get_u = pltpu.make_async_copy(u_hbm, ZR.at[inner], ls.at[0])
    get_rhs = pltpu.make_async_copy(rhs_hbm, RHS, ls.at[1])
    keep_u = pltpu.make_async_copy(u_hbm, U, ls.at[2])
    get_u.start()
    get_rhs.start()
    keep_u.start()

    bar = pltpu.get_barrier_semaphore()
    greet = [(1, 0, 0), (3, 0, 0), (0, 1, 0), (0, 3, 0), (0, 0, 1), (0, 0, 7)]
    greet += [(dx, dy, dz) for dz in (0, 1, 7) for dx in range(NGX) for dy in range(NGY)]
    greet += [(dx, 0, dz) for dz in range(2, 7) for dx in (0, 2)]
    greet = list(dict.fromkeys(g for g in greet if any(g)))
    hops = ((0, 1, 2, 1), (0, 1, 2, 1), (0, 2, 1, 3, 2, 3, 1, 2))
    greet.sort(key=lambda g: -sum(h[d] for h, d in zip(hops, g)))
    near = {
        "gx": [gx, gxu, gx_far, gxd],
        "gy": [gy, gyu, lax.rem(gy + 2, NGY), gyd],
        "gz": [lax.rem(gz + dz, NGZ) for dz in range(NGZ)],
    }
    for dx, dy, dz in greet:
        pl.semaphore_signal(
            bar, inc=1, device_id_type=MESH, device_id={"gx": near["gx"][dx], "gy": near["gy"][dy], "gz": near["gz"][dz]}
        )
    def clear(*refs):
        def run():
            for ref in refs:
                ref[...] = jnp.zeros_like(ref)

        return run

    pl.when(jnp.logical_not(x_dn))(clear(ZR.at[3]))
    pl.when(jnp.logical_not(x_up))(clear(ZR.at[36]))
    for i, there in enumerate((y_dn, y_up, z_dn, z_up)):
        pl.when(jnp.logical_not(there))(clear(R1R.at[i]))
    get_u.wait()

    lane8 = iota((8, LANES), 1)
    row8 = iota((8, LANES), 0)
    lane32 = iota((32, LANES), 1)
    lane40 = iota((40, LANES), 1)

    diagonals = []
    for up_x in (True, False):
        for up_y in (True, False):
            diagonals.append((
                {"gx": gxu if up_x else gxd, "gy": gyu if up_y else gyd},
                (x_up if up_x else x_dn) & (y_up if up_y else y_dn),
                (x_dn if up_x else x_up) & (y_dn if up_y else y_up),
            ))

    r1x = [
        rcopy(ZR.at[pl.ds(35, 1), pl.ds(8, 32)], ZR.at[pl.ds(3, 1), pl.ds(8, 32)], 0, {"gx": gxu}),
        rcopy(ZR.at[pl.ds(4, 1), pl.ds(8, 32)], ZR.at[pl.ds(36, 1), pl.ds(8, 32)], 1, {"gx": gxd}),
    ]
    devs = [{"gy": gyu}, {"gy": gyd}, {"gz": gzu}, {"gz": gzd}]
    conds = [y_up, y_dn, z_up, z_dn]
    backs = [y_dn, y_up, z_dn, z_up]
    r1 = [rcopy(R1S.at[min(i, 2)], R1R.at[i], 2 + i, devs[i]) for i in range(4)]
    zz = jnp.zeros((32, LANES), F32)
    for p in range(32):
        zz = jnp.where(lane32 >> 1 == p, roll(ZR[p + 4, 8:40], 2 * p + 1, 1), zz)
    R1S[2] = zz
    for p in range(32):
        R1S[0, p : p + 1, :] = ZR[p + 4, 39:40, :]
        R1S[1, p : p + 1, :] = ZR[p + 4, 8:9, :]
    pl.semaphore_wait(bar, len(greet))
    send(r1[2], conds[2])
    send(r1[3], conds[3])
    send(r1x[0], x_up)
    send(r1x[1], x_dn)
    send(r1[0], conds[0])
    send(r1[1], conds[1])

    for k in range(2):
        pl.when(jnp.logical_not(x_dn))(clear(G0.at[k, pl.ds(0, 4)], XR.at[k, 0]))
        pl.when(jnp.logical_not(x_up))(clear(G0.at[k, pl.ds(36, 4)], XR.at[k, 1]))
        pl.when(jnp.logical_not(y_dn))(clear(YR.at[k, 0]))
        pl.when(jnp.logical_not(y_up))(clear(YR.at[k, 1]))
        pl.when(jnp.logical_not(z_dn))(clear(ZCR.at[k, 0], ZLR.at[k, 0], C3.at[k, 1]))
        pl.when(jnp.logical_not(z_up))(clear(ZCR.at[k, 1], ZLR.at[k, 1], C3.at[k, 2]))
        for d, (_, _, from_there) in enumerate(diagonals):
            pl.when(jnp.logical_not(from_there))(clear(DR.at[k, d]))
    for ref in (G3, SA3, SB3, C3P, G4, SA4, SB4, G5, SA5, SB5, Q2):
        ref[...] = jnp.zeros_like(ref)
    kk, jj = iota((LANES, LANES), 0), iota((LANES, LANES), 1)

    def const(cond, value):
        return jnp.where(cond, F32(value), F32(0.0)).astype(BF16)

    rz1 = const((kk >> 1) == (jj & 63), 0.5)
    rz2 = const((kk >> 2) == (jj & 31), 0.25)
    rz3 = jnp.concatenate([const((kk >> 3) + 16 * i == jj, 0.125) for i in range(4)], axis=0)
    ring_k = jnp.where(kk < 96, kk >> 1, (kk >> 1) + 64)
    ring_j = jnp.where(jj < 96, jj >> 1, (jj >> 1) + 64)
    rring = const(ring_k == jj, 0.5)
    pring = const(ring_j == kk, 1.0)
    p0 = jnp.concatenate([const((jj >> 1) == kk, 1.0), const((jj >> 1) + 64 == kk, 1.0)], axis=1)

    ninth = F32(1.0 / 9.0)

    def mask9(rows, lo_rows, hi_rows, lanes_in):
        row, lane = iota((rows, LANES), 0), iota((rows, LANES), 1)
        my = jnp.where(row < lo_rows, fyd, jnp.where(row < hi_rows, F32(1.0), fyu))
        mz = jnp.where(lane < lanes_in, F32(1.0), jnp.where(lane < 96, fzu, fzd))
        return my * mz * ninth

    get_rhs.wait()
    recv(r1x[0], x_dn)
    recv(r1x[1], x_up)
    for i in range(4):
        recv(r1[i], backs[i])
    for c, cond in zip(r1x, (x_up, x_dn)):
        sent(c, cond)
    faces = jnp.where((lane32 & 1) == 0, R1R[2], R1R[3])
    for p in range(32):
        ZR[p + 4, 7:8, :] = R1R[0, p : p + 1, :]
        ZR[p + 4, 40:41, :] = R1R[1, p : p + 1, :]
        ZO[p] = roll(faces, -(2 * p + 1), 1)

    def apply_plane(p):
        c = ZR[p + 4, 8:40]
        o = ZO[p]
        left = roll(jnp.where(lane32 == 127, o, c), 1, 1)
        right = roll(jnp.where(lane32 == 0, o, c), -1, 1)
        ysum = ZR[p + 4, 7:39] + ZR[p + 4, 9:41]
        xsum = ZR[p + 3, 8:40] + ZR[p + 5, 8:40]
        return c, 6.0 * c - ((xsum + ysum) + (left + right))

    for p in range(32):
        _, a = apply_plane(p)
        G0[0, p + 4, 8:40] = RHS[p] - a

    m0 = mask9(40, 4, 36, 128)
    m1 = mask9(24, 4, 20, 64)
    m2 = mask9(16, 4, 12, 32)
    m3 = mask9(16, 0, 16, 16)
    m4 = mask9(8, 0, 8, 8)
    m5 = jnp.where(row8 < 4, mask9(8, 0, 8, 4), F32(0.0))
    slot_lane = lane40 - 12 * sum((lane40 >= 12 * i).astype(jnp.int32) for i in range(1, 11))
    slot_low = slot_lane < 6
    my0 = jnp.where(lane40 < 12, fxd, jnp.where(lane40 < 108, F32(1.0), fxu)) * m0
    ms_lo = my0 * jnp.where(slot_low, fzd, F32(1.0))
    ms_hi = my0 * jnp.where(slot_low, F32(1.0), fzu)

    def in_slot(lane, s):
        return (lane >= 12 * s) & (lane < 12 * s + 12)

    def stencil_sum(v, up_row, dn_row, prev, nxt):
        return ((up_row + dn_row) + (prev + nxt)) + (roll(v, 1, 1) + roll(v, -1, 1))

    def sweep_plane(src, dst, g, p, r0, r1, m):
        v = src[p, r0:r1]
        n = stencil_sum(v, src[p, r0 - 1 : r1 - 1], src[p, r0 + 1 : r1 + 1], src[p - 1, r0:r1], src[p + 1, r0:r1])
        dst[p, r0:r1] = m * (3.0 * v + n) + g[p, r0:r1]

    def sweep0(src, dst, g, j):
        for p in range(j, 4):
            sweep_plane(src, dst, g, p, 4, 44, m0 * fxd)

        for p in range(4, 36):
            sweep_plane(src, dst, g, p, 4, 44, m0)
        for p in range(36, 40 - j):
            sweep_plane(src, dst, g, p, 4, 44, m0 * fxu)

    def sweeps12(g, sa, sb, n, m):
        lo, hi = m * fxd, m * fxu
        for j, (src, dst) in enumerate(((g, sa), (sa, sb), (sb, sa)), 1):
            for p in range(j, n + 8 - j):
                sweep_plane(src, dst, g, p, 4, 12 + n, lo if p < 4 else m if p < n + 4 else hi)

    def sweeps_small(g, sa, sb, n, rows, m):
        for src, dst in ((g, sa), (sa, sb), (sb, sa)):
            for p in range(1, n + 1):
                sweep_plane(src, dst, g, p, 8, 8 + rows, m)
        return sa

    def sweep_slab(src, dst, g, m):
        for q in range(4):
            v = src[q, 4:44]
            prev = src[q - 1, 4:44] if q else roll(src[3, 4:44], 12, 1)
            nxt = src[q + 1, 4:44] if q < 3 else roll(src[0, 4:44], -12, 1)
            n = stencil_sum(v, src[q, 3:43], src[q, 5:45], prev, nxt)
            dst[q, 4:44] = m * (3.0 * v + n) + g[q, 4:44]

    def pair_mean(a, b, first_row, rows):
        even, odd = pl.ds(first_row, rows, stride=2), pl.ds(first_row + 1, rows, stride=2)
        return 0.25 * ((a[even, :] + a[odd, :]) + (b[even, :] + b[odd, :]))

    def double_rows(dst, v):
        n = v.shape[0]
        dst[pl.ds(0, n, stride=2), :] = v
        dst[pl.ds(1, n, stride=2), :] = v

    def all_reduce_start(tile, k):
        o = S_SET + SET * k
        mine = lax.rem(gx, 2) * NGY + gy
        ARA[k, mine] = tile
        copies = []
        for dc in range(2):
            for dy in range(NGY):
                if dc or dy:
                    dev = {"gx": gx_core if dc else gx, "gy": lax.rem(gy + dy, NGY)}
                    copies.append(rcopy(ARA.at[k, mine], ARA.at[k, mine], o + O_ARA + dc * NGY + dy, dev))
        return copies

    def total(ref, k, n):
        t = [ref[k, i] for i in range(n)]
        while len(t) > 1:
            t = [t[i] + t[i + 1] for i in range(0, len(t), 2)]
        return t[0]

    def all_reduce_next(copies, k):
        o = S_SET + SET * k
        for c in copies:
            recv(c)
        mine = (gx >> 1) * NGZ + gz
        ARB[k, mine] = total(ARA, k, 8)
        out = []
        for far in range(2):
            for dz in range(NGZ):
                if far or dz:
                    dev = {"gx": gx_far if far else gx, "gz": lax.rem(gz + dz, NGZ)}
                    out.append(rcopy(ARB.at[k, mine], ARB.at[k, mine], o + O_ARB + far * NGZ + dz, dev))
        return out

    def all_reduce_end(copies, k):
        for c in copies:
            recv(c)
        tile = total(ARB, k, 16)
        along = jnp.sum(tile[0:1], axis=1, keepdims=True)
        curve = jnp.sum(tile[1:2], axis=1, keepdims=True)
        return along / curve

    def dots_tile(a, b):
        a = jnp.sum(a, axis=0, keepdims=True)
        b = jnp.sum(b, axis=0, keepdims=True)
        return jnp.concatenate([a, b], axis=0)

    def fold(x):
        return (x[0:8] + x[8:16]) + (x[16:24] + x[24:32])

    def precondition(k, ar):
        o = S_SET + SET * k
        g0, g1, g2 = G0.at[k], G1.at[k], G2.at[k]
        xs = [
            (rcopy(g0.at[pl.ds(32, 4), pl.ds(8, 32)], g0.at[pl.ds(0, 4), pl.ds(8, 32)], o + O_X + 0, {"gx": gxu}), x_up, x_dn),
            (rcopy(g0.at[pl.ds(4, 4), pl.ds(8, 32)], g0.at[pl.ds(36, 4), pl.ds(8, 32)], o + O_X + 1, {"gx": gxd}), x_dn, x_up),
        ]
        ys = []
        for d in range(2):
            r0 = 36 if d == 0 else 8
            for h in range(2):
                YS[k, d, 0:16, pl.ds(4 * h, 4)] = g0[4 + 16 * h : 20 + 16 * h, r0 : r0 + 4]
            dev, s, r = (({"gy": gyu}, y_up, y_dn), ({"gy": gyd}, y_dn, y_up))[d]
            ys.append((rcopy(YS.at[k, d, pl.ds(0, 16)], YR.at[k, d, pl.ds(0, 16)], o + O_Y + d, dev), s, r))
        if ar is not None:
            send_all(ar)
        for c, s, _ in ys + xs:
            send(c, s)
        for i in range(16):
            Q1[i] = pair_mean(g0.at[2 * i + 4], g0.at[2 * i + 5], 8, 16)
        for i in range(8):
            Q2[i, 0:8] = pair_mean(Q1.at[2 * i], Q1.at[2 * i + 1], 0, 8)
        q3 = jnp.concatenate([pair_mean(Q2.at[2 * i], Q2.at[2 * i + 1], 0, 8) for i in range(4)], axis=1)
        T3[...] = dotx(q3, rz3)
        t3 = jnp.where(lane40[0:4] < 64, T3[pl.ds(0, 4, stride=2), :], roll(T3[pl.ds(1, 4, stride=2), :], 64, 1))
        mine = gx * NGY + gy
        C3[k, 0, mine] = t3[0:2]
        c3 = []
        for dz, dev_z, s, r in ((0, gz, None, None), (1, gzu, z_up, z_dn), (2, gzd, z_dn, z_up)):
            for dx in range(NGX):
                for dy in range(NGY):
                    if dz or dx or dy:
                        c3.append((rcopy(
                            C3.at[k, 0, mine], C3.at[k, dz, mine], o + O_C3 + 16 * dz + dx * NGY + dy,
                            {"gx": lax.rem(gx + dx, NGX), "gy": lax.rem(gy + dy, NGY), "gz": dev_z},
                        ), s, r))
        for n, cond in ((15, None), (16, z_up), (16, z_dn)):
            group = [c for c, s, _ in c3 if s is cond]
            assert len(group) == n

            def start(group=group):
                for c in group:
                    c.start()

            start() if cond is None else pl.when(cond)(start)
            pending.extend((c, cond) for c in group)
        g2[4:12, 8:16] = dotx(Q2[:, 0:8].reshape(64, LANES), rz2).reshape(8, 8, LANES)
        g1[4:20, 8:24] = dotx(Q1[...].reshape(256, LANES), rz1).reshape(16, 16, LANES)
        lane4 = iota((1, 4, LANES), 2)
        quarter = [lane4 < 32, lane4 < 64, lane4 < 96]

        def four(v):
            return jnp.where(quarter[1], jnp.where(quarter[0], v[0], v[1]), jnp.where(quarter[2], v[2], v[3]))

        ds = []
        for d in range(2):
            r1, r2 = (20, 12) if d == 0 else (8, 8)
            for h in range(2):
                rows = pl.ds(4 * h, 4)
                a, b = g1[4 + 4 * h : 8 + 4 * h, r1 : r1 + 4], g1[12 + 4 * h : 16 + 4 * h, r1 : r1 + 4]
                YS[k, d, 16:20, rows] = jnp.where(quarter[1], a, b)
                YS[k, d, 20:21, rows] = four([g2[4 + 2 * i + h : 5 + 2 * i + h, r2 : r2 + 4] for i in range(4)])
            dev, s, r = (({"gy": gyu}, y_up, y_dn), ({"gy": gyd}, y_dn, y_up))[d]
            ys.append((rcopy(YS.at[k, d, pl.ds(16, 5)], YR.at[k, d, pl.ds(16, 5)], o + O_Y + 2 + d, dev), s, r))
        for d, (dev, s, r) in enumerate(diagonals):
            up_x, up_y = d < 2, d % 2 == 0
            at = lambda n, i: 3 + n - (i - 1) if up_x else 4 + i - 1
            row = lambda n, m: 8 + n - m if up_y else 8
            for i, m, to in ((1, 3, 0), (2, 2, 3), (3, 1, 5)):
                DS[k, d, to : to + m] = g0[at(32, i), pl.ds(row(32, m), m)]
            low3 = lane40[0:3] < 64
            DS[k, d, 8:11] = jnp.where(low3, g1[at(16, 1), pl.ds(row(16, 3), 3)], g1[at(16, 2), pl.ds(row(16, 3), 3)])
            DS[k, d, 11:12] = g1[at(16, 3), pl.ds(row(16, 1), 1)]
            v = [g2[at(8, i), pl.ds(row(8, 3), 3)] for i in (1, 2, 3)]
            DS[k, d, 12:15] = jnp.where(low3, jnp.where(lane40[0:3] < 32, v[0], v[1]), v[2])
            ds.append((rcopy(DS.at[k, d], DR.at[k, d], o + O_D + d, dev), s, r))
        lane16 = iota((16, LANES), 1)
        eighth = [lane8 < 32, lane8 < 64, lane8 < 96]
        more = []
        for d in range(2):
            p1, p2 = (16, 8) if d == 0 else (4, 4)
            for h in range(2):
                XS[k, d, 16 * h : 16 * h + 16] = jnp.where(lane16 < 64, g1[p1 + h, 8:24], g1[p1 + 2 + h, 8:24])
            v = [g2[p2 + i, 8:16] for i in range(4)]
            XS[k, d, 32:40] = jnp.where(eighth[1], jnp.where(eighth[0], v[0], v[1]), jnp.where(eighth[2], v[2], v[3]))
            dev, s, r = (({"gx": gxu}, x_up, x_dn), ({"gx": gxd}, x_dn, x_up))[d]
            more.append((rcopy(XS.at[k, d], XR.at[k, d], o + O_X + 2 + d, dev), s, r))
        for c, s, _ in ys[2:] + ds + more:
            send(c, s)
        for q in range(4):
            acc = jnp.zeros((32, LANES), F32)
            for s in range(1, 9):
                acc = jnp.where(in_slot(lane32, s), roll(g0[4 * s + q, 8:40], 12 * s + 6, 1), acc)
            ZC[k, q, 4:36] = acc
        if ar is not None:
            ar = all_reduce_next(ar, 0)
            send_all(ar)
        for c, _, r in xs + more + ys + ds:
            recv(c, r)
        for d in range(2):
            p1, p2 = (0, 0) if d == 0 else (20, 12)
            for h in range(2):
                v = XR[k, d, 16 * h : 16 * h + 16]
                w = roll(v, 64, 1)
                g1[p1 + h, 8:24] = jnp.where(lane16 < 64, v, w)
                g1[p1 + 2 + h, 8:24] = jnp.where(lane16 < 64, w, v)
            v = XR[k, d, 32:40]
            w = [roll(v, 32 * i, 1) for i in range(4)]
            for i in range(4):
                g2[p2 + i, 8:16] = jnp.where(eighth[0], w[(4 - i) % 4], w[(5 - i) % 4])
        for d in range(2):
            r0, r1, r2 = (4, 4, 4) if d == 0 else (40, 24, 16)
            for h in range(2):
                rows = pl.ds(4 * h, 4)
                g0[4 + 16 * h : 20 + 16 * h, r0 : r0 + 4] = YR[k, d, 0:16, rows]
                v = YR[k, d, 16:20, rows]
                w = roll(v, 64, 2)
                g1[4 + 4 * h : 8 + 4 * h, r1 : r1 + 4] = jnp.where(quarter[1], v, w)
                g1[12 + 4 * h : 16 + 4 * h, r1 : r1 + 4] = jnp.where(quarter[1], w, v)
                v = YR[k, d, 20:21, rows]
                w = [roll(v, 32 * i, 2) for i in range(4)]
                for i in range(4):
                    g2[4 + 2 * i + h : 5 + 2 * i + h, r2 : r2 + 4] = jnp.where(quarter[0], w[(4 - i) % 4], w[(5 - i) % 4])
        for d in range(4):
            up_x, up_y = d < 2, d % 2 == 0
            at = lambda n, i: 4 - i if up_x else 3 + n + i
            row = lambda n, m: 8 - m if up_y else 8 + n
            for i, m, to in ((1, 3, 0), (2, 2, 3), (3, 1, 5)):
                g0[at(32, i), pl.ds(row(32, m), m)] = DR[k, d, to : to + m]
            low3 = lane40[0:3] < 64
            v = DR[k, d, 8:11]
            w = roll(v, 64, 1)
            g1[at(16, 1), pl.ds(row(16, 3), 3)] = jnp.where(low3, v, w)
            g1[at(16, 2), pl.ds(row(16, 3), 3)] = jnp.where(low3, w, v)
            g1[at(16, 3), pl.ds(row(16, 1), 1)] = DR[k, d, 11:12]
            v = DR[k, d, 12:15]
            w = [roll(v, 32 * i, 1) for i in range(4)]
            for i in range(3):
                g2[at(8, i + 1), pl.ds(row(8, 3), 3)] = jnp.where(lane40[0:3] < 32, w[(4 - i) % 4], w[(5 - i) % 4])
        half_slots = []
        for h in range(2):
            acc = jnp.zeros((24, LANES), F32)
            for s in range(12):
                acc = jnp.where(lane40[0:24] >> 3 == s, roll(g1[12 * h + s, 4:28], 8 * s - 60, 1), acc)
            half_slots.append(acc)
        acc = jnp.zeros((16, LANES), F32)
        for s in range(16):
            acc = jnp.where(lane40[0:16] >> 3 == s, roll(g2[s, 4:20], 8 * s - 28, 1), acc)
        half_slots += [acc[0:8], acc[8:16]]
        for i, n in ((0, 24), (2, 8)):
            a, b = half_slots[i : i + 2]
            first_four = (lane40[0:n] & 4) == 0
            rows = pl.ds(12 * i, n)
            ZL[k, 0, rows] = jnp.where(first_four, a, roll(b, 4, 1))
            ZL[k, 1, rows] = jnp.where(first_four, roll(a, -4, 1), b)
        zl = [
            (rcopy(ZL.at[k, 0], ZLR.at[k, 0], o + O_ZL + 0, {"gz": gzu}), z_up, z_dn),
            (rcopy(ZL.at[k, 1], ZLR.at[k, 1], o + O_ZL + 1, {"gz": gzd}), z_dn, z_up),
        ]
        for c, s, _ in zl:
            send(c, s)
        for q in range(4):
            mid = ZC[k, q, 4:36]
            for s in (0, 9):
                mid = jnp.where(in_slot(lane32, s), roll(g0[4 * s + q, 8:40], 12 * s + 6, 1), mid)
            ZC[k, q, 4:36] = mid
            acc = jnp.zeros((8, LANES), F32)
            for s in range(10):
                g = g0.at[4 * s + q]
                v = jnp.concatenate([g[4:8], g[40:44]], axis=0)
                acc = jnp.where(in_slot(lane8, s), roll(v, 12 * s + 6, 1), acc)
            ZC[k, q, 0:4] = acc[0:4]
            ZC[k, q, 36:40] = acc[4:8]
        for i in range(2):
            a, b = ZC[k, 2 * i], ZC[k, 2 * i + 1]
            ZCS[k, 0, i] = jnp.where(slot_low, a, roll(b, 6, 1))
            ZCS[k, 1, i] = jnp.where(slot_low, roll(a, -6, 1), b)
        zs = [
            (rcopy(ZCS.at[k, 0], ZCR.at[k, 0], o + O_Z + 0, {"gz": gzu}), z_up, z_dn),
            (rcopy(ZCS.at[k, 1], ZCR.at[k, 1], o + O_Z + 1, {"gz": gzd}), z_dn, z_up),
        ]
        for c, s, _ in zs:
            send(c, s)
        sweep0(g0, SA0, g0, 1)
        sweep0(SA0, SB0, g0, 2)
        sweep0(SB0, SA0, g0, 3)
        for cond in (None, z_dn, z_up):
            group = [c for c, _, r in c3 if r is cond]

            def wait(group=group):
                for c in group:
                    c.wait_recv()

            wait() if cond is None else pl.when(cond)(wait)
        for g in range(4):
            own, lo, hi = (jnp.concatenate([C3[k, i, 4 * g + j] for j in range(4)], axis=0) for i in range(3))
            for px in range(4):
                for odd in range(2):
                    off = 16 * px + 64 * odd
                    v = jnp.where(lane8 < 32, roll(hi, 16 - off, 1), roll(lo, 112 - off, 1))
                    v = jnp.where(lane8 < 16, roll(own, -off, 1), v)
                    G3.at[4 * g + px + 1][pl.ds(8 + odd, 8, stride=2), :] = v
        q = jnp.concatenate([pair_mean(G3.at[2 * i + 1], G3.at[2 * i + 2], 8, 8) for i in range(8)], axis=0)
        q = dotx(q, rring)
        for i in range(8):
            G4[i + 1, 8:16] = q[8 * i : 8 * i + 8]
        q = jnp.concatenate([pair_mean(G4.at[2 * i + 1], G4.at[2 * i + 2], 8, 8) for i in range(4)], axis=0)
        q = dotx(q, rring)
        for i in range(4):
            G5[i + 1, 8:16] = jnp.where(row8 < 4, q[8 * i : 8 * i + 8], F32(0.0))
        s5 = sweeps_small(G5, SA5, SB5, 4, 8, m5)
        s4 = sweeps_small(G4, SA4, SB4, 8, 8, m4)
        s3 = sweeps_small(G3, SA3, SB3, 16, 16, m3)
        t5 = dotx(jnp.concatenate([s5[i + 1, 8:16] for i in range(4)], axis=0) * F32(4.0**5 / 9.0), pring)
        for i in range(4):
            double_rows(ZP4.at[i], t5[8 * i : 8 * i + 8])
        c4 = jnp.concatenate([s4[i + 1, 8:16] * F32(4.0**4 / 9.0) + ZP4[i // 2, 0:8] for i in range(8)], axis=0)
        t4 = dotx(c4, pring)
        for i in range(8):
            double_rows(ZP3.at[i], t4[8 * i : 8 * i + 8])
        for i in range(16):
            C3P[i + 1, 8:24] = s3[i + 1, 8:24] * F32(4.0**3 / 9.0) + ZP3[i // 2]
        start = 8 + 4 * gy - 2
        c3l = [C3P[4 * gx + i, pl.ds(start, 8), :] for i in range(6)]
        t3 = dotx(jnp.concatenate(c3l, axis=0), pring)
        for i in range(6):
            double_rows(ZP2.at[i], t3[8 * i : 8 * i + 8])
        for c, _, r in zl:
            recv(c, r)
        lane24, lane16 = lane40[0:24], lane40[0:16]
        lo, hi = ZLR[k, 0, 0:24], ZLR[k, 1, 0:24]
        for p in range(24):
            at = 8 * (p % 12) + 4 * (p // 12)
            v = jnp.where(lane24 < 96, roll(hi, 64 - at, 1), roll(lo, 124 - at, 1))
            g1[p, 4:28] = jnp.where(lane24 < 64, g1[p, 4:28], v)
        lo = jnp.concatenate([ZLR[k, 0, 24:32], roll(ZLR[k, 0, 24:32], -4, 1)], axis=0)
        hi = jnp.concatenate([ZLR[k, 1, 24:32], roll(ZLR[k, 1, 24:32], -4, 1)], axis=0)
        for p in range(16):
            v = jnp.where(lane16 < 96, roll(hi, 32 - 8 * p, 1), roll(lo, 124 - 8 * p, 1))
            g2[p, 4:20] = jnp.where(lane16 < 32, g2[p, 4:20], v)
        sweeps12(g2, SA2, SB2, 8, m2)
        sweeps12(g1, SA1, SB1, 16, m1)
        for c, _, r in zs:
            recv(c, r)
        for i in range(2):
            below, above = ZCR[k, 0, i], ZCR[k, 1, i]
            a, b = ZC[k, 2 * i], ZC[k, 2 * i + 1]
            SLA[0, 2 * i, 4:44] = jnp.where(slot_low, below, a)
            SLA[0, 2 * i + 1, 4:44] = jnp.where(slot_low, roll(below, -6, 1), b)
            SHA[0, 2 * i, 4:44] = jnp.where(slot_low, a, roll(above, 6, 1))
            SHA[0, 2 * i + 1, 4:44] = jnp.where(slot_low, b, above)
        slabs = ((SLA, SLB, ms_lo), (SHA, SHB, ms_hi))
        c2 = [SA2[p, 4:20] * F32(16.0 / 9.0) + ZP2[(p - 2) // 2] for p in range(3, 13)]
        t2 = dotx(jnp.concatenate(c2, axis=0), pring)
        for a, b, m in slabs:
            sweep_slab(a.at[0], a.at[1], a.at[0], m)
        for i in range(10):
            double_rows(ZP1.at[i], t2[16 * i : 16 * i + 16])
        c1 = [SA1[p, 4:28] * F32(4.0 / 9.0) + ZP1[(p - 2) // 2, 4:28] for p in range(3, 21)]
        t1 = dotx(jnp.concatenate(c1, axis=0), p0)
        for a, b, m in slabs:
            sweep_slab(a.at[1], b, a.at[0], m)
            sweep_slab(b, a.at[1], a.at[0], m)
        for i in range(18):
            double_rows(ZP0.at[i], t1[24 * i : 24 * i + 24, 0:128])
            double_rows(ZPO.at[i], t1[24 * i : 24 * i + 24, 128:256])
        edge40 = (lane40 < 3) | (lane40 >= 125)
        merged = [jnp.where(slot_low, SHA[1, q, 4:44], SLA[1, q, 4:44]) for q in range(4)]
        for q in range(4):
            SLB[q, 4:44] = merged[q]
            SHB[q, 4:44] = jnp.where(slot_low, SLA[1, q, 4:44], SHA[1, q, 4:44])
        for p in range(3, 37):
            s, q = p // 4, p % 4
            e = roll(SLB[q, 4:44], -(12 * s + 6), 1)
            z = jnp.where(edge40, e, SA0[p, 4:44])
            ZR[p, 4:44] = z * ninth + ZP0[(p - 2) // 2, 4:44]
            if 4 <= p < 36:
                e = roll(SHB[q, 8:40], -(12 * s + 6), 1)
                ZO[p - 4] = e * ninth + ZPO[(p - 2) // 2, 8:40]
        return ar

    precondition(0, None)

    zero8 = jnp.zeros((8, LANES), F32)
    a = b = zero8
    for p in range(32):
        z, w = apply_plane(p)
        Z0[p] = z
        G0[1, p + 4, 8:40] = w
        a = a + fold(G0[0, p + 4, 8:40] * z)
        b = b + fold(z * w)
    ar = all_reduce_start(dots_tile(a, b), 0)
    ar = precondition(1, ar)
    alpha = all_reduce_end(ar, 0)
    keep_u.wait()

    a = b = zero8
    for p in range(32):
        y, v = apply_plane(p)
        z = Z0[p]
        w = G0[1, p + 4, 8:40]
        r1 = G0[0, p + 4, 8:40] - alpha * w
        z1 = z - alpha * y
        w1 = w - alpha * v
        sol[p] = U[p] + alpha * z
        res[p] = r1
        Y0[p] = z1
        V[p] = w1
        a = a + fold(r1 * z1)
        b = b + fold(z1 * w1)
    ar = all_reduce_start(dots_tile(a, b), 1)
    send_all(ar)
    early = pending[: -len(ar)]
    pending[:] = pending[-len(ar) :]
    finish(early)
    ar = all_reduce_next(ar, 1)
    send_all(ar)
    alpha1 = all_reduce_end(ar, 1)

    last_alpha[...] = jnp.broadcast_to(alpha1, (8, LANES))
    finish(pending)


def update_kernel(sol, res, z, w, alpha, sol_out, res_out, new_sol, new_res, sems):
    a = alpha[0:1]
    copies = []
    for c in range(4):
        for p in range(8 * c, 8 * c + 8):
            new_sol[p] = sol[p] + a * z[p]
            new_res[p] = res[p] - a * w[p]
        part = pl.ds(8 * c, 8)
        copies.append(pltpu.make_async_copy(new_sol.at[part], sol_out.at[part], sems.at[2 * c]))
        copies.append(pltpu.make_async_copy(new_res.at[part], res_out.at[part], sems.at[2 * c + 1]))
        copies[-2].start()
        copies[-1].start()
    for copy in copies:
        copy.wait()


def shards(rhs, u):
    v = lambda *shape: pltpu.VMEM(shape, F32)
    field = v(32, 32, 128)
    scratch = [
        field, field,
        v(40, 48, 128), field,
        v(2, 40, 48, 128), v(2, 24, 32, 128), v(2, 16, 24, 128),
        v(40, 48, 128), v(40, 48, 128),
        v(24, 32, 128), v(24, 32, 128), v(16, 24, 128), v(16, 24, 128),
        field,
        v(16, 16, 128), v(8, 16, 128),
        v(2, 2, 21, 8, 128), v(2, 2, 21, 8, 128), v(2, 4, 16, 128), v(2, 4, 16, 128), v(2, 2, 40, 128), v(2, 2, 40, 128),
        v(2, 4, 40, 128), v(2, 2, 2, 40, 128), v(2, 2, 2, 40, 128),
        v(2, 2, 32, 128), v(2, 2, 32, 128),
        v(2, 4, 48, 128), v(4, 48, 128), v(2, 4, 48, 128), v(4, 48, 128),
        v(4, 32, 128), v(4, 32, 128),
        v(2, 3, 16, 2, 128), v(8, 128),
        v(18, 32, 128), v(18, 32, 128), v(18, 32, 128), v(18, 32, 128),
        v(10, 24, 128), v(10, 24, 128), v(10, 24, 128),
        v(6, 24, 128), v(6, 24, 128), v(6, 24, 128),
        v(18, 48, 128), v(18, 48, 128), v(10, 32, 128), v(6, 16, 128), v(8, 16, 128), v(4, 16, 128),
        v(2, 8, 2, 128), v(2, 16, 2, 128),
        pltpu.SemaphoreType.DMA((NSEM,)), pltpu.SemaphoreType.DMA((NSEM,)), pltpu.SemaphoreType.DMA((3,)),
    ]
    block = jax.ShapeDtypeStruct((32, 32, 128), F32)
    fields = pl.pallas_call(
        kernel,
        out_shape=(block,) * 4 + (jax.ShapeDtypeStruct((8, 128), F32),),
        in_specs=[pl.BlockSpec(memory_space=pltpu.HBM)] * 2,
        out_specs=[pl.BlockSpec(memory_space=pltpu.VMEM)] * 5,
        scratch_shapes=scratch,
        compiler_params=pltpu.CompilerParams(
            collective_id=0, has_side_effects=True, vmem_limit_bytes=24 * 2**20
        ),
    )(pltpu.with_memory_space_constraint(rhs, pltpu.HBM), pltpu.with_memory_space_constraint(u, pltpu.HBM))
    return pl.pallas_call(
        update_kernel,
        out_shape=(block, block),
        in_specs=[pl.BlockSpec(memory_space=pltpu.VMEM)] * 5,
        out_specs=[pl.BlockSpec(memory_space=pltpu.HBM)] * 2,
        scratch_shapes=[v(32, 32, 128), v(32, 32, 128), pltpu.SemaphoreType.DMA((8,))],
        compiler_params=pltpu.CompilerParams(vmem_limit_bytes=4 * 2**20),
    )(*fields)


def solution(mesh):
    spec = P("gx", "gy", "gz")
    return jax.shard_map(
        shards, mesh=mesh, in_specs=(spec, spec), out_specs=(spec, spec), check_vma=False
    )
```

```python
import functools

import jax
import jax.numpy as jnp
from jax import lax
from jax.experimental import pallas as pl
from jax.experimental.pallas import tpu as pltpu
from jax.sharding import PartitionSpec as P

F32 = jnp.float32
BF16 = jnp.bfloat16
MESH = pl.DeviceIdType.MESH
NGX, NGY, NGZ = 4, 4, 8
LANES = 128

S_SET = 6
O_X, O_Y, O_D, O_Z, O_ZL, O_C3, O_ARA, O_ARB = 0, 6, 10, 14, 16, 18, 66, 74
SET = 90
NSEM = S_SET + 2 * SET


def roll(v, shift, axis):
    n = v.shape[axis]
    shift = shift % n
    return v if shift == 0 else pltpu.roll(v, shift, axis)


def iota(shape, axis):
    return lax.broadcasted_iota(jnp.int32, shape, axis)


def dotx(x, m):
    hi = x.astype(BF16)
    rest = x - hi.astype(F32)
    mid = rest.astype(BF16)
    low = (rest - mid.astype(F32)).astype(BF16)
    n = x.shape[0]
    y = jnp.dot(jnp.concatenate([hi, mid, low], axis=0), m, preferred_element_type=F32)
    return y[0:n] + y[n : 2 * n] + y[2 * n : 3 * n]


def kernel(
    rhs_hbm, u_hbm, sol, res, Y0, V, last_alpha,
    RHS, U, ZR, ZO, G0, G1, G2, SA0, SB0, SA1, SB1, SA2, SB2, Z0,
    Q1, Q2, YS, YR, DS, DR, XS, XR, ZC, ZCS, ZCR, ZL, ZLR, SLA, SLB, SHA, SHB, R1S, R1R, C3, T3,
    G3, SA3, SB3, C3P, G4, SA4, SB4, G5, SA5, SB5,
    ZP0, ZPO, ZP1, ZP2, ZP3, ZP4, ARA, ARB, ss, rs, ls,
):
    gx, gy, gz = lax.axis_index("gx"), lax.axis_index("gy"), lax.axis_index("gz")
    x_up, x_dn = gx < NGX - 1, gx > 0
    y_up, y_dn = gy < NGY - 1, gy > 0
    z_up, z_dn = gz < NGZ - 1, gz > 0
    one = lambda c: jnp.where(c, F32(1.0), F32(0.0))
    fxu, fxd, fyu, fyd, fzu, fzd = map(one, (x_up, x_dn, y_up, y_dn, z_up, z_dn))
    gxu, gxd = lax.rem(gx + 1, NGX), lax.rem(gx + NGX - 1, NGX)
    gyu, gyd = lax.rem(gy + 1, NGY), lax.rem(gy + NGY - 1, NGY)
    gzu, gzd = lax.rem(gz + 1, NGZ), lax.rem(gz + NGZ - 1, NGZ)
    gx_core = gx + 1 - 2 * lax.rem(gx, 2)
    gx_far = lax.rem(gx + 2, NGX)

    pending = []

    def rcopy(src, dst, i, dev):
        return pltpu.make_async_remote_copy(
            src_ref=src, dst_ref=dst, send_sem=ss.at[i], recv_sem=rs.at[i],
            device_id=dev, device_id_type=MESH,
        )

    def send(copy, cond=None):
        if cond is None:
            copy.start()
        else:
            pl.when(cond)(lambda: copy.start())
        pending.append((copy, cond))

    def sent(copy, cond):
        pending[:] = [q for q in pending if q[0] is not copy]
        pl.when(cond)(copy.wait_send)

    def recv(copy, cond=None):
        if cond is None:
            copy.wait_recv()
        else:
            pl.when(cond)(lambda: copy.wait_recv())

    def finish(copies):
        for copy, cond in copies:
            if cond is None:
                copy.wait_send()
            else:
                pl.when(cond)(copy.wait_send)

    def send_all(copies):
        for c in copies:
            send(c)

    inner = (pl.ds(4, 32), pl.ds(8, 32))
    get_u = pltpu.make_async_copy(u_hbm, ZR.at[inner], ls.at[0])
    get_rhs = pltpu.make_async_copy(rhs_hbm, RHS, ls.at[1])
    keep_u = pltpu.make_async_copy(u_hbm, U, ls.at[2])
    get_u.start()
    get_rhs.start()
    keep_u.start()

    bar = pltpu.get_barrier_semaphore()
    greet = [(1, 0, 0), (3, 0, 0), (0, 1, 0), (0, 3, 0), (0, 0, 1), (0, 0, 7)]
    greet += [(dx, dy, dz) for dz in (0, 1, 7) for dx in range(NGX) for dy in range(NGY)]
    greet += [(dx, 0, dz) for dz in range(2, 7) for dx in (0, 2)]
    greet = list(dict.fromkeys(g for g in greet if any(g)))
    hops = ((0, 1, 2, 1), (0, 1, 2, 1), (0, 2, 1, 3, 2, 3, 1, 2))
    greet.sort(key=lambda g: -sum(h[d] for h, d in zip(hops, g)))
    near = {
        "gx": [gx, gxu, gx_far, gxd],
        "gy": [gy, gyu, lax.rem(gy + 2, NGY), gyd],
        "gz": [lax.rem(gz + dz, NGZ) for dz in range(NGZ)],
    }
    for dx, dy, dz in greet:
        pl.semaphore_signal(
            bar, inc=1, device_id_type=MESH, device_id={"gx": near["gx"][dx], "gy": near["gy"][dy], "gz": near["gz"][dz]}
        )
    def clear(*refs):
        def run():
            for ref in refs:
                ref[...] = jnp.zeros_like(ref)

        return run

    pl.when(jnp.logical_not(x_dn))(clear(ZR.at[3]))
    pl.when(jnp.logical_not(x_up))(clear(ZR.at[36]))
    for i, there in enumerate((y_dn, y_up, z_dn, z_up)):
        pl.when(jnp.logical_not(there))(clear(R1R.at[i]))
    get_u.wait()

    lane8 = iota((8, LANES), 1)
    row8 = iota((8, LANES), 0)
    lane32 = iota((32, LANES), 1)
    lane40 = iota((40, LANES), 1)

    diagonals = []
    for up_x in (True, False):
        for up_y in (True, False):
            diagonals.append((
                {"gx": gxu if up_x else gxd, "gy": gyu if up_y else gyd},
                (x_up if up_x else x_dn) & (y_up if up_y else y_dn),
                (x_dn if up_x else x_up) & (y_dn if up_y else y_up),
            ))

    r1x = [
        rcopy(ZR.at[pl.ds(35, 1), pl.ds(8, 32)], ZR.at[pl.ds(3, 1), pl.ds(8, 32)], 0, {"gx": gxu}),
        rcopy(ZR.at[pl.ds(4, 1), pl.ds(8, 32)], ZR.at[pl.ds(36, 1), pl.ds(8, 32)], 1, {"gx": gxd}),
    ]
    devs = [{"gy": gyu}, {"gy": gyd}, {"gz": gzu}, {"gz": gzd}]
    conds = [y_up, y_dn, z_up, z_dn]
    backs = [y_dn, y_up, z_dn, z_up]
    r1 = [rcopy(R1S.at[min(i, 2)], R1R.at[i], 2 + i, devs[i]) for i in range(4)]
    zz = jnp.zeros((32, LANES), F32)
    for p in range(32):
        zz = jnp.where(lane32 >> 1 == p, roll(ZR[p + 4, 8:40], 2 * p + 1, 1), zz)
    R1S[2] = zz
    for p in range(32):
        R1S[0, p : p + 1, :] = ZR[p + 4, 39:40, :]
        R1S[1, p : p + 1, :] = ZR[p + 4, 8:9, :]
    pl.semaphore_wait(bar, len(greet))
    send(r1[2], conds[2])
    send(r1[3], conds[3])
    send(r1x[0], x_up)
    send(r1x[1], x_dn)
    send(r1[0], conds[0])
    send(r1[1], conds[1])

    for k in range(2):
        pl.when(jnp.logical_not(x_dn))(clear(G0.at[k, pl.ds(0, 4)], XR.at[k, 0]))
        pl.when(jnp.logical_not(x_up))(clear(G0.at[k, pl.ds(36, 4)], XR.at[k, 1]))
        pl.when(jnp.logical_not(y_dn))(clear(YR.at[k, 0]))
        pl.when(jnp.logical_not(y_up))(clear(YR.at[k, 1]))
        pl.when(jnp.logical_not(z_dn))(clear(ZCR.at[k, 0], ZLR.at[k, 0], C3.at[k, 1]))
        pl.when(jnp.logical_not(z_up))(clear(ZCR.at[k, 1], ZLR.at[k, 1], C3.at[k, 2]))
        for d, (_, _, from_there) in enumerate(diagonals):
            pl.when(jnp.logical_not(from_there))(clear(DR.at[k, d]))
    for ref in (G3, SA3, SB3, C3P, G4, SA4, SB4, G5, SA5, SB5, Q2):
        ref[...] = jnp.zeros_like(ref)
    kk, jj = iota((LANES, LANES), 0), iota((LANES, LANES), 1)

    def const(cond, value):
        return jnp.where(cond, F32(value), F32(0.0)).astype(BF16)

    rz1 = const((kk >> 1) == (jj & 63), 0.5)
    rz2 = const((kk >> 2) == (jj & 31), 0.25)
    rz3 = jnp.concatenate([const((kk >> 3) + 16 * i == jj, 0.125) for i in range(4)], axis=0)
    ring_k = jnp.where(kk < 96, kk >> 1, (kk >> 1) + 64)
    ring_j = jnp.where(jj < 96, jj >> 1, (jj >> 1) + 64)
    rring = const(ring_k == jj, 0.5)
    pring = const(ring_j == kk, 1.0)
    p0 = jnp.concatenate([const((jj >> 1) == kk, 1.0), const((jj >> 1) + 64 == kk, 1.0)], axis=1)

    ninth = F32(1.0 / 9.0)

    def mask9(rows, lo_rows, hi_rows, lanes_in):
        row, lane = iota((rows, LANES), 0), iota((rows, LANES), 1)
        my = jnp.where(row < lo_rows, fyd, jnp.where(row < hi_rows, F32(1.0), fyu))
        mz = jnp.where(lane < lanes_in, F32(1.0), jnp.where(lane < 96, fzu, fzd))
        return my * mz * ninth

    get_rhs.wait()
    recv(r1x[0], x_dn)
    recv(r1x[1], x_up)
    for i in range(4):
        recv(r1[i], backs[i])
    for c, cond in zip(r1x, (x_up, x_dn)):
        sent(c, cond)
    faces = jnp.where((lane32 & 1) == 0, R1R[2], R1R[3])
    for p in range(32):
        ZR[p + 4, 7:8, :] = R1R[0, p : p + 1, :]
        ZR[p + 4, 40:41, :] = R1R[1, p : p + 1, :]
        ZO[p] = roll(faces, -(2 * p + 1), 1)

    def apply_plane(p):
        c = ZR[p + 4, 8:40]
        o = ZO[p]
        left = roll(jnp.where(lane32 == 127, o, c), 1, 1)
        right = roll(jnp.where(lane32 == 0, o, c), -1, 1)
        ysum = ZR[p + 4, 7:39] + ZR[p + 4, 9:41]
        xsum = ZR[p + 3, 8:40] + ZR[p + 5, 8:40]
        return c, 6.0 * c - ((xsum + ysum) + (left + right))

    for p in range(32):
        _, a = apply_plane(p)
        G0[0, p + 4, 8:40] = RHS[p] - a

    m0 = mask9(40, 4, 36, 128)
    m1 = mask9(24, 4, 20, 64)
    m2 = mask9(16, 4, 12, 32)
    m3 = mask9(16, 0, 16, 16)
    m4 = mask9(8, 0, 8, 8)
    m5 = jnp.where(row8 < 4, mask9(8, 0, 8, 4), F32(0.0))
    slot_lane = lane40 - 12 * sum((lane40 >= 12 * i).astype(jnp.int32) for i in range(1, 11))
    slot_low = slot_lane < 6
    my0 = jnp.where(lane40 < 12, fxd, jnp.where(lane40 < 108, F32(1.0), fxu)) * m0
    ms_lo = my0 * jnp.where(slot_low, fzd, F32(1.0))
    ms_hi = my0 * jnp.where(slot_low, F32(1.0), fzu)

    def in_slot(lane, s):
        return (lane >= 12 * s) & (lane < 12 * s + 12)

    def stencil_sum(v, up_row, dn_row, prev, nxt):
        return ((up_row + dn_row) + (prev + nxt)) + (roll(v, 1, 1) + roll(v, -1, 1))

    def sweep_plane(src, dst, g, p, r0, r1, m):
        v = src[p, r0:r1]
        n = stencil_sum(v, src[p, r0 - 1 : r1 - 1], src[p, r0 + 1 : r1 + 1], src[p - 1, r0:r1], src[p + 1, r0:r1])
        dst[p, r0:r1] = m * (3.0 * v + n) + g[p, r0:r1]

    def sweep0(src, dst, g, j):
        for p in range(j, 4):
            sweep_plane(src, dst, g, p, 4, 44, m0 * fxd)

        for p in range(4, 36):
            sweep_plane(src, dst, g, p, 4, 44, m0)
        for p in range(36, 40 - j):
            sweep_plane(src, dst, g, p, 4, 44, m0 * fxu)

    def sweeps12(g, sa, sb, n, m):
        lo, hi = m * fxd, m * fxu
        for j, (src, dst) in enumerate(((g, sa), (sa, sb), (sb, sa)), 1):
            for p in range(j, n + 8 - j):
                sweep_plane(src, dst, g, p, 4, 12 + n, lo if p < 4 else m if p < n + 4 else hi)

    def sweeps_small(g, sa, sb, n, rows, m):
        for src, dst in ((g, sa), (sa, sb), (sb, sa)):
            for p in range(1, n + 1):
                sweep_plane(src, dst, g, p, 8, 8 + rows, m)
        return sa

    def sweep_slab(src, dst, g, m):
        for q in range(4):
            v = src[q, 4:44]
            prev = src[q - 1, 4:44] if q else roll(src[3, 4:44], 12, 1)
            nxt = src[q + 1, 4:44] if q < 3 else roll(src[0, 4:44], -12, 1)
            n = stencil_sum(v, src[q, 3:43], src[q, 5:45], prev, nxt)
            dst[q, 4:44] = m * (3.0 * v + n) + g[q, 4:44]

    def pair_mean(a, b, first_row, rows):
        even, odd = pl.ds(first_row, rows, stride=2), pl.ds(first_row + 1, rows, stride=2)
        return 0.25 * ((a[even, :] + a[odd, :]) + (b[even, :] + b[odd, :]))

    def double_rows(dst, v):
        n = v.shape[0]
        dst[pl.ds(0, n, stride=2), :] = v
        dst[pl.ds(1, n, stride=2), :] = v

    def all_reduce_start(tile, k):
        o = S_SET + SET * k
        mine = lax.rem(gx, 2) * NGY + gy
        ARA[k, mine] = tile
        copies = []
        for dc in range(2):
            for dy in range(NGY):
                if dc or dy:
                    dev = {"gx": gx_core if dc else gx, "gy": lax.rem(gy + dy, NGY)}
                    copies.append(rcopy(ARA.at[k, mine], ARA.at[k, mine], o + O_ARA + dc * NGY + dy, dev))
        return copies

    def total(ref, k, n):
        t = [ref[k, i] for i in range(n)]
        while len(t) > 1:
            t = [t[i] + t[i + 1] for i in range(0, len(t), 2)]
        return t[0]

    def all_reduce_next(copies, k):
        o = S_SET + SET * k
        for c in copies:
            recv(c)
        mine = (gx >> 1) * NGZ + gz
        ARB[k, mine] = total(ARA, k, 8)
        out = []
        for far in range(2):
            for dz in range(NGZ):
                if far or dz:
                    dev = {"gx": gx_far if far else gx, "gz": lax.rem(gz + dz, NGZ)}
                    out.append(rcopy(ARB.at[k, mine], ARB.at[k, mine], o + O_ARB + far * NGZ + dz, dev))
        return out

    def all_reduce_end(copies, k):
        for c in copies:
            recv(c)
        tile = total(ARB, k, 16)
        along = jnp.sum(tile[0:1], axis=1, keepdims=True)
        curve = jnp.sum(tile[1:2], axis=1, keepdims=True)
        return along / curve

    def dots_tile(a, b):
        a = jnp.sum(a, axis=0, keepdims=True)
        b = jnp.sum(b, axis=0, keepdims=True)
        return jnp.concatenate([a, b], axis=0)

    def fold(x):
        return (x[0:8] + x[8:16]) + (x[16:24] + x[24:32])

    def precondition(k, ar):
        o = S_SET + SET * k
        g0, g1, g2 = G0.at[k], G1.at[k], G2.at[k]
        xs = [
            (rcopy(g0.at[pl.ds(32, 4), pl.ds(8, 32)], g0.at[pl.ds(0, 4), pl.ds(8, 32)], o + O_X + 0, {"gx": gxu}), x_up, x_dn),
            (rcopy(g0.at[pl.ds(4, 4), pl.ds(8, 32)], g0.at[pl.ds(36, 4), pl.ds(8, 32)], o + O_X + 1, {"gx": gxd}), x_dn, x_up),
        ]
        ys = []
        for d in range(2):
            r0 = 36 if d == 0 else 8
            for h in range(2):
                YS[k, d, 0:16, pl.ds(4 * h, 4)] = g0[4 + 16 * h : 20 + 16 * h, r0 : r0 + 4]
            dev, s, r = (({"gy": gyu}, y_up, y_dn), ({"gy": gyd}, y_dn, y_up))[d]
            ys.append((rcopy(YS.at[k, d, pl.ds(0, 16)], YR.at[k, d, pl.ds(0, 16)], o + O_Y + d, dev), s, r))
        if ar is not None:
            send_all(ar)
        for c, s, _ in ys + xs:
            send(c, s)
        for i in range(16):
            Q1[i] = pair_mean(g0.at[2 * i + 4], g0.at[2 * i + 5], 8, 16)
        for i in range(8):
            Q2[i, 0:8] = pair_mean(Q1.at[2 * i], Q1.at[2 * i + 1], 0, 8)
        q3 = jnp.concatenate([pair_mean(Q2.at[2 * i], Q2.at[2 * i + 1], 0, 8) for i in range(4)], axis=1)
        T3[...] = dotx(q3, rz3)
        t3 = jnp.where(lane40[0:4] < 64, T3[pl.ds(0, 4, stride=2), :], roll(T3[pl.ds(1, 4, stride=2), :], 64, 1))
        mine = gx * NGY + gy
        C3[k, 0, mine] = t3[0:2]
        c3 = []
        for dz, dev_z, s, r in ((0, gz, None, None), (1, gzu, z_up, z_dn), (2, gzd, z_dn, z_up)):
            for dx in range(NGX):
                for dy in range(NGY):
                    if dz or dx or dy:
                        c3.append((rcopy(
                            C3.at[k, 0, mine], C3.at[k, dz, mine], o + O_C3 + 16 * dz + dx * NGY + dy,
                            {"gx": lax.rem(gx + dx, NGX), "gy": lax.rem(gy + dy, NGY), "gz": dev_z},
                        ), s, r))
        for n, cond in ((15, None), (16, z_up), (16, z_dn)):
            group = [c for c, s, _ in c3 if s is cond]
            assert len(group) == n

            def start(group=group):
                for c in group:
                    c.start()

            start() if cond is None else pl.when(cond)(start)
            pending.extend((c, cond) for c in group)
        g2[4:12, 8:16] = dotx(Q2[:, 0:8].reshape(64, LANES), rz2).reshape(8, 8, LANES)
        g1[4:20, 8:24] = dotx(Q1[...].reshape(256, LANES), rz1).reshape(16, 16, LANES)
        lane4 = iota((1, 4, LANES), 2)
        quarter = [lane4 < 32, lane4 < 64, lane4 < 96]

        def four(v):
            return jnp.where(quarter[1], jnp.where(quarter[0], v[0], v[1]), jnp.where(quarter[2], v[2], v[3]))

        ds = []
        for d in range(2):
            r1, r2 = (20, 12) if d == 0 else (8, 8)
            for h in range(2):
                rows = pl.ds(4 * h, 4)
                a, b = g1[4 + 4 * h : 8 + 4 * h, r1 : r1 + 4], g1[12 + 4 * h : 16 + 4 * h, r1 : r1 + 4]
                YS[k, d, 16:20, rows] = jnp.where(quarter[1], a, b)
                YS[k, d, 20:21, rows] = four([g2[4 + 2 * i + h : 5 + 2 * i + h, r2 : r2 + 4] for i in range(4)])
            dev, s, r = (({"gy": gyu}, y_up, y_dn), ({"gy": gyd}, y_dn, y_up))[d]
            ys.append((rcopy(YS.at[k, d, pl.ds(16, 5)], YR.at[k, d, pl.ds(16, 5)], o + O_Y + 2 + d, dev), s, r))
        for d, (dev, s, r) in enumerate(diagonals):
            up_x, up_y = d < 2, d % 2 == 0
            at = lambda n, i: 3 + n - (i - 1) if up_x else 4 + i - 1
            row = lambda n, m: 8 + n - m if up_y else 8
            for i, m, to in ((1, 3, 0), (2, 2, 3), (3, 1, 5)):
                DS[k, d, to : to + m] = g0[at(32, i), pl.ds(row(32, m), m)]
            low3 = lane40[0:3] < 64
            DS[k, d, 8:11] = jnp.where(low3, g1[at(16, 1), pl.ds(row(16, 3), 3)], g1[at(16, 2), pl.ds(row(16, 3), 3)])
            DS[k, d, 11:12] = g1[at(16, 3), pl.ds(row(16, 1), 1)]
            v = [g2[at(8, i), pl.ds(row(8, 3), 3)] for i in (1, 2, 3)]
            DS[k, d, 12:15] = jnp.where(low3, jnp.where(lane40[0:3] < 32, v[0], v[1]), v[2])
            ds.append((rcopy(DS.at[k, d], DR.at[k, d], o + O_D + d, dev), s, r))
        lane16 = iota((16, LANES), 1)
        eighth = [lane8 < 32, lane8 < 64, lane8 < 96]
        more = []
        for d in range(2):
            p1, p2 = (16, 8) if d == 0 else (4, 4)
            for h in range(2):
                XS[k, d, 16 * h : 16 * h + 16] = jnp.where(lane16 < 64, g1[p1 + h, 8:24], g1[p1 + 2 + h, 8:24])
            v = [g2[p2 + i, 8:16] for i in range(4)]
            XS[k, d, 32:40] = jnp.where(eighth[1], jnp.where(eighth[0], v[0], v[1]), jnp.where(eighth[2], v[2], v[3]))
            dev, s, r = (({"gx": gxu}, x_up, x_dn), ({"gx": gxd}, x_dn, x_up))[d]
            more.append((rcopy(XS.at[k, d], XR.at[k, d], o + O_X + 2 + d, dev), s, r))
        for c, s, _ in ys[2:] + ds + more:
            send(c, s)
        for q in range(4):
            acc = jnp.zeros((32, LANES), F32)
            for s in range(1, 9):
                acc = jnp.where(in_slot(lane32, s), roll(g0[4 * s + q, 8:40], 12 * s + 6, 1), acc)
            ZC[k, q, 4:36] = acc
        if ar is not None:
            ar = all_reduce_next(ar, 0)
            send_all(ar)
        for c, _, r in xs + more + ys + ds:
            recv(c, r)
        for d in range(2):
            p1, p2 = (0, 0) if d == 0 else (20, 12)
            for h in range(2):
                v = XR[k, d, 16 * h : 16 * h + 16]
                w = roll(v, 64, 1)
                g1[p1 + h, 8:24] = jnp.where(lane16 < 64, v, w)
                g1[p1 + 2 + h, 8:24] = jnp.where(lane16 < 64, w, v)
            v = XR[k, d, 32:40]
            w = [roll(v, 32 * i, 1) for i in range(4)]
            for i in range(4):
                g2[p2 + i, 8:16] = jnp.where(eighth[0], w[(4 - i) % 4], w[(5 - i) % 4])
        for d in range(2):
            r0, r1, r2 = (4, 4, 4) if d == 0 else (40, 24, 16)
            for h in range(2):
                rows = pl.ds(4 * h, 4)
                v = YR[k, d, 16:20, rows]
                w = roll(v, 64, 2)
                g1[4 + 4 * h : 8 + 4 * h, r1 : r1 + 4] = jnp.where(quarter[1], v, w)
                g1[12 + 4 * h : 16 + 4 * h, r1 : r1 + 4] = jnp.where(quarter[1], w, v)
                v = YR[k, d, 20:21, rows]
                w = [roll(v, 32 * i, 2) for i in range(4)]
                for i in range(4):
                    g2[4 + 2 * i + h : 5 + 2 * i + h, r2 : r2 + 4] = jnp.where(quarter[0], w[(4 - i) % 4], w[(5 - i) % 4])
        for d in range(4):
            up_x, up_y = d < 2, d % 2 == 0
            at = lambda n, i: 4 - i if up_x else 3 + n + i
            row = lambda n, m: 8 - m if up_y else 8 + n
            low3 = lane40[0:3] < 64
            v = DR[k, d, 8:11]
            w = roll(v, 64, 1)
            g1[at(16, 1), pl.ds(row(16, 3), 3)] = jnp.where(low3, v, w)
            g1[at(16, 2), pl.ds(row(16, 3), 3)] = jnp.where(low3, w, v)
            g1[at(16, 3), pl.ds(row(16, 1), 1)] = DR[k, d, 11:12]
            v = DR[k, d, 12:15]
            w = [roll(v, 32 * i, 1) for i in range(4)]
            for i in range(3):
                g2[at(8, i + 1), pl.ds(row(8, 3), 3)] = jnp.where(lane40[0:3] < 32, w[(4 - i) % 4], w[(5 - i) % 4])
        half_slots = []
        for h in range(2):
            acc = jnp.zeros((24, LANES), F32)
            for s in range(12):
                acc = jnp.where(lane40[0:24] >> 3 == s, roll(g1[12 * h + s, 4:28], 8 * s - 60, 1), acc)
            half_slots.append(acc)
        acc = jnp.zeros((16, LANES), F32)
        for s in range(16):
            acc = jnp.where(lane40[0:16] >> 3 == s, roll(g2[s, 4:20], 8 * s - 28, 1), acc)
        half_slots += [acc[0:8], acc[8:16]]
        for i, n in ((0, 24), (2, 8)):
            a, b = half_slots[i : i + 2]
            first_four = (lane40[0:n] & 4) == 0
            rows = pl.ds(12 * i, n)
            ZL[k, 0, rows] = jnp.where(first_four, a, roll(b, 4, 1))
            ZL[k, 1, rows] = jnp.where(first_four, roll(a, -4, 1), b)
        zl = [
            (rcopy(ZL.at[k, 0], ZLR.at[k, 0], o + O_ZL + 0, {"gz": gzu}), z_up, z_dn),
            (rcopy(ZL.at[k, 1], ZLR.at[k, 1], o + O_ZL + 1, {"gz": gzd}), z_dn, z_up),
        ]
        for c, s, _ in zl:
            send(c, s)
        for d in range(2):
            r0 = 4 if d == 0 else 40
            for h in range(2):
                g0[4 + 16 * h : 20 + 16 * h, r0 : r0 + 4] = YR[k, d, 0:16, pl.ds(4 * h, 4)]
        for d in range(4):
            up_x, up_y = d < 2, d % 2 == 0
            for i, m, to in ((1, 3, 0), (2, 2, 3), (3, 1, 5)):
                g0[4 - i if up_x else 35 + i, pl.ds(8 - m if up_y else 40, m)] = DR[k, d, to : to + m]
        for q in range(4):
            mid = ZC[k, q, 4:36]
            for s in (0, 9):
                mid = jnp.where(in_slot(lane32, s), roll(g0[4 * s + q, 8:40], 12 * s + 6, 1), mid)
            ZC[k, q, 4:36] = mid
            acc = jnp.zeros((8, LANES), F32)
            for s in range(10):
                g = g0.at[4 * s + q]
                v = jnp.concatenate([g[4:8], g[40:44]], axis=0)
                acc = jnp.where(in_slot(lane8, s), roll(v, 12 * s + 6, 1), acc)
            ZC[k, q, 0:4] = acc[0:4]
            ZC[k, q, 36:40] = acc[4:8]
        for i in range(2):
            a, b = ZC[k, 2 * i], ZC[k, 2 * i + 1]
            ZCS[k, 0, i] = jnp.where(slot_low, a, roll(b, 6, 1))
            ZCS[k, 1, i] = jnp.where(slot_low, roll(a, -6, 1), b)
        zs = [
            (rcopy(ZCS.at[k, 0], ZCR.at[k, 0], o + O_Z + 0, {"gz": gzu}), z_up, z_dn),
            (rcopy(ZCS.at[k, 1], ZCR.at[k, 1], o + O_Z + 1, {"gz": gzd}), z_dn, z_up),
        ]
        for c, s, _ in zs:
            send(c, s)
        sweep0(g0, SA0, g0, 1)
        sweep0(SA0, SB0, g0, 2)
        sweep0(SB0, SA0, g0, 3)
        for cond in (None, z_dn, z_up):
            group = [c for c, _, r in c3 if r is cond]

            def wait(group=group):
                for c in group:
                    c.wait_recv()

            wait() if cond is None else pl.when(cond)(wait)
        for g in range(4):
            own, lo, hi = (jnp.concatenate([C3[k, i, 4 * g + j] for j in range(4)], axis=0) for i in range(3))
            for px in range(4):
                for odd in range(2):
                    off = 16 * px + 64 * odd
                    v = jnp.where(lane8 < 32, roll(hi, 16 - off, 1), roll(lo, 112 - off, 1))
                    v = jnp.where(lane8 < 16, roll(own, -off, 1), v)
                    G3.at[4 * g + px + 1][pl.ds(8 + odd, 8, stride=2), :] = v
        q = jnp.concatenate([pair_mean(G3.at[2 * i + 1], G3.at[2 * i + 2], 8, 8) for i in range(8)], axis=0)
        q = dotx(q, rring)
        for i in range(8):
            G4[i + 1, 8:16] = q[8 * i : 8 * i + 8]
        q = jnp.concatenate([pair_mean(G4.at[2 * i + 1], G4.at[2 * i + 2], 8, 8) for i in range(4)], axis=0)
        q = dotx(q, rring)
        for i in range(4):
            G5[i + 1, 8:16] = jnp.where(row8 < 4, q[8 * i : 8 * i + 8], F32(0.0))
        s5 = sweeps_small(G5, SA5, SB5, 4, 8, m5)
        s4 = sweeps_small(G4, SA4, SB4, 8, 8, m4)
        s3 = sweeps_small(G3, SA3, SB3, 16, 16, m3)
        t5 = dotx(jnp.concatenate([s5[i + 1, 8:16] for i in range(4)], axis=0) * F32(4.0**5 / 9.0), pring)
        for i in range(4):
            double_rows(ZP4.at[i], t5[8 * i : 8 * i + 8])
        c4 = jnp.concatenate([s4[i + 1, 8:16] * F32(4.0**4 / 9.0) + ZP4[i // 2, 0:8] for i in range(8)], axis=0)
        t4 = dotx(c4, pring)
        for i in range(8):
            double_rows(ZP3.at[i], t4[8 * i : 8 * i + 8])
        for i in range(16):
            C3P[i + 1, 8:24] = s3[i + 1, 8:24] * F32(4.0**3 / 9.0) + ZP3[i // 2]
        start = 8 + 4 * gy - 2
        c3l = [C3P[4 * gx + i, pl.ds(start, 8), :] for i in range(6)]
        t3 = dotx(jnp.concatenate(c3l, axis=0), pring)
        for i in range(6):
            double_rows(ZP2.at[i], t3[8 * i : 8 * i + 8])
        for c, _, r in zl:
            recv(c, r)
        lane24, lane16 = lane40[0:24], lane40[0:16]
        lo, hi = ZLR[k, 0, 0:24], ZLR[k, 1, 0:24]
        for p in range(24):
            at = 8 * (p % 12) + 4 * (p // 12)
            v = jnp.where(lane24 < 96, roll(hi, 64 - at, 1), roll(lo, 124 - at, 1))
            g1[p, 4:28] = jnp.where(lane24 < 64, g1[p, 4:28], v)
        lo = jnp.concatenate([ZLR[k, 0, 24:32], roll(ZLR[k, 0, 24:32], -4, 1)], axis=0)
        hi = jnp.concatenate([ZLR[k, 1, 24:32], roll(ZLR[k, 1, 24:32], -4, 1)], axis=0)
        for p in range(16):
            v = jnp.where(lane16 < 96, roll(hi, 32 - 8 * p, 1), roll(lo, 124 - 8 * p, 1))
            g2[p, 4:20] = jnp.where(lane16 < 32, g2[p, 4:20], v)
        sweeps12(g2, SA2, SB2, 8, m2)
        sweeps12(g1, SA1, SB1, 16, m1)
        for c, _, r in zs:
            recv(c, r)
        for i in range(2):
            below, above = ZCR[k, 0, i], ZCR[k, 1, i]
            a, b = ZC[k, 2 * i], ZC[k, 2 * i + 1]
            SLA[0, 2 * i, 4:44] = jnp.where(slot_low, below, a)
            SLA[0, 2 * i + 1, 4:44] = jnp.where(slot_low, roll(below, -6, 1), b)
            SHA[0, 2 * i, 4:44] = jnp.where(slot_low, a, roll(above, 6, 1))
            SHA[0, 2 * i + 1, 4:44] = jnp.where(slot_low, b, above)
        slabs = ((SLA, SLB, ms_lo), (SHA, SHB, ms_hi))
        c2 = [SA2[p, 4:20] * F32(16.0 / 9.0) + ZP2[(p - 2) // 2] for p in range(3, 13)]
        t2 = dotx(jnp.concatenate(c2, axis=0), pring)
        for a, b, m in slabs:
            sweep_slab(a.at[0], a.at[1], a.at[0], m)
        for i in range(10):
            double_rows(ZP1.at[i], t2[16 * i : 16 * i + 16])
        c1 = [SA1[p, 4:28] * F32(4.0 / 9.0) + ZP1[(p - 2) // 2, 4:28] for p in range(3, 21)]
        t1 = dotx(jnp.concatenate(c1, axis=0), p0)
        for a, b, m in slabs:
            sweep_slab(a.at[1], b, a.at[0], m)
            sweep_slab(b, a.at[1], a.at[0], m)
        for i in range(18):
            double_rows(ZP0.at[i], t1[24 * i : 24 * i + 24, 0:128])
            double_rows(ZPO.at[i], t1[24 * i : 24 * i + 24, 128:256])
        edge40 = (lane40 < 3) | (lane40 >= 125)
        merged = [jnp.where(slot_low, SHA[1, q, 4:44], SLA[1, q, 4:44]) for q in range(4)]
        for q in range(4):
            SLB[q, 4:44] = merged[q]
            SHB[q, 4:44] = jnp.where(slot_low, SLA[1, q, 4:44], SHA[1, q, 4:44])
        for p in range(3, 37):
            s, q = p // 4, p % 4
            e = roll(SLB[q, 4:44], -(12 * s + 6), 1)
            z = jnp.where(edge40, e, SA0[p, 4:44])
            ZR[p, 4:44] = z * ninth + ZP0[(p - 2) // 2, 4:44]
            if 4 <= p < 36:
                e = roll(SHB[q, 8:40], -(12 * s + 6), 1)
                ZO[p - 4] = e * ninth + ZPO[(p - 2) // 2, 8:40]
        return ar

    precondition(0, None)

    zero8 = jnp.zeros((8, LANES), F32)
    a = b = zero8
    for p in range(32):
        z, w = apply_plane(p)
        Z0[p] = z
        G0[1, p + 4, 8:40] = w
        a = a + fold(G0[0, p + 4, 8:40] * z)
        b = b + fold(z * w)
    ar = all_reduce_start(dots_tile(a, b), 0)
    ar = precondition(1, ar)
    alpha = all_reduce_end(ar, 0)
    keep_u.wait()

    a = b = zero8
    for p in range(32):
        y, v = apply_plane(p)
        z = Z0[p]
        w = G0[1, p + 4, 8:40]
        r1 = G0[0, p + 4, 8:40] - alpha * w
        z1 = z - alpha * y
        w1 = w - alpha * v
        sol[p] = U[p] + alpha * z
        res[p] = r1
        Y0[p] = z1
        V[p] = w1
        a = a + fold(r1 * z1)
        b = b + fold(z1 * w1)
    ar = all_reduce_start(dots_tile(a, b), 1)
    send_all(ar)
    early = pending[: -len(ar)]
    pending[:] = pending[-len(ar) :]
    finish(early)
    ar = all_reduce_next(ar, 1)
    send_all(ar)
    alpha1 = all_reduce_end(ar, 1)

    last_alpha[...] = jnp.broadcast_to(alpha1, (8, LANES))
    finish(pending)


def update_kernel(sol, res, z, w, alpha, sol_out, res_out, new_sol, new_res, sems):
    a = alpha[0:1]
    copies = []
    for c in range(4):
        for p in range(8 * c, 8 * c + 8):
            new_sol[p] = sol[p] + a * z[p]
            new_res[p] = res[p] - a * w[p]
        part = pl.ds(8 * c, 8)
        copies.append(pltpu.make_async_copy(new_sol.at[part], sol_out.at[part], sems.at[2 * c]))
        copies.append(pltpu.make_async_copy(new_res.at[part], res_out.at[part], sems.at[2 * c + 1]))
        copies[-2].start()
        copies[-1].start()
    for copy in copies:
        copy.wait()


def shards(rhs, u):
    v = lambda *shape: pltpu.VMEM(shape, F32)
    field = v(32, 32, 128)
    scratch = [
        field, field,
        v(40, 48, 128), field,
        v(2, 40, 48, 128), v(2, 24, 32, 128), v(2, 16, 24, 128),
        v(40, 48, 128), v(40, 48, 128),
        v(24, 32, 128), v(24, 32, 128), v(16, 24, 128), v(16, 24, 128),
        field,
        v(16, 16, 128), v(8, 16, 128),
        v(2, 2, 21, 8, 128), v(2, 2, 21, 8, 128), v(2, 4, 16, 128), v(2, 4, 16, 128), v(2, 2, 40, 128), v(2, 2, 40, 128),
        v(2, 4, 40, 128), v(2, 2, 2, 40, 128), v(2, 2, 2, 40, 128),
        v(2, 2, 32, 128), v(2, 2, 32, 128),
        v(2, 4, 48, 128), v(4, 48, 128), v(2, 4, 48, 128), v(4, 48, 128),
        v(4, 32, 128), v(4, 32, 128),
        v(2, 3, 16, 2, 128), v(8, 128),
        v(18, 32, 128), v(18, 32, 128), v(18, 32, 128), v(18, 32, 128),
        v(10, 24, 128), v(10, 24, 128), v(10, 24, 128),
        v(6, 24, 128), v(6, 24, 128), v(6, 24, 128),
        v(18, 48, 128), v(18, 48, 128), v(10, 32, 128), v(6, 16, 128), v(8, 16, 128), v(4, 16, 128),
        v(2, 8, 2, 128), v(2, 16, 2, 128),
        pltpu.SemaphoreType.DMA((NSEM,)), pltpu.SemaphoreType.DMA((NSEM,)), pltpu.SemaphoreType.DMA((3,)),
    ]
    block = jax.ShapeDtypeStruct((32, 32, 128), F32)
    fields = pl.pallas_call(
        kernel,
        out_shape=(block,) * 4 + (jax.ShapeDtypeStruct((8, 128), F32),),
        in_specs=[pl.BlockSpec(memory_space=pltpu.HBM)] * 2,
        out_specs=[pl.BlockSpec(memory_space=pltpu.VMEM)] * 5,
        scratch_shapes=scratch,
        compiler_params=pltpu.CompilerParams(
            collective_id=0, has_side_effects=True, vmem_limit_bytes=24 * 2**20
        ),
    )(pltpu.with_memory_space_constraint(rhs, pltpu.HBM), pltpu.with_memory_space_constraint(u, pltpu.HBM))
    return pl.pallas_call(
        update_kernel,
        out_shape=(block, block),
        in_specs=[pl.BlockSpec(memory_space=pltpu.VMEM)] * 5,
        out_specs=[pl.BlockSpec(memory_space=pltpu.HBM)] * 2,
        scratch_shapes=[v(32, 32, 128), v(32, 32, 128), pltpu.SemaphoreType.DMA((8,))],
        compiler_params=pltpu.CompilerParams(vmem_limit_bytes=4 * 2**20),
    )(*fields)


def solution(mesh):
    spec = P("gx", "gy", "gz")
    return jax.shard_map(
        shards, mesh=mesh, in_specs=(spec, spec), out_specs=(spec, spec), check_vma=False
    )
```
